256 devices in a mesh: dp: 16 (over z_lo, x), shard: 16 (over z_hi, y, core).
Axes of the slice: x: 4, y: 4, z: 8 (z_hi: 2, z_lo: 4; z = z_hi * 4 + z_lo), core: 2. Of those that a mesh axis runs over, the one named last changes fastest.
Arguments:
- hidden_in: bfloat16 [65536, 5120], P(('dp', 'shard')), may hold values from -24 to 24
- teacher: bfloat16 [65536, 768], P(('dp', 'shard')), may hold values from -6 to 6
- norm_gain: bfloat16 [5120], P('shard'), may hold values from 0.5 to 1.5
- w_key: bfloat16 [5120, 768], P('shard'), may hold values from -0.078125 to 0.078125
- group_rows: int32 [16], P('dp'), may hold values from 64 to 256
- member: int32 [16, 16], P('dp', 'shard'), may hold values from 0 to 1, as said below
Outputs:
- loss: float32 [], replicated
- grad_gain: float32 [5120], P('shard')
- grad_key: float32 [5120, 768], P('shard')
The draws below stay inside these ranges and needn't reach their ends.
Inputs may be any that keep to these rules, and one draw needn't show every extreme that they name: The first group_rows[p] token slots of each surviving device of group p hold valid tokens. `member`: 1 marks a surviving device; the first device of every group survives.
All inputs are finite; a program needn't handle non-finite values.
Results may differ from the reference program's by a relative error of at most 0.0023.
Values may be sent and summed in bfloat16 or wider, within the bound.
A program may use at most 128 MiB of HBM per device.

```python
import jax
import jax.numpy as jnp
from jax import lax

D = 5120
KV = 768
TOK_DEV = 256
GROUPS = 16
MEMBERS = 16
TOKENS = 65536


def draw_member(key, part):
    picks = jax.random.randint(key, (GROUPS, MEMBERS), 0, 4)
    first = jnp.arange(MEMBERS)[None, :] == 0
    return jnp.where((picks > 0) | first, 1, 0).astype(jnp.int32)


def touch_ends(values, key, low, top_value):
    longest = values.shape.index(max(values.shape))
    spots = []
    for shift in (0, 1):
        where = [jax.random.randint(jax.random.fold_in(key, axis), (), 0, length) for axis, length in enumerate(values.shape)]
        where[longest] = (where[longest] + shift) % values.shape[longest]
        spots.append(tuple(where))
    return values.at[spots[0]].set(low).at[spots[1]].set(top_value)


def strengthened(drawn, key, source, target, blocks, factor):
    owner, partner = [(jnp.arange(drawn.shape[dim]) // (drawn.shape[dim] // blocks)).reshape([-1 if axis == dim else 1 for axis in range(drawn.ndim)]) for dim in (source, target)]
    chosen = jax.random.permutation(key, blocks)[partner]
    strong = (owner == chosen) | (owner == (partner + blocks // 2) % blocks)
    return jnp.where(strong, factor * drawn, drawn)


def block_scale(rng, dims, cuts, smallest, high):
    gain, own = 1.0, jax.random.fold_in(rng, 6)
    for dim, shards_of in cuts:
        draws = jnp.exp(jax.random.uniform(jax.random.fold_in(own, dim), (shards_of,), jnp.float32, smallest / len(cuts), high / len(cuts)))
        gain = gain * jnp.repeat(draws, dims[dim] // shards_of).reshape([-1 if axis == dim else 1 for axis in range(len(dims))])
    return gain


def noise(rng, shape, deviation, limit, cuts=(), dtype=jnp.bfloat16):
    result = deviation * jax.random.normal(rng, shape, jnp.float32)
    if cuts:
        result = result * block_scale(rng, shape, cuts, -0.22, 0.18)
    return jnp.clip(result, -limit, limit).astype(dtype)


def noise_with(rng, extent, deviation, limit, pieces, heavy, held_as=jnp.bfloat16):
    values = deviation * jax.random.normal(rng, extent, jnp.float32)
    if pieces:
        values = values * block_scale(rng, extent, pieces, -0.22, 0.18)
    return jnp.clip(strengthened(values, jax.random.fold_in(rng, 3), *heavy), -limit, limit).astype(held_as)


def setup_inputs(seed: int = 0) -> dict:
    seeds = jax.random.split(jax.random.key(seed), 7)
    return {
        "hidden_in": noise_with(seeds[0], (TOKENS, D), 1.0, 24.0, ((0, 256),), (0, 1, 256, 6.0)),
        "teacher": noise(seeds[1], (TOKENS, KV), 1.0, 6.0, ((0, 256),)),
        "norm_gain": jnp.clip(1.0 + 0.1 * jax.random.normal(seeds[2], (D,), jnp.float32), 0.5, 1.5).astype(jnp.bfloat16),
        "w_key": noise(seeds[3], (D, KV), D ** -0.5, 0.078125, ((0, 16),)),
        "group_rows": touch_ends(jax.random.randint(seeds[4], (GROUPS,), TOK_DEV // 4, TOK_DEV + 1), jax.random.fold_in(seeds[4], 1), TOK_DEV // 4, TOK_DEV).astype(jnp.int32),
        "member": draw_member(jax.random.fold_in(seeds[6], 71), 0),
    }


EPSILON = 1e-06
SCALE = 1024.0

def reference(hidden_in, teacher, norm_gain, w_key, group_rows, member):
    blocks = GROUPS * MEMBERS
    live_rows = jnp.repeat(group_rows, MEMBERS).astype(jnp.int32)
    alive = member.reshape(blocks).astype(jnp.int32)
    total_count = jnp.sum(member.astype(jnp.float32) * group_rows.astype(jnp.float32)[:, None])
    gains = norm_gain.astype(jnp.float32)

    def one_block(carry, inputs):
        loss_sum, gain_acc, key_acc = carry
        block_in, block_teacher, block_rows, block_alive = inputs
        position = lax.broadcasted_iota(jnp.int32, (TOK_DEV, 1), 0)
        valid = jnp.where((position < block_rows) & (block_alive == 1), 1.0, 0.0).astype(jnp.float32)
        values = block_in.astype(jnp.float32)
        inverse_rms = lax.rsqrt(lax.optimization_barrier(jnp.mean(values * values, axis=1, keepdims=True)) + EPSILON)
        scaled = values * inverse_rms
        normed = (scaled * gains).astype(jnp.bfloat16)
        keys = jnp.dot(normed, w_key, preferred_element_type=jnp.float32)
        diff = keys - block_teacher.astype(jnp.float32)
        loss_sum = loss_sum + jnp.sum(valid * diff * diff)
        upstream = (SCALE / total_count * valid * diff).astype(jnp.bfloat16)
        term_key = jnp.dot(normed.T, upstream, preferred_element_type=jnp.float32)
        dnormed = jnp.dot(upstream, w_key.T, preferred_element_type=jnp.float32)
        term_gain = lax.optimization_barrier(jnp.sum(dnormed * scaled, axis=0))
        return ((loss_sum, gain_acc + term_gain, key_acc + term_key), None)
    start = (jnp.zeros((), jnp.float32), jnp.zeros((D,), jnp.float32), jnp.zeros((D, KV), jnp.float32))
    inputs = (hidden_in.reshape(blocks, TOK_DEV, D), teacher.reshape(blocks, TOK_DEV, KV), live_rows, alive)
    final, unused = lax.scan(one_block, start, inputs)
    loss_sum, gain_acc, key_acc = final
    loss = loss_sum / (2.0 * KV * total_count)
    return (loss, gain_acc, key_acc)
```

```python
import jax
import jax.numpy as jnp
from jax import lax
from jax.experimental import pallas as pl
from jax.experimental.pallas import tpu as pltpu
from jax.sharding import Mesh
from jax.sharding import PartitionSpec as P

SHARD = ("shard_0", "shard_1", "shard_2")
DP_SHARD = ("dp_0", "dp_1", "shard_0", "shard_1", "shard_2")
DP = ("dp_0", "dp_1")
MESH = pl.DeviceIdType.MESH
F32, BF16 = jnp.float32, jnp.bfloat16

EPSILON = 1e-06
SCALE = 1024.0

TOK = 256
D = 5120
KV = 768
HK = KV // 2
SL = 320
PC = 2 * SL
YB = 2 * PC
QK = HK // 2
XK = QK // 4

SMALL = ("info", "w", "tea", "hid", "lsib", "out")


def slots(*groups):
    place, at = {}, 0
    for name, count in groups:
        place[name] = at
        at += count
    return place, at


SLOT, N_SLOT = slots(
    *((name, 1) for name in SMALL),
    ("ginfo", 8), ("lsh", 8), ("cnt", 16), ("ldp", 16),
    ("wy", 12), ("wz", 4), ("ry", 4), ("rx", 16), ("s2y", 4), ("s2x", 4),
    ("s3", 8), ("agz", 4), ("agx", 8),
)


def kernel(
    hid, tea, w, info, loss_o, gain_o, key_o,
    hbuf, tbuf, wbuf, nbuf, inv, keys, dkt, gbuf, ry, rx, s2y, sx, r2y, r2x, t3, r3,
    fin, kt, outs, isib, gfull, cbuf, lown, lsib, lsh, ldp,
    lsem, ssem, rsem, zsem,
):
    zl, x = lax.axis_index("dp_0"), lax.axis_index("dp_1")
    h, y, c = (lax.axis_index(a) for a in SHARD)

    def ring4(v, d):
        return lax.rem(v + d, 4)

    def to_y(d):
        return {"shard_1": ring4(y, d)}

    def to_x(d):
        return {"dp_1": ring4(x, d)}

    sib = {"shard_2": 1 - c}

    def send(src, dst, slot, dev):
        return pltpu.make_async_remote_copy(
            src_ref=src, dst_ref=dst, send_sem=ssem.at[slot], recv_sem=rsem.at[slot],
            device_id=dev, device_id_type=MESH,
        )

    shard_peers = [
        (dh * 4 + dy, {"shard_0": lax.rem(h + dh, 2), "shard_1": ring4(y, dy)})
        for dh in range(2) for dy in range(4) if dh or dy
    ]
    dp_peers = [
        (dl * 4 + dx, {"dp_0": ring4(zl, dl), "dp_1": ring4(x, dx)})
        for dl in range(4) for dx in range(4) if dl or dx
    ]
    z_peers = [
        (dh * 4 + dl, {"shard_0": lax.rem(h + dh, 2), "dp_0": ring4(zl, dl)})
        for dh in range(2) for dl in range(4) if dh or dl
    ]
    extra = [dev for at, dev in z_peers if at > 4]
    everyone = [sib] + [dev for _, dev in shard_peers + dp_peers] + extra

    own_rows = pl.ds(pl.multiple_of(h * PC + c * SL, 64), SL)
    my_cols = pl.ds(pl.multiple_of(c * HK, 128), HK)
    sib_cols = pl.ds(pl.multiple_of((1 - c) * HK, 128), HK)
    mine = y * 2 + h
    gid = zl * 4 + x

    own_hid = pltpu.make_async_copy(hid, hbuf.at[c], lsem.at[0])
    own_hid.start()
    own_w = pltpu.make_async_copy(w.at[:, my_cols], wbuf.at[y, own_rows], lsem.at[1])
    own_w.start()
    own_tea = pltpu.make_async_copy(tea.at[:, my_cols], tbuf.at[c], lsem.at[2])
    own_tea.start()

    barrier = pltpu.get_barrier_semaphore()
    for dev in everyone:
        pl.semaphore_signal(barrier, inc=1, device_id=dev, device_id_type=MESH)
    pl.semaphore_wait(barrier, len(everyone))

    sib_w = send(w.at[:, sib_cols], wbuf.at[y, own_rows], SLOT["w"], sib)
    sib_w.start()
    sib_info = send(info, isib, SLOT["info"], sib)
    sib_info.start()
    sib_tea = send(tea.at[:, sib_cols], tbuf.at[c], SLOT["tea"], sib)
    sib_tea.start()
    sib_hid = send(hid, hbuf.at[c], SLOT["hid"], sib)
    sib_hid.start()

    edge = (zl == 0) | (zl == 3)
    over = {"shard_0": 1 - h, "dp_0": 3 - zl}
    inner = {"dp_0": jnp.where(zl == 0, 1, 2)}
    zrows = PC // 4

    def z_piece(half, i):
        return wbuf.at[y, pl.ds(pl.multiple_of(half * PC + i * zrows, 32), zrows)]

    def z_over(i):
        return send(z_piece(h, i), z_piece(h, i), SLOT["wz"] + i, over)

    def z_in(i):
        ref = z_piece(1 - h, i)
        return pltpu.make_async_remote_copy(
            src_ref=ref, dst_ref=ref, send_sem=zsem.at[i], recv_sem=rsem.at[SLOT["wz"] + i],
            device_id=inner, device_id_type=MESH,
        )

    def y_copies(g):
        half = h if g == 0 else 1 - h
        base = SLOT["wy"] + 6 * g

        def part(owner, b):
            return wbuf.at[owner, pl.ds(pl.multiple_of(half * PC + b * SL, 64), SL)]

        def copy(owner, b, d, i):
            return send(part(owner, b), part(owner, b), base + i, to_y(d))

        return [
            copy(y, 0, 1, 0), copy(y, 1, 3, 1), copy(y, 1, 1, 2), copy(y, 0, 3, 3),
            copy(ring4(y, 3), 0, 1, 4), copy(ring4(y, 1), 1, 3, 5),
        ]

    first, second = y_copies(0), y_copies(1)
    own_w.wait()
    sib_w.wait_recv()

    @pl.when(edge)
    def _():
        for i in range(4):
            z_over(i).start()

    for copy in first[:4]:
        copy.start()

    sib_info.wait_recv()
    gfull[mine] = info[...] + isib[...]
    gsend = [
        send(gfull.at[mine], gfull.at[mine], SLOT["ginfo"] + at, dev) for at, dev in shard_peers
    ]
    for copy in gsend:
        copy.start()

    def norms(which):
        @pl.loop(0, TOK // 32)
        def _(i):
            rows = pl.ds(pl.multiple_of(i * 32, 32), 32)
            v = hbuf[which, rows, :].astype(F32)
            mean = jnp.sum(v * v, axis=1, keepdims=True) * (1.0 / D)
            inv[which, rows, :] = jnp.broadcast_to(lax.rsqrt(mean + EPSILON), (32, 128))

    own_hid.wait()
    norms(c)
    for copy in gsend:
        copy.wait_recv()
    group = gfull[0, :, 0:128]
    for i in range(1, 8):
        group = group + gfull[i, :, 0:128]
    cbuf[gid] = group
    csend = [send(cbuf.at[gid], cbuf.at[gid], SLOT["cnt"] + at, dev) for at, dev in dp_peers]
    for copy in csend:
        copy.start()
    sib_hid.wait_recv()
    norms(1 - c)

    for yy in range(4):
        for hh in range(2):
            src = (hh * 4 + yy) * PC
            dst = (yy * 2 + hh) * PC
            gain = gfull[yy * 2 + hh, 0:1, :]
            for which in range(2):
                @pl.loop(0, TOK // 32)
                def _(i):
                    rows = pl.ds(pl.multiple_of(i * 32, 32), 32)
                    out = pl.ds(pl.multiple_of(which * TOK + i * 32, 32), 32)
                    v = hbuf[which, rows, src : src + PC].astype(F32)
                    nbuf[out, dst : dst + PC] = (v * inv[which, rows, 0:1] * gain).astype(BF16)

    def project(owner, half, start=False):
        cols = pl.ds(pl.multiple_of(owner * YB + half * PC, 128), PC)
        rows = pl.ds(pl.multiple_of(half * PC, 64), PC)
        part = jnp.dot(nbuf[:, cols], wbuf[owner, rows, :], preferred_element_type=F32)
        keys[...] = part if start else keys[...] + part

    def y_steps(copies, half):
        copies[0].wait_recv()
        copies[4].start()
        copies[1].wait_recv()
        copies[5].start()
        copies[2].wait_recv()
        copies[3].wait_recv()

    y_steps(first, h)
    project(y, h, True)
    project(ring4(y, 3), h)
    project(ring4(y, 1), h)
    first[4].wait_recv()
    first[5].wait_recv()
    project(ring4(y, 2), h)

    for i in range(4):
        z_in(i).wait_recv()

        @pl.when(edge)
        def _():
            z_in(i).start()

    for copy in second[:4]:
        copy.start()
    project(y, 1 - h)
    y_steps(second, 1 - h)
    project(ring4(y, 3), 1 - h)
    project(ring4(y, 1), 1 - h)
    for copy in csend:
        copy.wait_recv()
    second[4].wait_recv()
    second[5].wait_recv()
    project(ring4(y, 2), 1 - h)

    count = cbuf[0]
    for i in range(1, 16):
        count = count + cbuf[i]
    count = count[1:2, 0:1]
    scale = SCALE / count
    sib_tea.wait_recv()
    own_tea.wait()
    own_n = info[1:2, 0:1]
    sib_n = isib[1:2, 0:1]
    position = lax.broadcasted_iota(jnp.int32, (TOK, 1), 0).astype(F32)
    squares = jnp.zeros((1, HK), F32)
    for which in range(2):
        live = jnp.where(c == which, own_n, sib_n)
        valid = jnp.where(position < live, 1.0, 0.0)
        rows = slice(which * TOK, (which + 1) * TOK)
        diff = keys[rows, :] - tbuf[which].astype(F32)
        squares = squares + jnp.sum(valid * diff * diff, axis=0, keepdims=True)
        dk = scale * valid * diff
        dkt[:, rows] = jnp.transpose(dk).astype(BF16)
    lown[...] = jnp.broadcast_to(jnp.sum(squares, axis=1, keepdims=True), (8, 128))
    lsend = send(lown, lsib, SLOT["lsib"], sib)
    lsend.start()

    stage1 = []
    for j in (1, 3, 2, 0):
        yy = ring4(y, j)
        cols = pl.ds(pl.multiple_of(yy * YB, 128), YB)
        gbuf[yy] = jnp.dot(dkt[...], nbuf[:, cols], preferred_element_type=F32).astype(BF16)
        if j:
            copy = send(gbuf.at[yy, 0:QK], ry.at[j - 1], SLOT["ry"] + j, to_y(j))
            copy.start()
            stage1.append(copy)
        for i in (1, 3, 2):
            rows = pl.ds(pl.multiple_of(QK + XK * ring4(x, i), 16), XK)
            copy = send(
                gbuf.at[yy, rows], rx.at[i - 1, yy], SLOT["rx"] + 4 * i + j, to_x(i)
            )
            copy.start()
            stage1.append(copy)

    lsend.wait_recv()
    lsh[mine] = lown[...] + lsib[...]
    lsends = [send(lsh.at[mine], lsh.at[mine], SLOT["lsh"] + at, dev) for at, dev in shard_peers]
    for copy in lsends:
        copy.start()

    for copy in stage1:
        copy.wait_recv()

    stage2 = []
    s2y[...] = (
        gbuf[y, 0:QK].astype(F32) + ry[0].astype(F32) + ry[1].astype(F32) + ry[2].astype(F32)
    )
    for i in (1, 3, 2):
        rows = pl.ds(pl.multiple_of(XK * ring4(x, i), 16), XK)
        copy = send(s2y.at[rows], r2y.at[i - 1], SLOT["s2y"] + i, to_x(i))
        copy.start()
        stage2.append(copy)
    my_x = pl.ds(pl.multiple_of(QK + XK * x, 16), XK)
    for j in (1, 3, 2, 0):
        yy = ring4(y, j)
        sx[yy] = (
            gbuf[yy, my_x, :].astype(F32)
            + rx[0, yy].astype(F32) + rx[1, yy].astype(F32) + rx[2, yy].astype(F32)
        )
        if j:
            copy = send(sx.at[yy], r2x.at[j - 1], SLOT["s2x"] + j, to_y(j))
            copy.start()
            stage2.append(copy)

    for copy in lsends:
        copy.wait_recv()
    total = lsh[0]
    for i in range(1, 8):
        total = total + lsh[i]
    ldp[gid] = total
    lsends2 = [send(ldp.at[gid], ldp.at[gid], SLOT["ldp"] + at, dev) for at, dev in dp_peers]
    for copy in lsends2:
        copy.start()

    for copy in stage2:
        copy.wait_recv()
    upper = s2y[pl.ds(pl.multiple_of(XK * x, 16), XK), :] + r2y[0] + r2y[1] + r2y[2]
    lower = sx[y] + r2x[0] + r2x[1] + r2x[2]
    for hh in range(2):
        for l in range(4):
            part = upper if l < 2 else lower
            t3[hh, l] = part[24 * (l % 2) : 24 * (l % 2) + 24, hh * PC : (hh + 1) * PC]
    stage3 = []
    for at, dev in z_peers:
        dh, dl = at // 4, at % 4
        copy = send(
            t3.at[lax.rem(h + dh, 2), ring4(zl, dl)], r3.at[at], SLOT["s3"] + at, dev
        )
        copy.start()
        stage3.append(copy)
    for copy in stage3:
        copy.wait_recv()
    piece = t3[h, zl]
    for at in range(1, 8):
        piece = piece + r3[at]
    fin[x, zl] = piece

    agz = [
        send(fin.at[x, zl], fin.at[x, zl], SLOT["agz"] + d, {"dp_0": ring4(zl, d)})
        for d in (1, 3, 2)
    ]
    for copy in agz:
        copy.start()
    for copy in agz:
        copy.wait_recv()
    agx = [send(fin.at[x], fin.at[x], SLOT["agx"] + d, to_x(d)) for d in (1, 3, 2)]
    for copy in agx:
        copy.start()

    for copy in lsends2:
        copy.wait_recv()
    total = ldp[0]
    for i in range(1, 16):
        total = total + ldp[i]
    loss_o[...] = total / (2.0 * KV * count)

    for copy in agx:
        copy.wait_recv()
    ordered = []
    for side in range(2):
        for xx in range(4):
            ordered += [fin[xx, 2 * side], fin[xx, 2 * side + 1]]
    kt[...] = jnp.transpose(jnp.concatenate(ordered, axis=0))
    osend = send(
        kt.at[pl.ds(pl.multiple_of((1 - c) * SL, 64), SL)], outs.at[:, my_cols],
        SLOT["out"], sib,
    )
    osend.start()
    own_out = pltpu.make_async_copy(
        kt.at[pl.ds(pl.multiple_of(c * SL, 64), SL)], outs.at[:, my_cols], lsem.at[3]
    )
    own_out.start()
    own_out.wait()
    osend.wait_recv()
    key_out = pltpu.make_async_copy(outs, key_o, lsem.at[4])
    key_out.start()
    terms = outs[...] * w[...].astype(F32)
    gain_o[...] = lax.dot_general(
        jnp.ones((8, KV), F32), terms, (((1,), (1,)), ((), ())),
        preferred_element_type=F32, precision=lax.Precision.HIGHEST,
    )
    key_out.wait()

    for copy in (
        [sib_w, sib_info, sib_tea, sib_hid, lsend, osend] + first + second + gsend + csend
        + stage1 + lsends + stage2 + lsends2 + stage3 + agz + agx
    ):
        copy.wait_send()

    @pl.when(edge)
    def _():
        for i in range(4):
            z_over(i).wait_send()
            z_in(i).wait_send()


def body(hidden_in, teacher, norm_gain, w_key, group_rows, member):
    core = lax.axis_index("shard_2")
    gain = norm_gain.astype(F32)
    row = lax.broadcasted_iota(jnp.int32, (8, PC), 0)
    lane = lax.broadcasted_iota(jnp.int32, (8, PC), 1)
    own = (row == 0) & (lane >= core * SL) & (lane < core * SL + SL)
    live = (member[0, 0] * group_rows[0]).astype(F32)
    info = jnp.where(own, jnp.concatenate([gain, gain])[None, :], jnp.where(row == 1, live, 0.0))
    vm = pl.BlockSpec(memory_space=pltpu.VMEM)
    hbm = pl.BlockSpec(memory_space=pl.ANY)
    loss, gain_sum, grad_key = pl.pallas_call(
        kernel,
        out_shape=(
            jax.ShapeDtypeStruct((8, 128), F32),
            jax.ShapeDtypeStruct((8, SL), F32),
            jax.ShapeDtypeStruct((SL, KV), F32),
        ),
        in_specs=[hbm, vm, vm, vm],
        out_specs=(vm, vm, hbm),
        scratch_shapes=[
            pltpu.VMEM((2, TOK, D), BF16),
            pltpu.VMEM((2, TOK, HK), BF16),
            pltpu.VMEM((4, YB, HK), BF16),
            pltpu.VMEM((2 * TOK, D), BF16),
            pltpu.VMEM((2, TOK, 128), F32),
            pltpu.VMEM((2 * TOK, HK), F32),
            pltpu.VMEM((HK, 2 * TOK), BF16),
            pltpu.VMEM((4, HK, YB), BF16),
            pltpu.VMEM((3, QK, YB), BF16),
            pltpu.VMEM((3, 4, XK, YB), BF16),
            pltpu.VMEM((QK, YB), F32),
            pltpu.VMEM((4, XK, YB), F32),
            pltpu.VMEM((3, XK, YB), F32),
            pltpu.VMEM((3, XK, YB), F32),
            pltpu.VMEM((2, 4, 24, PC), F32),
            pltpu.VMEM((8, 24, PC), F32),
            pltpu.VMEM((4, 4, 24, PC), F32),
            pltpu.VMEM((PC, HK), F32),
            pltpu.VMEM((SL, KV), F32),
            pltpu.VMEM((8, PC), F32),
            pltpu.VMEM((8, 8, PC), F32),
            pltpu.VMEM((16, 8, 128), F32),
            pltpu.VMEM((8, 128), F32),
            pltpu.VMEM((8, 128), F32),
            pltpu.VMEM((8, 8, 128), F32),
            pltpu.VMEM((16, 8, 128), F32),
            pltpu.SemaphoreType.DMA((5,)),
            pltpu.SemaphoreType.DMA((N_SLOT,)),
            pltpu.SemaphoreType.DMA((N_SLOT,)),
            pltpu.SemaphoreType.DMA((4,)),
        ],
        compiler_params=pltpu.CompilerParams(
            collective_id=0, has_side_effects=True, vmem_limit_bytes=62 * 2**20
        ),
    )(hidden_in, teacher, w_key, info)
    return loss[0, 0], gain_sum[0] / gain, grad_key


def solution(mesh):
    split = Mesh(mesh.devices.reshape(4, 4, 2, 4, 2), DP_SHARD)
    return jax.shard_map(
        body,
        mesh=split,
        in_specs=(
            P(DP_SHARD, None),
            P(DP_SHARD, None),
            P(SHARD),
            P(SHARD, None),
            P(DP),
            P(DP, SHARD),
        ),
        out_specs=(P(), P(SHARD), P(SHARD, None)),
        check_vma=False,
    )
```

```python
import jax
import jax.numpy as jnp
from jax import lax
from jax.experimental import pallas as pl
from jax.experimental.pallas import tpu as pltpu
from jax.sharding import Mesh
from jax.sharding import PartitionSpec as P

SHARD = ("shard_0", "shard_1", "shard_2")
DP_SHARD = ("dp_0", "dp_1", "shard_0", "shard_1", "shard_2")
DP = ("dp_0", "dp_1")
MESH = pl.DeviceIdType.MESH
F32, BF16 = jnp.float32, jnp.bfloat16

EPSILON = 1e-06
SCALE = 1024.0

TOK = 256
D = 5120
KV = 768
HK = KV // 2
SL = 320
PC = 2 * SL
YB = 2 * PC
QK = HK // 2
XK = QK // 4

DR = 160
SR = 80
SA = 48

SMALL = ("info", "w", "tea", "hid", "lsib", "out")


def slots(*groups):
    place, at = {}, 0
    for name, count in groups:
        place[name] = at
        at += count
    return place, at


SLOT, N_SLOT = slots(
    *((name, 1) for name in SMALL),
    ("ginfo", 8), ("lsh", 8), ("cnt", 16), ("ldp", 16),
    ("wy", 20), ("wx", 32), ("wz", 3), ("ry", 4), ("rx", 16), ("s2y", 4), ("s2x", 4),
    ("s3", 8), ("agz", 4), ("agx", 8),
)


def kernel(
    hid, tea, w, gain, info, loss_o, gain_o, key_o,
    hbuf, tbuf, wbuf, nbuf, inv, keys, dkt, gbuf, ry, rx, s2y, sx, r2y, r2x, t3, r3,
    fin, kt, outs, isib, gfull, cbuf, lown, lsib, lsh, ldp,
    lsem, ssem, rsem, zsem,
):
    zl, x = lax.axis_index("dp_0"), lax.axis_index("dp_1")
    h, y, c = (lax.axis_index(a) for a in SHARD)

    def ring4(v, d):
        return lax.rem(v + d, 4)

    def to_y(d):
        return {"shard_1": ring4(y, d)}

    def to_x(d):
        return {"dp_1": ring4(x, d)}

    sib = {"shard_2": 1 - c}

    def send(src, dst, slot, dev):
        return pltpu.make_async_remote_copy(
            src_ref=src, dst_ref=dst, send_sem=ssem.at[slot], recv_sem=rsem.at[slot],
            device_id=dev, device_id_type=MESH,
        )

    shard_peers = [
        (dh * 4 + dy, {"shard_0": lax.rem(h + dh, 2), "shard_1": ring4(y, dy)})
        for dh in range(2) for dy in range(4) if dh or dy
    ]
    dp_peers = [
        (dl * 4 + dx, {"dp_0": ring4(zl, dl), "dp_1": ring4(x, dx)})
        for dl in range(4) for dx in range(4) if dl or dx
    ]
    z_peers = [
        (dh * 4 + dl, {"shard_0": lax.rem(h + dh, 2), "dp_0": ring4(zl, dl)})
        for dh in range(2) for dl in range(4) if dh or dl
    ]
    extra = [dev for at, dev in z_peers if at > 4]
    everyone = [sib] + [dev for _, dev in shard_peers + dp_peers] + extra

    own_rows = pl.ds(pl.multiple_of(h * PC + c * SL, 64), SL)
    my_cols = pl.ds(pl.multiple_of(c * HK, 128), HK)
    sib_cols = pl.ds(pl.multiple_of((1 - c) * HK, 128), HK)
    mine = y * 2 + h
    gid = zl * 4 + x

    own_hid = pltpu.make_async_copy(hid, hbuf.at[c], lsem.at[0])
    own_hid.start()
    own_w = pltpu.make_async_copy(w.at[:, my_cols], wbuf.at[y, own_rows], lsem.at[1])
    own_w.start()
    own_tea = pltpu.make_async_copy(tea.at[:, my_cols], tbuf.at[c], lsem.at[2])
    own_tea.start()

    barrier = pltpu.get_barrier_semaphore()
    for dev in everyone:
        pl.semaphore_signal(barrier, inc=1, device_id=dev, device_id_type=MESH)
    pl.semaphore_wait(barrier, len(everyone))

    sib_w = send(w.at[:, sib_cols], wbuf.at[y, own_rows], SLOT["w"], sib)
    sib_w.start()
    sib_info = send(info, isib, SLOT["info"], sib)
    sib_info.start()
    sib_tea = send(tea.at[:, sib_cols], tbuf.at[c], SLOT["tea"], sib)
    sib_tea.start()
    sib_hid = send(hid, hbuf.at[c], SLOT["hid"], sib)
    sib_hid.start()

    edge = (zl == 0) | (zl == 3)
    over = {"shard_0": 1 - h, "dp_0": 3 - zl}
    inner = {"dp_0": jnp.where(zl == 0, 1, 2)}
    split = PC // 2 + SR * x

    def part(owner, half, at, n):
        return wbuf.at[owner, pl.ds(pl.multiple_of(half * PC + at, 16), n)]

    z_parts = ((split, SR), (0, DR), (DR, DR))

    def z_over(i):
        ref = part(y, h, *z_parts[i])
        return send(ref, ref, SLOT["wz"] + i, over)

    def z_in(i):
        ref = part(y, 1 - h, *z_parts[i])
        return pltpu.make_async_remote_copy(
            src_ref=ref, dst_ref=ref, send_sem=zsem.at[i], recv_sem=rsem.at[SLOT["wz"] + i],
            device_id=inner, device_id_type=MESH,
        )

    def z_take(i):
        z_in(i).wait_recv()

        @pl.when(edge)
        def _():
            z_in(i).start()

    def y_copies(g):
        half = h if g == 0 else 1 - h
        back, ahead = ring4(y, 3), ring4(y, 1)
        plan = (
            (y, split, SR, 1), (y, split, SR, 3),
            (y, 0, DR, 1), (y, DR, DR, 3), (y, DR, DR, 1), (y, 0, DR, 3),
            (back, split, SA, 1), (ahead, split + SA, SR - SA, 3),
            (back, 0, DR, 1), (ahead, DR, DR, 3),
        )
        copies = []
        for i, (owner, at, n, d) in enumerate(plan):
            ref = part(owner, half, at, n)
            copies.append(send(ref, ref, SLOT["wy"] + 10 * g + i, to_y(d)))
        return copies

    first, second = y_copies(0), y_copies(1)
    handed = {}

    def hand(g, k):
        ref = part(ring4(y, k), h if g == 0 else 1 - h, split, SR)
        handed[g, k] = [
            send(ref, ref, SLOT["wx"] + 16 * g + 4 * k + i, to_x(i)) for i in (1, 3, 2)
        ]
        for copy in handed[g, k]:
            copy.start()

    def take(*copies):
        for copy in copies:
            copy.wait_recv()

    def go(*copies):
        for copy in copies:
            copy.start()

    sib_info.wait_recv()
    gfull[mine] = info[...] + isib[...]
    gsend = [
        send(gfull.at[mine], gfull.at[mine], SLOT["ginfo"] + at, dev) for at, dev in shard_peers
    ]
    go(*gsend)
    own_w.wait()
    sib_w.wait_recv()
    go(first[0], first[1])

    @pl.when(edge)
    def _():
        z_over(0).start()

    go(first[2], first[3])

    @pl.when(edge)
    def _():
        z_over(1).start()
        z_over(2).start()

    def norms(which):
        @pl.loop(0, TOK // 32)
        def _(i):
            rows = pl.ds(pl.multiple_of(i * 32, 32), 32)
            v = hbuf[which, rows, :].astype(F32)
            mean = jnp.sum(v * v, axis=1, keepdims=True) * (1.0 / D)
            inv[which, rows, :] = jnp.broadcast_to(lax.rsqrt(mean + EPSILON), (32, 128))

    def normalize(yy, hh):
        src = (hh * 4 + yy) * PC
        dst = (yy * 2 + hh) * PC
        for which in range(2):
            @pl.loop(0, TOK // 64)
            def _(i):
                rows = pl.ds(pl.multiple_of(i * 64, 64), 64)
                out = pl.ds(pl.multiple_of(which * TOK + i * 64, 64), 64)
                scale = inv[which, rows, :]
                for lane in range(0, PC, 128):
                    by = gfull[yy * 2 + hh, 0:1, lane : lane + 128]
                    v = hbuf[which, rows, src + lane : src + lane + 128].astype(F32)
                    nbuf[out, dst + lane : dst + lane + 128] = (v * scale * by).astype(BF16)

    def project(k, g, start=False):
        half = h if g == 0 else 1 - h
        owner = ring4(y, k)
        cols = pl.ds(pl.multiple_of(owner * YB + half * PC, 128), PC)
        rows = pl.ds(pl.multiple_of(half * PC, 64), PC)
        term = jnp.dot(nbuf[:, cols], wbuf[owner, rows, :], preferred_element_type=F32)
        keys[...] = term if start else keys[...] + term

    own_hid.wait()
    norms(c)
    take(first[0], first[1])
    go(first[6], first[7])
    hand(0, 3)
    hand(0, 1)
    go(first[4], first[5])
    z_take(0)
    go(second[0], second[1])
    hand(1, 0)
    take(*gsend)
    group = gfull[0, :, 0:128]
    for i in range(1, 8):
        group = group + gfull[i, :, 0:128]
    cbuf[gid] = group
    csend = [send(cbuf.at[gid], cbuf.at[gid], SLOT["cnt"] + at, dev) for at, dev in dp_peers]
    go(*csend)
    sib_hid.wait_recv()
    norms(1 - c)
    take(first[2], first[3])
    go(first[8], first[9])
    z_take(1)
    go(second[2], second[5])
    normalize(0, 0)
    take(second[0], second[1])
    go(second[6], second[7])
    hand(1, 3)
    hand(1, 1)
    normalize(0, 1)
    take(first[6], first[7])
    hand(0, 2)
    normalize(1, 0)
    z_take(2)
    go(second[3], second[4])
    normalize(1, 1)
    normalize(2, 0)
    take(second[2])
    go(second[8])
    take(second[6], second[7])
    hand(1, 2)
    normalize(2, 1)
    normalize(3, 0)
    normalize(3, 1)
    take(second[3])
    go(second[9])
    project(0, 0, True)
    take(*handed[0, 3], *handed[0, 1], first[4], first[5])
    project(3, 0)
    project(1, 0)
    take(*handed[1, 0])
    project(0, 1)
    take(*handed[0, 2], first[8], first[9])
    project(2, 0)
    take(*csend)
    take(*handed[1, 3], *handed[1, 1], second[4], second[5])
    project(3, 1)
    project(1, 1)
    take(*handed[1, 2], second[8], second[9])
    project(2, 1)

    count = cbuf[0]
    for i in range(1, 16):
        count = count + cbuf[i]
    count = count[1:2, 0:1]
    scale = SCALE / count
    sib_tea.wait_recv()
    own_tea.wait()
    own_n = info[1:2, 0:1]
    sib_n = isib[1:2, 0:1]
    position = lax.broadcasted_iota(jnp.int32, (TOK, 1), 0).astype(F32)
    squares = jnp.zeros((1, HK), F32)
    for which in range(2):
        live = jnp.where(c == which, own_n, sib_n)
        valid = jnp.where(position < live, 1.0, 0.0)
        rows = slice(which * TOK, (which + 1) * TOK)
        diff = keys[rows, :] - tbuf[which].astype(F32)
        squares = squares + jnp.sum(valid * diff * diff, axis=0, keepdims=True)
        dk = scale * valid * diff
        dkt[:, rows] = jnp.transpose(dk).astype(BF16)
    lown[...] = jnp.broadcast_to(jnp.sum(squares, axis=1, keepdims=True), (8, 128))
    lsend = send(lown, lsib, SLOT["lsib"], sib)
    lsend.start()

    stage1 = []
    for j in (1, 3, 2, 0):
        yy = ring4(y, j)
        cols = pl.ds(pl.multiple_of(yy * YB, 128), YB)
        gbuf[yy] = jnp.dot(dkt[...], nbuf[:, cols], preferred_element_type=F32).astype(BF16)
        if j:
            copy = send(gbuf.at[yy, 0:QK], ry.at[j - 1], SLOT["ry"] + j, to_y(j))
            copy.start()
            stage1.append(copy)
        for i in (1, 3, 2):
            rows = pl.ds(pl.multiple_of(QK + XK * ring4(x, i), 16), XK)
            copy = send(
                gbuf.at[yy, rows], rx.at[i - 1, yy], SLOT["rx"] + 4 * i + j, to_x(i)
            )
            copy.start()
            stage1.append(copy)

    lsend.wait_recv()
    lsh[mine] = lown[...] + lsib[...]
    lsends = [send(lsh.at[mine], lsh.at[mine], SLOT["lsh"] + at, dev) for at, dev in shard_peers]
    for copy in lsends:
        copy.start()

    for copy in stage1:
        copy.wait_recv()

    stage2 = []
    s2y[...] = (
        gbuf[y, 0:QK].astype(F32) + ry[0].astype(F32) + ry[1].astype(F32) + ry[2].astype(F32)
    )
    for i in (1, 3, 2):
        rows = pl.ds(pl.multiple_of(XK * ring4(x, i), 16), XK)
        copy = send(s2y.at[rows], r2y.at[i - 1], SLOT["s2y"] + i, to_x(i))
        copy.start()
        stage2.append(copy)
    my_x = pl.ds(pl.multiple_of(QK + XK * x, 16), XK)
    for j in (1, 3, 2, 0):
        yy = ring4(y, j)
        sx[yy] = (
            gbuf[yy, my_x, :].astype(F32)
            + rx[0, yy].astype(F32) + rx[1, yy].astype(F32) + rx[2, yy].astype(F32)
        )
        if j:
            copy = send(sx.at[yy], r2x.at[j - 1], SLOT["s2x"] + j, to_y(j))
            copy.start()
            stage2.append(copy)

    for copy in lsends:
        copy.wait_recv()
    total = lsh[0]
    for i in range(1, 8):
        total = total + lsh[i]
    ldp[gid] = total
    lsends2 = [send(ldp.at[gid], ldp.at[gid], SLOT["ldp"] + at, dev) for at, dev in dp_peers]
    for copy in lsends2:
        copy.start()

    for copy in stage2:
        copy.wait_recv()
    upper = s2y[pl.ds(pl.multiple_of(XK * x, 16), XK), :] + r2y[0] + r2y[1] + r2y[2]
    lower = sx[y] + r2x[0] + r2x[1] + r2x[2]
    for hh in range(2):
        for l in range(4):
            rows = upper if l < 2 else lower
            t3[hh, l] = rows[24 * (l % 2) : 24 * (l % 2) + 24, hh * PC : (hh + 1) * PC]
    stage3 = []
    for at, dev in z_peers:
        dh, dl = at // 4, at % 4
        copy = send(
            t3.at[lax.rem(h + dh, 2), ring4(zl, dl)], r3.at[at], SLOT["s3"] + at, dev
        )
        copy.start()
        stage3.append(copy)
    for copy in stage3:
        copy.wait_recv()
    piece = t3[h, zl]
    for at in range(1, 8):
        piece = piece + r3[at]
    fin[x, zl] = piece.astype(BF16)

    agz = [
        send(fin.at[x, zl], fin.at[x, zl], SLOT["agz"] + d, {"dp_0": ring4(zl, d)})
        for d in (1, 3, 2)
    ]
    for copy in agz:
        copy.start()
    for copy in agz:
        copy.wait_recv()
    agx = [send(fin.at[x], fin.at[x], SLOT["agx"] + d, to_x(d)) for d in (1, 3, 2)]
    for copy in agx:
        copy.start()

    for copy in lsends2:
        copy.wait_recv()
    total = ldp[0]
    for i in range(1, 16):
        total = total + ldp[i]
    loss_o[...] = (total / (2.0 * KV * count))[0:1, 0:1]

    for copy in agx:
        copy.wait_recv()
    ordered = []
    for side in range(2):
        for xx in range(4):
            ordered += [fin[xx, 2 * side + l].astype(F32) for l in range(2)]
    kt[...] = jnp.transpose(jnp.concatenate(ordered, axis=0))
    osend = send(
        kt.at[pl.ds(pl.multiple_of((1 - c) * SL, 64), SL)], outs.at[:, my_cols],
        SLOT["out"], sib,
    )
    osend.start()
    own_out = pltpu.make_async_copy(
        kt.at[pl.ds(pl.multiple_of(c * SL, 64), SL)], outs.at[:, my_cols], lsem.at[3]
    )
    own_out.start()
    own_out.wait()
    osend.wait_recv()
    key_out = pltpu.make_async_copy(outs, key_o, lsem.at[4])
    key_out.start()
    terms = outs[...] * w[...].astype(F32)
    summed = lax.dot_general(
        jnp.ones((8, KV), F32), terms, (((1,), (1,)), ((), ())),
        preferred_element_type=F32, precision=lax.Precision.HIGHEST,
    )
    gain_o[...] = summed[0:1, :] / gain[...]
    key_out.wait()

    for copy in (
        [sib_w, sib_info, sib_tea, sib_hid, lsend, osend] + first + second + gsend + csend
        + sum(handed.values(), []) + stage1 + lsends + stage2 + lsends2 + stage3 + agz + agx
    ):
        copy.wait_send()

    @pl.when(edge)
    def _():
        for i in range(3):
            z_over(i).wait_send()
            z_in(i).wait_send()


def body(hidden_in, teacher, norm_gain, w_key, group_rows, member):
    core = lax.axis_index("shard_2")
    gain = norm_gain.astype(F32)
    row = lax.broadcasted_iota(jnp.int32, (8, PC), 0)
    lane = lax.broadcasted_iota(jnp.int32, (8, PC), 1)
    own = (row == 0) & (lane >= core * SL) & (lane < core * SL + SL)
    live = (member[0, 0] * group_rows[0]).astype(F32)
    info = jnp.where(own, jnp.concatenate([gain, gain])[None, :], jnp.where(row == 1, live, 0.0))
    vm = pl.BlockSpec(memory_space=pltpu.VMEM)
    hbm = pl.BlockSpec(memory_space=pl.ANY)
    loss, grad_gain, grad_key = pl.pallas_call(
        kernel,
        out_shape=(
            jax.ShapeDtypeStruct((1, 1), F32),
            jax.ShapeDtypeStruct((1, SL), F32),
            jax.ShapeDtypeStruct((SL, KV), F32),
        ),
        in_specs=[hbm, vm, vm, vm, vm],
        out_specs=(vm, vm, hbm),
        scratch_shapes=[
            pltpu.VMEM((2, TOK, D), BF16),
            pltpu.VMEM((2, TOK, HK), BF16),
            pltpu.VMEM((4, YB, HK), BF16),
            pltpu.VMEM((2 * TOK, D), BF16),
            pltpu.VMEM((2, TOK, 128), F32),
            pltpu.VMEM((2 * TOK, HK), F32),
            pltpu.VMEM((HK, 2 * TOK), BF16),
            pltpu.VMEM((4, HK, YB), BF16),
            pltpu.VMEM((3, QK, YB), BF16),
            pltpu.VMEM((3, 4, XK, YB), BF16),
            pltpu.VMEM((QK, YB), F32),
            pltpu.VMEM((4, XK, YB), F32),
            pltpu.VMEM((3, XK, YB), F32),
            pltpu.VMEM((3, XK, YB), F32),
            pltpu.VMEM((2, 4, 24, PC), F32),
            pltpu.VMEM((8, 24, PC), F32),
            pltpu.VMEM((4, 4, 24, PC), BF16),
            pltpu.VMEM((PC, HK), F32),
            pltpu.VMEM((SL, KV), F32),
            pltpu.VMEM((8, PC), F32),
            pltpu.VMEM((8, 8, PC), F32),
            pltpu.VMEM((16, 8, 128), F32),
            pltpu.VMEM((8, 128), F32),
            pltpu.VMEM((8, 128), F32),
            pltpu.VMEM((8, 8, 128), F32),
            pltpu.VMEM((16, 8, 128), F32),
            pltpu.SemaphoreType.DMA((5,)),
            pltpu.SemaphoreType.DMA((N_SLOT,)),
            pltpu.SemaphoreType.DMA((N_SLOT,)),
            pltpu.SemaphoreType.DMA((3,)),
        ],
        compiler_params=pltpu.CompilerParams(
            collective_id=0, has_side_effects=True, vmem_limit_bytes=62 * 2**20
        ),
    )(hidden_in, teacher, w_key, gain[None, :], info)
    return loss.reshape(()), grad_gain.reshape(SL), grad_key


def solution(mesh):
    split = Mesh(mesh.devices.reshape(4, 4, 2, 4, 2), DP_SHARD)
    return jax.shard_map(
        body,
        mesh=split,
        in_specs=(
            P(DP_SHARD, None),
            P(DP_SHARD, None),
            P(SHARD),
            P(SHARD, None),
            P(DP),
            P(DP, SHARD),
        ),
        out_specs=(P(), P(SHARD), P(SHARD, None)),
        check_vma=False,
    )
```

```python
import jax
import jax.numpy as jnp
from jax import lax
from jax.experimental import pallas as pl
from jax.experimental.pallas import tpu as pltpu
from jax.sharding import Mesh
from jax.sharding import PartitionSpec as P

SHARD = ("shard_0", "shard_1", "shard_2")
DP_SHARD = ("dp_0", "dp_1", "shard_0", "shard_1", "shard_2")
DP = ("dp_0", "dp_1")
MESH = pl.DeviceIdType.MESH
F32, BF16 = jnp.float32, jnp.bfloat16

EPSILON = 1e-06
SCALE = 1024.0

TOK = 256
D = 5120
KV = 768
HK = KV // 2
SL = 320
PC = 2 * SL
YB = 2 * PC
QK = HK // 2
CH = 3
CK = QK // CH
XK = CK // 4
ZK = XK // 2

DR = 160
SR = 80
SA = 48

SMALL = ("info", "w", "tea", "hid", "lsib", "out")


def slots(*groups):
    place, at = {}, 0
    for name, count in groups:
        place[name] = at
        at += count
    return place, at


SLOT, N_SLOT = slots(
    *((name, 1) for name in SMALL),
    ("ginfo", 8), ("lsh", 8), ("cnt", 16), ("ldp", 16),
    ("wy", 20), ("wx", 32), ("wz", 3), ("ry", 4 * CH), ("rx", 4 * (CH + 3)), ("s2y", 4 * CH), ("s2x", 4 * CH),
    ("s3", 8 * CH), ("agz", 4 * CH), ("agx", 4 * CH),
)


def kernel(
    hid, tea, w, gain, rows_of, alive, loss_o, gain_o, key_o,
    hbuf, tbuf, wbuf, nbuf, inv, keys, dkt, gup, glow, ry, rx, s2y, sx, r2y, r2x, t3, r3,
    fin, kt, outs, info, isib, gfull, cbuf, lown, lsib, lsh, ldp,
    lsem, ssem, rsem, zsem,
):
    zl, x = lax.axis_index("dp_0"), lax.axis_index("dp_1")
    h, y, c = (lax.axis_index(a) for a in SHARD)

    def ring4(v, d):
        return lax.rem(v + d, 4)

    def to_y(d):
        return {"shard_1": ring4(y, d)}

    def to_x(d):
        return {"dp_1": ring4(x, d)}

    sib = {"shard_2": 1 - c}

    def send(src, dst, slot, dev):
        return pltpu.make_async_remote_copy(
            src_ref=src, dst_ref=dst, send_sem=ssem.at[slot], recv_sem=rsem.at[slot],
            device_id=dev, device_id_type=MESH,
        )

    shard_peers = [
        (dh * 4 + dy, {"shard_0": lax.rem(h + dh, 2), "shard_1": ring4(y, dy)})
        for dh in range(2) for dy in range(4) if dh or dy
    ]
    dp_peers = [
        (dl * 4 + dx, {"dp_0": ring4(zl, dl), "dp_1": ring4(x, dx)})
        for dl in range(4) for dx in range(4) if dl or dx
    ]
    z_peers = [
        (dh * 4 + dl, {"shard_0": lax.rem(h + dh, 2), "dp_0": ring4(zl, dl)})
        for dh in range(2) for dl in range(4) if dh or dl
    ]
    extra = [dev for at, dev in z_peers if at > 4]
    everyone = [sib] + [dev for _, dev in shard_peers + dp_peers] + extra

    own_rows = pl.ds(pl.multiple_of(h * PC + c * SL, 64), SL)
    my_cols = pl.ds(pl.multiple_of(c * HK, 128), HK)
    sib_cols = pl.ds(pl.multiple_of((1 - c) * HK, 128), HK)
    mine = y * 2 + h
    gid = zl * 4 + x

    own_hid = pltpu.make_async_copy(hid, hbuf.at[c], lsem.at[0])
    own_hid.start()
    own_w = pltpu.make_async_copy(w.at[:, my_cols], wbuf.at[y, own_rows], lsem.at[1])
    own_w.start()
    own_tea = pltpu.make_async_copy(tea.at[:, my_cols], tbuf.at[c], lsem.at[2])
    own_tea.start()

    own_gain = gain[...].astype(F32).reshape(1, SL)
    lane = lax.broadcasted_iota(jnp.int32, (1, PC), 1)
    own = (lane >= c * SL) & (lane < c * SL + SL)
    info[:, 0:PC] = jnp.where(own, jnp.concatenate([own_gain, own_gain], axis=1), 0.0)
    info[:, PC:] = jnp.full((1, 128), (alive[0, 0] * rows_of[0]).astype(F32))

    barrier = pltpu.get_barrier_semaphore()
    for dev in everyone:
        pl.semaphore_signal(barrier, inc=1, device_id=dev, device_id_type=MESH)
    pl.semaphore_wait(barrier, len(everyone))

    sib_w = send(w.at[:, sib_cols], wbuf.at[y, own_rows], SLOT["w"], sib)
    sib_w.start()
    sib_info = send(info, isib, SLOT["info"], sib)
    sib_info.start()
    sib_tea = send(tea.at[:, sib_cols], tbuf.at[c], SLOT["tea"], sib)
    sib_tea.start()
    sib_hid = send(hid, hbuf.at[c], SLOT["hid"], sib)
    sib_hid.start()

    edge = (zl == 0) | (zl == 3)
    over = {"shard_0": 1 - h, "dp_0": 3 - zl}
    inner = {"dp_0": jnp.where(zl == 0, 1, 2)}
    split = PC // 2 + SR * x

    def part(owner, half, at, n):
        return wbuf.at[owner, pl.ds(pl.multiple_of(half * PC + at, 16), n)]

    z_parts = ((split, SR), (0, DR), (DR, DR))

    def z_over(i):
        ref = part(y, h, *z_parts[i])
        return send(ref, ref, SLOT["wz"] + i, over)

    def z_in(i):
        ref = part(y, 1 - h, *z_parts[i])
        return pltpu.make_async_remote_copy(
            src_ref=ref, dst_ref=ref, send_sem=zsem.at[i], recv_sem=rsem.at[SLOT["wz"] + i],
            device_id=inner, device_id_type=MESH,
        )

    def z_take(i):
        z_in(i).wait_recv()

        @pl.when(edge)
        def _():
            z_in(i).start()

    def y_copies(g):
        half = h if g == 0 else 1 - h
        back, ahead = ring4(y, 3), ring4(y, 1)
        plan = (
            (y, split, SR, 1), (y, split, SR, 3),
            (y, 0, DR, 1), (y, DR, DR, 3), (y, DR, DR, 1), (y, 0, DR, 3),
            (back, split, SA, 1), (ahead, split + SA, SR - SA, 3),
            (back, 0, DR, 1), (ahead, DR, DR, 3),
        )
        copies = []
        for i, (owner, at, n, d) in enumerate(plan):
            ref = part(owner, half, at, n)
            copies.append(send(ref, ref, SLOT["wy"] + 10 * g + i, to_y(d)))
        return copies

    first, second = y_copies(0), y_copies(1)
    handed = {}

    def hand(g, k):
        ref = part(ring4(y, k), h if g == 0 else 1 - h, split, SR)
        handed[g, k] = [
            send(ref, ref, SLOT["wx"] + 16 * g + 4 * k + i, to_x(i)) for i in (1, 3, 2)
        ]
        for copy in handed[g, k]:
            copy.start()

    def take(*copies):
        for copy in copies:
            copy.wait_recv()

    def go(*copies):
        for copy in copies:
            copy.start()

    sib_info.wait_recv()
    gfull[mine] = info[...] + isib[...]
    gsend = [
        send(gfull.at[mine], gfull.at[mine], SLOT["ginfo"] + at, dev) for at, dev in shard_peers
    ]
    go(*gsend)
    own_w.wait()
    sib_w.wait_recv()
    go(first[0], first[1])

    @pl.when(edge)
    def _():
        z_over(0).start()

    go(first[2], first[3])

    @pl.when(edge)
    def _():
        z_over(1).start()
        z_over(2).start()

    def norms(which):
        @pl.loop(0, TOK // 32)
        def _(i):
            rows = pl.ds(pl.multiple_of(i * 32, 32), 32)
            v = hbuf[which, rows, :].astype(F32)
            mean = jnp.sum(v * v, axis=1, keepdims=True) * (1.0 / D)
            inv[which, rows, :] = jnp.broadcast_to(lax.rsqrt(mean + EPSILON), (32, 128))

    def normalize(yy, hh):
        src = (hh * 4 + yy) * PC
        dst = (yy * 2 + hh) * PC
        for which in range(2):
            @pl.loop(0, TOK // 64)
            def _(i):
                rows = pl.ds(pl.multiple_of(i * 64, 64), 64)
                out = pl.ds(pl.multiple_of(which * TOK + i * 64, 64), 64)
                scale = inv[which, rows, :]
                for lane in range(0, PC, 128):
                    by = gfull[yy * 2 + hh, :, lane : lane + 128]
                    v = hbuf[which, rows, src + lane : src + lane + 128].astype(F32)
                    nbuf[out, dst + lane : dst + lane + 128] = (v * scale * by).astype(BF16)

    def project(k, g, start=False):
        half = h if g == 0 else 1 - h
        owner = ring4(y, k)
        cols = pl.ds(pl.multiple_of(owner * YB + half * PC, 128), PC)
        rows = pl.ds(pl.multiple_of(half * PC, 64), PC)
        term = jnp.dot(nbuf[:, cols], wbuf[owner, rows, :], preferred_element_type=F32)
        keys[...] = term if start else keys[...] + term

    own_hid.wait()
    norms(c)
    take(first[0], first[1])
    go(first[6], first[7])
    hand(0, 3)
    hand(0, 1)
    go(first[4], first[5])
    z_take(0)
    go(second[0], second[1])
    hand(1, 0)
    take(*gsend)
    group = gfull[0, :, PC:]
    for i in range(1, 8):
        group = group + gfull[i, :, PC:]
    cbuf[gid] = group
    csend = [send(cbuf.at[gid], cbuf.at[gid], SLOT["cnt"] + at, dev) for at, dev in dp_peers]
    go(*csend)
    sib_hid.wait_recv()
    norms(1 - c)
    take(first[2], first[3])
    go(first[8], first[9])
    z_take(1)
    go(second[2], second[5])
    normalize(0, 0)
    take(second[0], second[1])
    go(second[6], second[7])
    hand(1, 3)
    hand(1, 1)
    normalize(0, 1)
    take(first[6], first[7])
    hand(0, 2)
    normalize(1, 0)
    z_take(2)
    go(second[3], second[4])
    normalize(1, 1)
    normalize(2, 0)
    take(second[2])
    go(second[8])
    take(second[6], second[7])
    hand(1, 2)
    normalize(2, 1)
    normalize(3, 0)
    normalize(3, 1)
    take(second[3])
    go(second[9])
    project(0, 0, True)
    take(*handed[0, 3], *handed[0, 1], first[4], first[5])
    project(3, 0)
    project(1, 0)
    take(*handed[1, 0])
    project(0, 1)
    take(*handed[0, 2], first[8], first[9])
    project(2, 0)
    take(*csend)
    take(*handed[1, 3], *handed[1, 1], second[4], second[5])
    project(3, 1)
    project(1, 1)
    take(*handed[1, 2], second[8], second[9])
    project(2, 1)

    count = cbuf[0]
    for i in range(1, 16):
        count = count + cbuf[i]
    count = count[:, 0:1]
    scale = SCALE / count
    sib_tea.wait_recv()
    own_tea.wait()
    own_n = info[:, PC : PC + 1]
    sib_n = isib[:, PC : PC + 1]
    position = lax.broadcasted_iota(jnp.int32, (TOK, 1), 0).astype(F32)
    squares = jnp.zeros((1, HK), F32)
    for which in range(2):
        live = jnp.where(c == which, own_n, sib_n)
        valid = jnp.where(position < live, 1.0, 0.0)
        rows = slice(which * TOK, (which + 1) * TOK)
        diff = keys[rows, :] - tbuf[which].astype(F32)
        squares = squares + jnp.sum(valid * diff * diff, axis=0, keepdims=True)
        dk = scale * valid * diff
        dkt[:, rows] = jnp.transpose(dk).astype(BF16)
    lown[...] = jnp.broadcast_to(jnp.sum(squares, axis=1, keepdims=True), (1, 128))
    lsend = send(lown, lsib, SLOT["lsib"], sib)
    lsend.start()

    def up_copy(i, j):
        rows = pl.ds(CK * i, CK)
        return send(
            gup.at[ring4(y, j), rows], ry.at[j - 1, rows], SLOT["ry"] + CH * j + i, to_y(j)
        )

    def low_rows(i, xx):
        return pl.ds(pl.multiple_of(CK * i + XK * xx, 16), XK)

    stage1 = [[] for _ in range(CH)]
    for j in (1, 3, 2, 0):
        yy = ring4(y, j)
        cols = pl.ds(pl.multiple_of(yy * YB, 128), YB)
        term = jnp.dot(dkt[...], nbuf[:, cols], preferred_element_type=F32)
        gup[yy] = term[:QK].astype(BF16)
        glow[:, cols] = term[QK:].astype(BF16)
        if j:
            stage1[0].append(up_copy(0, j))
            stage1[0][-1].start()
        for d in (1, 3, 2):
            copy = send(
                glow.at[low_rows(0, ring4(x, d)), cols], rx.at[d - 1, 0, :, cols],
                SLOT["rx"] + 4 * j + d, to_x(d),
            )
            copy.start()
            stage1[0].append(copy)
    for i in range(1, CH):
        for d in (1, 3, 2):
            stage1[i].append(up_copy(i, d))
            stage1[i].append(send(
                glow.at[low_rows(i, ring4(x, d))], rx.at[d - 1, i],
                SLOT["rx"] + 4 * (3 + i) + d, to_x(d),
            ))
        go(*stage1[i])

    take(lsend)
    lsh[mine] = lown[...] + lsib[...]
    lsends = [send(lsh.at[mine], lsh.at[mine], SLOT["lsh"] + at, dev) for at, dev in shard_peers]
    go(*lsends)

    stage2 = [[] for _ in range(CH)]
    stage3 = [[] for _ in range(CH)]
    agz = [[] for _ in range(CH)]
    agx = [[] for _ in range(CH)]

    def reduce1(i):
        take(*stage1[i])
        rows = slice(CK * i, CK * i + CK)
        s2y[rows] = (
            gup[y, rows].astype(F32) + ry[0, rows].astype(F32)
            + ry[1, rows].astype(F32) + ry[2, rows].astype(F32)
        )
        for d in (1, 3, 2):
            stage2[i].append(
                send(s2y.at[low_rows(i, ring4(x, d))], r2y.at[i, d - 1],
                     SLOT["s2y"] + CH * d + i, to_x(d))
            )
            stage2[i][-1].start()
        for j in (1, 3, 2, 0):
            yy = ring4(y, j)
            cols = pl.ds(pl.multiple_of(yy * YB, 128), YB)
            sx[i, yy] = (
                glow[low_rows(i, x), cols].astype(F32) + rx[0, i, :, cols].astype(F32)
                + rx[1, i, :, cols].astype(F32) + rx[2, i, :, cols].astype(F32)
            )
            if j:
                stage2[i].append(
                    send(sx.at[i, yy], r2x.at[i, j - 1], SLOT["s2x"] + CH * j + i, to_y(j))
                )
                stage2[i][-1].start()

    def reduce2(i):
        take(*stage2[i])
        upper = s2y[low_rows(i, x), :] + r2y[i, 0] + r2y[i, 1] + r2y[i, 2]
        lower = sx[i, y] + r2x[i, 0] + r2x[i, 1] + r2x[i, 2]
        for hh in range(2):
            for l in range(4):
                both = upper if l < 2 else lower
                at = ZK * (l % 2)
                t3[i, hh, l] = both[at : at + ZK, hh * PC : (hh + 1) * PC]
        for at, dev in z_peers:
            copy = send(
                t3.at[i, lax.rem(h + at // 4, 2), ring4(zl, at % 4)], r3.at[i, at],
                SLOT["s3"] + 8 * i + at, dev,
            )
            copy.start()
            stage3[i].append(copy)

    def reduce3(i):
        take(*stage3[i])
        piece = t3[i, h, zl]
        for at in range(1, 8):
            piece = piece + r3[i, at]
        fin[i, x, zl] = piece.astype(BF16)
        for d in (1, 3, 2):
            agz[i].append(
                send(fin.at[i, x, zl], fin.at[i, x, zl], SLOT["agz"] + 4 * i + d,
                     {"dp_0": ring4(zl, d)})
            )
        go(*agz[i])

    def gather(i):
        take(*agz[i])
        for d in (1, 3, 2):
            agx[i].append(send(fin.at[i, x], fin.at[i, x], SLOT["agx"] + 4 * i + d, to_x(d)))
        go(*agx[i])

    reduce1(0)
    reduce1(1)
    reduce1(2)
    take(*lsends)
    total = lsh[0]
    for i in range(1, 8):
        total = total + lsh[i]
    ldp[gid] = total
    lsends2 = [send(ldp.at[gid], ldp.at[gid], SLOT["ldp"] + at, dev) for at, dev in dp_peers]
    go(*lsends2)
    reduce2(0)
    reduce2(1)
    reduce3(0)
    reduce2(2)
    gather(0)
    reduce3(1)
    gather(1)
    reduce3(2)
    take(*lsends2)
    total = ldp[0]
    for i in range(1, 16):
        total = total + ldp[i]
    loss_o[...] = (total / (2.0 * KV * count))[:, 0:1]
    gather(2)
    for i in range(CH):
        take(*agx[i])
    ordered = [
        fin[i, xx, 2 * side + l].astype(F32)
        for side in range(2) for i in range(CH) for xx in range(4) for l in range(2)
    ]
    kt[...] = jnp.transpose(jnp.concatenate(ordered, axis=0)).astype(BF16)
    osend = send(
        kt.at[pl.ds(pl.multiple_of((1 - c) * SL, 64), SL)], outs.at[:, my_cols],
        SLOT["out"], sib,
    )
    osend.start()
    own_out = pltpu.make_async_copy(
        kt.at[pl.ds(pl.multiple_of(c * SL, 64), SL)], outs.at[:, my_cols], lsem.at[3]
    )
    own_out.start()
    own_out.wait()
    osend.wait_recv()
    key_out = pltpu.make_async_copy(outs, key_o, lsem.at[4])
    key_out.start()
    terms = outs[...].astype(F32) * w[...].astype(F32)
    summed = lax.dot_general(
        jnp.ones((8, KV), F32), terms, (((1,), (1,)), ((), ())),
        preferred_element_type=F32, precision=lax.Precision.HIGHEST,
    )
    gain_o[...] = (summed[0:1, :] / own_gain).reshape(SL)
    key_out.wait()

    for copy in (
        [sib_w, sib_info, sib_tea, sib_hid, lsend, osend] + first + second + gsend + csend
        + sum(handed.values(), []) + lsends + lsends2
        + sum(stage1 + stage2 + stage3 + agz + agx, [])
    ):
        copy.wait_send()

    @pl.when(edge)
    def _():
        for i in range(3):
            z_over(i).wait_send()
            z_in(i).wait_send()


def body(hidden_in, teacher, norm_gain, w_key, group_rows, member):
    vm = pl.BlockSpec(memory_space=pltpu.VMEM)
    hbm = pl.BlockSpec(memory_space=pl.ANY)
    sm = pl.BlockSpec(memory_space=pltpu.SMEM)
    loss, grad_gain, grad_key = pl.pallas_call(
        kernel,
        out_shape=(
            jax.ShapeDtypeStruct((1, 1), F32),
            jax.ShapeDtypeStruct((SL,), F32),
            jax.ShapeDtypeStruct((SL, KV), BF16),
        ),
        in_specs=[hbm, vm, vm, vm, sm, sm],
        out_specs=(vm, vm, hbm),
        scratch_shapes=[
            pltpu.VMEM((2, TOK, D), BF16),
            pltpu.VMEM((2, TOK, HK), BF16),
            pltpu.VMEM((4, YB, HK), BF16),
            pltpu.VMEM((2 * TOK, D), BF16),
            pltpu.VMEM((2, TOK, 128), F32),
            pltpu.VMEM((2 * TOK, HK), F32),
            pltpu.VMEM((HK, 2 * TOK), BF16),
            pltpu.VMEM((4, QK, YB), BF16),
            pltpu.VMEM((QK, 4 * YB), BF16),
            pltpu.VMEM((3, QK, YB), BF16),
            pltpu.VMEM((3, CH, XK, 4 * YB), BF16),
            pltpu.VMEM((QK, YB), F32),
            pltpu.VMEM((CH, 4, XK, YB), F32),
            pltpu.VMEM((CH, 3, XK, YB), F32),
            pltpu.VMEM((CH, 3, XK, YB), F32),
            pltpu.VMEM((CH, 2, 4, ZK, PC), F32),
            pltpu.VMEM((CH, 8, ZK, PC), F32),
            pltpu.VMEM((CH, 4, 4, ZK, PC), BF16),
            pltpu.VMEM((PC, HK), BF16),
            pltpu.VMEM((SL, KV), BF16),
            pltpu.VMEM((1, PC + 128), F32),
            pltpu.VMEM((1, PC + 128), F32),
            pltpu.VMEM((8, 1, PC + 128), F32),
            pltpu.VMEM((16, 1, 128), F32),
            pltpu.VMEM((1, 128), F32),
            pltpu.VMEM((1, 128), F32),
            pltpu.VMEM((8, 1, 128), F32),
            pltpu.VMEM((16, 1, 128), F32),
            pltpu.SemaphoreType.DMA((5,)),
            pltpu.SemaphoreType.DMA((N_SLOT,)),
            pltpu.SemaphoreType.DMA((N_SLOT,)),
            pltpu.SemaphoreType.DMA((3,)),
        ],
        compiler_params=pltpu.CompilerParams(
            collective_id=0, has_side_effects=True, vmem_limit_bytes=62 * 2**20
        ),
    )(hidden_in, teacher, w_key, norm_gain, group_rows, member)
    return loss.reshape(()), grad_gain, grad_key.astype(F32)


def solution(mesh):
    split = Mesh(mesh.devices.reshape(4, 4, 2, 4, 2), DP_SHARD)
    return jax.shard_map(
        body,
        mesh=split,
        in_specs=(
            P(DP_SHARD, None),
            P(DP_SHARD, None),
            P(SHARD),
            P(SHARD, None),
            P(DP),
            P(DP, SHARD),
        ),
        out_specs=(P(), P(SHARD), P(SHARD, None)),
        check_vma=False,
    )
```

```python
import jax
import jax.numpy as jnp
from jax import lax
from jax.experimental import pallas as pl
from jax.experimental.pallas import tpu as pltpu
from jax.sharding import Mesh
from jax.sharding import PartitionSpec as P

SHARD = ("shard_0", "shard_1", "shard_2")
DP_SHARD = ("dp_0", "dp_1", "shard_0", "shard_1", "shard_2")
DP = ("dp_0", "dp_1")
MESH = pl.DeviceIdType.MESH
F32, BF16 = jnp.float32, jnp.bfloat16

EPSILON = 1e-06
SCALE = 1024.0

TOK = 256
D = 5120
KV = 768
HK = KV // 2
SL = 320
PC = 2 * SL
YB = 2 * PC
QK = HK // 2
CH = 3
CK = QK // CH
XK = CK // 4
ZK = XK // 2

HR = 80
DR = 2 * HR
SR = 80
SA = 48

def slots(*groups):
    place, at = {}, 0
    for name, count in groups:
        place[name] = at
        at += count
    return place, at


SLOT, N_SLOT = slots(
    *((name, 1) for name in ("info", "w", "tea", "hid", "lsib", "ginfo", "lsh", "cnt", "ldp")),
    ("wy", 12), ("wx", 8), ("wz", 3), ("qy", CH), ("qx", CH), ("ry", 2 * CH), ("rx", 2 * CH),
    ("s2y", CH), ("s2x", CH), ("s3", CH), ("agz", CH), ("agx", CH), ("out", CH),
)


def kernel(
    hid, tea, w, gain, rows_of, alive, loss_o, key_o,
    wv, hbuf, tbuf, wbuf, nbuf, inv, keys, dkt, gup, glow, qy, qx, ry, rx,
    s2y, sx, r2y, r2x, t3, r3, fin, kt, info, isib, gfull, cbuf, lown, lsib, lsh, ldp,
    lsem, ssem, rsem, zsem,
):
    zl, x = lax.axis_index("dp_0"), lax.axis_index("dp_1")
    h, y, c = (lax.axis_index(a) for a in SHARD)

    def ring4(v, d):
        return lax.rem(v + d, 4)

    def to_y(d):
        return {"shard_1": ring4(y, d)}

    def to_x(d):
        return {"dp_1": ring4(x, d)}

    sib = {"shard_2": 1 - c}

    def send(src, dst, slot, dev):
        return pltpu.make_async_remote_copy(
            src_ref=src, dst_ref=dst, send_sem=ssem.at[slot], recv_sem=rsem.at[slot],
            device_id=dev, device_id_type=MESH,
        )

    class Group:
        def __init__(self, slot, whole, parts):
            self.copies = [send(src, dst, slot, dev) for src, dst, dev in parts]
            self.whole = send(whole, whole, slot, sib)

        def start(self):
            for copy in self.copies:
                copy.start()

        def wait_recv(self):
            self.whole.wait_recv()

        def wait_send(self):
            self.whole.wait_send()

    shard_peers = [
        (dh * 4 + dy, {"shard_0": lax.rem(h + dh, 2), "shard_1": ring4(y, dy)})
        for dh in range(2) for dy in range(4) if dh or dy
    ]
    dp_peers = [
        (dl * 4 + dx, {"dp_0": ring4(zl, dl), "dp_1": ring4(x, dx)})
        for dl in range(4) for dx in range(4) if dl or dx
    ]
    z_peers = [
        (dh * 4 + dl, {"shard_0": lax.rem(h + dh, 2), "dp_0": ring4(zl, dl)})
        for dh in range(2) for dl in range(4) if dh or dl
    ]
    extra = [dev for at, dev in z_peers if at > 4]
    everyone = [sib] + [dev for _, dev in shard_peers + dp_peers] + extra

    own_rows = pl.ds(pl.multiple_of(h * PC + c * SL, 64), SL)
    my_cols = pl.ds(pl.multiple_of(c * HK, 128), HK)
    sib_cols = pl.ds(pl.multiple_of((1 - c) * HK, 128), HK)
    mine = y * 2 + h
    gid = zl * 4 + x

    own_hid = pltpu.make_async_copy(hid, hbuf.at[c], lsem.at[0])
    own_hid.start()
    own_w = pltpu.make_async_copy(w.at[:, my_cols], wbuf.at[y, own_rows], lsem.at[1])
    own_w.start()
    own_tea = pltpu.make_async_copy(tea.at[:, my_cols], tbuf.at[c], lsem.at[2])
    own_tea.start()
    stage_w = pltpu.make_async_copy(w, wv, lsem.at[3])
    stage_w.start()

    own_gain = gain[...].astype(F32).reshape(1, SL)
    lane = lax.broadcasted_iota(jnp.int32, (1, PC), 1)
    own = (lane >= c * SL) & (lane < c * SL + SL)
    info[:, 0:PC] = jnp.where(own, jnp.concatenate([own_gain, own_gain], axis=1), 0.0)
    live = (alive[...] * rows_of[...].reshape(1, 1)).astype(F32)
    info[:, PC:] = jnp.broadcast_to(live, (1, 128))

    barrier = pltpu.get_barrier_semaphore()
    for dev in everyone:
        pl.semaphore_signal(barrier, inc=1, device_id=dev, device_id_type=MESH)
    pl.semaphore_wait(barrier, len(everyone))

    stage_w.wait()
    sib_w = send(wv.at[:, sib_cols], wbuf.at[y, own_rows], SLOT["w"], sib)
    sib_w.start()
    sib_info = send(info, isib, SLOT["info"], sib)
    sib_info.start()
    sib_tea = send(tea.at[:, sib_cols], tbuf.at[c], SLOT["tea"], sib)
    sib_tea.start()
    sib_hid = send(hid, hbuf.at[c], SLOT["hid"], sib)
    sib_hid.start()

    edge = (zl == 0) | (zl == 3)
    over = {"shard_0": 1 - h, "dp_0": 3 - zl}
    inner = {"dp_0": jnp.where(zl == 0, 1, 2)}
    split = PC // 2 + SR * x

    def part(owner, half, at, n):
        return wbuf.at[owner, pl.ds(pl.multiple_of(half * PC + at, 16), n)]

    z_parts = ((split, SR), (0, DR), (DR, DR))

    def z_over(i):
        ref = part(y, h, *z_parts[i])
        return send(ref, ref, SLOT["wz"] + i, over)

    def z_in(i):
        ref = part(y, 1 - h, *z_parts[i])
        return pltpu.make_async_remote_copy(
            src_ref=ref, dst_ref=ref, send_sem=zsem.at[i], recv_sem=rsem.at[SLOT["wz"] + i],
            device_id=inner, device_id_type=MESH,
        )

    def z_relay(i):
        @pl.when(edge)
        def _():
            z_in(i).wait_recv()
            z_in(i).start()

    def z_take(i):
        @pl.when(jnp.logical_not(edge))
        def _():
            z_in(i).wait_recv()

    def y_copies(g):
        half = h if g == 0 else 1 - h
        back, ahead = ring4(y, 3), ring4(y, 1)
        plan = (
            (y, split, SR, 1), (y, split, SR, 3),
            (y, 0, DR, 1), (y, 0, DR, 3), (y, DR, DR, 1), (y, DR, DR, 3),
            (back, split, SA, 1), (ahead, split + SA, SR - SA, 3),
            (back, 0, HR, 1), (ahead, HR, HR, 3),
            (back, DR, HR, 1), (ahead, DR + HR, HR, 3),
        )
        groups = []
        for i in range(0, len(plan), 2):
            pair = [(part(owner, half, at, n), d) for owner, at, n, d in plan[i : i + 2]]
            total = sum(n for _, _, n, _ in plan[i : i + 2])
            groups.append(Group(
                SLOT["wy"] + 6 * g + i // 2, wbuf.at[0, pl.ds(0, total)],
                [(ref, ref, to_y(d)) for ref, d in pair],
            ))
        return groups

    first, second = y_copies(0), y_copies(1)
    handed = {}

    def hand(g, k):
        ref = part(ring4(y, k), h if g == 0 else 1 - h, split, SR)
        handed[g, k] = Group(
            SLOT["wx"] + 4 * g + k, wbuf.at[0, pl.ds(0, 3 * SR)],
            [(ref, ref, to_x(i)) for i in (1, 3, 2)],
        )
        handed[g, k].start()

    def take(*copies):
        for copy in copies:
            copy.wait_recv()

    def go(*copies):
        for copy in copies:
            copy.start()

    sib_info.wait_recv()
    gfull[mine] = info[...] + isib[...]
    gsend = Group(
        SLOT["ginfo"], gfull.at[pl.ds(0, 7)],
        [(gfull.at[mine], gfull.at[mine], dev) for _, dev in shard_peers],
    )
    gsend.start()
    own_w.wait()
    sib_w.wait_recv()
    go(first[0])

    @pl.when(edge)
    def _():
        z_over(0).start()

    go(first[1])

    @pl.when(edge)
    def _():
        z_over(1).start()
        z_over(2).start()

    def norms(which):
        @pl.loop(0, TOK // 32)
        def _(i):
            rows = pl.ds(pl.multiple_of(i * 32, 32), 32)
            v = hbuf[which, rows, :].astype(F32)
            mean = jnp.sum(v * v, axis=1, keepdims=True) * (1.0 / D)
            inv[which, rows, :] = jnp.broadcast_to(lax.rsqrt(mean + EPSILON), (32, 128))

    def normalize(yy, hh):
        src = (hh * 4 + yy) * PC
        dst = (yy * 2 + hh) * PC
        for which in range(2):
            @pl.loop(0, TOK // 64)
            def _(i):
                rows = pl.ds(pl.multiple_of(i * 64, 64), 64)
                out = pl.ds(pl.multiple_of(which * TOK + i * 64, 64), 64)
                scale = inv[which, rows, :]
                for lane in range(0, PC, 128):
                    by = gfull[yy * 2 + hh, :, lane : lane + 128]
                    v = hbuf[which, rows, src + lane : src + lane + 128].astype(F32)
                    nbuf[out, dst + lane : dst + lane + 128] = (v * scale * by).astype(BF16)

    def project(k, g, start=False):
        half = h if g == 0 else 1 - h
        owner = ring4(y, k)
        cols = pl.ds(pl.multiple_of(owner * YB + half * PC, 128), PC)
        rows = pl.ds(pl.multiple_of(half * PC, 64), PC)
        term = jnp.dot(nbuf[:, cols], wbuf[owner, rows, :], preferred_element_type=F32)
        keys[...] = term if start else keys[...] + term

    own_hid.wait()
    norms(c)
    take(first[0])
    go(first[3])
    hand(0, 3)
    hand(0, 1)
    go(first[2])
    z_relay(0)
    z_take(0)
    go(second[0])
    hand(1, 0)
    z_relay(1)
    take(gsend)
    group = gfull[0, :, PC:]
    for i in range(1, 8):
        group = group + gfull[i, :, PC:]
    cbuf[gid] = group
    csend = Group(
        SLOT["cnt"], cbuf.at[pl.ds(0, 15)],
        [(cbuf.at[gid], cbuf.at[gid], dev) for _, dev in dp_peers],
    )
    csend.start()
    sib_hid.wait_recv()
    norms(1 - c)
    z_relay(2)
    take(first[1])
    go(first[4])
    z_take(1)
    go(second[1])
    take(first[2])
    go(first[5])
    normalize(0, 0)
    take(second[0])
    go(second[3])
    hand(1, 3)
    hand(1, 1)
    normalize(0, 1)
    take(first[3])
    hand(0, 2)
    normalize(1, 0)
    z_take(2)
    go(second[2])
    normalize(1, 1)
    normalize(2, 0)
    take(second[1])
    go(second[4])
    take(second[3])
    hand(1, 2)
    normalize(2, 1)
    normalize(3, 0)
    normalize(3, 1)
    project(0, 0, True)
    take(second[2])
    go(second[5])
    take(handed[0, 3], handed[0, 1])
    project(3, 0)
    project(1, 0)
    take(handed[1, 0])
    project(0, 1)
    take(handed[0, 2], *first[4:])
    project(2, 0)
    take(csend)
    take(handed[1, 3], handed[1, 1])
    project(3, 1)
    project(1, 1)
    take(handed[1, 2], *second[4:])
    project(2, 1)

    count = cbuf[0]
    for i in range(1, 16):
        count = count + cbuf[i]
    count = count[:, 0:1]
    scale = SCALE / count
    sib_tea.wait_recv()
    own_tea.wait()
    own_n = info[:, PC : PC + 1]
    sib_n = isib[:, PC : PC + 1]
    position = lax.broadcasted_iota(jnp.int32, (TOK, 1), 0).astype(F32)
    squares = jnp.zeros((1, HK), F32)
    for which in range(2):
        live = jnp.where(c == which, own_n, sib_n)
        valid = jnp.where(position < live, 1.0, 0.0)
        rows = slice(which * TOK, (which + 1) * TOK)
        diff = keys[rows, :] - tbuf[which].astype(F32)
        squares = squares + jnp.sum(valid * diff * diff, axis=0, keepdims=True)
        dk = scale * valid * diff
        dkt[:, rows] = jnp.transpose(dk).astype(BF16)
    lown[...] = jnp.broadcast_to(jnp.sum(squares, axis=1, keepdims=True), (1, 128))
    lsend = send(lown, lsib, SLOT["lsib"], sib)
    lsend.start()

    def low_rows(i, xx):
        return pl.ds(pl.multiple_of(CK * i + XK * xx, 16), XK)

    def cols_of(j):
        return pl.ds(pl.multiple_of(ring4(y, j) * YB, 128), YB)

    relay = [[] for _ in range(CH)]
    stage1 = [[] for _ in range(CH)]
    for j in (2, 3, 1, 0):
        term = jnp.dot(dkt[...], nbuf[:, cols_of(j)], preferred_element_type=F32)
        gup[ring4(y, j)] = term[:QK].astype(BF16)
        glow[:, cols_of(j)] = term[QK:].astype(BF16)
        for i in range(CH):
            rows = pl.ds(CK * i, CK)
            if j == 2:
                relay[i].append(Group(
                    SLOT["qy"] + i, gup.at[0, rows],
                    [(gup.at[ring4(y, 2), rows, pl.ds(at * PC, PC)], qy.at[at, rows], to_y(d))
                     for at, d in enumerate((1, 3))],
                ))
                relay[i][0].start()
            at = 0 if j in (2, 1) else 1
            part_x = (
                glow.at[low_rows(i, ring4(x, 2)), cols_of(j)], qx.at[i, j], to_x(1 + 2 * at)
            )
            send(part_x[0], part_x[1], SLOT["qx"] + i, part_x[2]).start()
        for i in range(CH):
            rows = pl.ds(CK * i, CK)
            if j in (1, 3):
                at = 0 if j == 1 else 1
                lanes = pl.ds((1 - at) * PC, PC)
                send(
                    gup.at[ring4(y, j), rows, lanes], ry.at[at, rows, lanes],
                    SLOT["ry"] + i, to_y(j),
                ).start()
            at = 1 if j in (2, 1) else 0
            d = 1 + 2 * at
            send(
                glow.at[low_rows(i, ring4(x, d)), cols_of(j)], rx.at[at, i, :, cols_of(j)],
                SLOT["rx"] + i, to_x(d),
            ).start()
    for i in range(CH):
        rows = pl.ds(CK * i, CK)
        relay[i].append(Group(SLOT["qx"] + i, qx.at[i], []))
        stage1[i] += [
            Group(SLOT["ry"] + i, gup.at[0, rows], []),
            Group(SLOT["rx"] + i, rx.at[0, i], []),
        ]

    def combine(i):
        take(*relay[i])
        rows = slice(CK * i, CK * i + CK)
        late_y, late_x = [], []
        for at, d in enumerate((1, 3)):
            yy, lanes = ring4(y, d), slice(at * PC, (at + 1) * PC)
            both = gup[yy, rows, lanes].astype(F32) + qy[at, rows].astype(F32)
            gup[yy, rows, lanes] = both.astype(BF16)
            late_y.append((gup.at[yy, rows, lanes], ry.at[at, rows, lanes], to_y(d)))
        for at, d in enumerate((1, 3)):
            there = low_rows(i, ring4(x, d))
            for j in ((2, 1), (3, 0))[at]:
                both = glow[there, cols_of(j)].astype(F32) + qx[i, j].astype(F32)
                glow[there, cols_of(j)] = both.astype(BF16)
                late_x.append(
                    (glow.at[there, cols_of(j)], rx.at[at, i, :, cols_of(j)], to_x(d))
                )
        rows = pl.ds(CK * i, CK)
        stage1[i] += [
            Group(SLOT["ry"] + CH + i, gup.at[0, rows], late_y),
            Group(SLOT["rx"] + CH + i, rx.at[0, i], late_x),
        ]
        go(*stage1[i][2:])

    take(lsend)
    lsh[mine] = lown[...] + lsib[...]
    lsends = Group(
        SLOT["lsh"], lsh.at[pl.ds(0, 7)],
        [(lsh.at[mine], lsh.at[mine], dev) for _, dev in shard_peers],
    )
    lsends.start()

    stage2 = [[] for _ in range(CH)]
    stage3 = [[] for _ in range(CH)]
    agz = [[] for _ in range(CH)]
    agx = [[] for _ in range(CH)]

    def reduce1(i):
        take(*stage1[i])
        rows = slice(CK * i, CK * i + CK)
        s2y[rows] = (
            gup[y, rows].astype(F32) + ry[0, rows].astype(F32) + ry[1, rows].astype(F32)
        )
        stage2[i].append(Group(
            SLOT["s2y"] + i, r2y.at[i],
            [(s2y.at[low_rows(i, ring4(x, d))], r2y.at[i, d - 1], to_x(d)) for d in (1, 3, 2)],
        ))
        stage2[i][0].start()
        for j in (1, 3, 2, 0):
            yy = ring4(y, j)
            cols = pl.ds(pl.multiple_of(yy * YB, 128), YB)
            sx[i, yy] = (
                glow[low_rows(i, x), cols].astype(F32) + rx[0, i, :, cols].astype(F32)
                + rx[1, i, :, cols].astype(F32)
            )
            if j:
                send(sx.at[i, yy], r2x.at[i, j - 1], SLOT["s2x"] + i, to_y(j)).start()
        stage2[i].append(Group(SLOT["s2x"] + i, r2x.at[i], []))

    def reduce2(i):
        take(*stage2[i])
        upper = s2y[low_rows(i, x), :] + r2y[i, 0] + r2y[i, 1] + r2y[i, 2]
        lower = sx[i, y] + r2x[i, 0] + r2x[i, 1] + r2x[i, 2]
        for hh in range(2):
            for l in range(4):
                both = upper if l < 2 else lower
                at = ZK * (l % 2)
                t3[i, hh, l] = both[at : at + ZK, hh * PC : (hh + 1) * PC]
        stage3[i].append(Group(
            SLOT["s3"] + i, r3.at[i, pl.ds(1, 7)],
            [(t3.at[i, lax.rem(h + at // 4, 2), ring4(zl, at % 4)], r3.at[i, at], dev)
             for at, dev in z_peers],
        ))
        stage3[i][0].start()

    def reduce3(i):
        take(*stage3[i])
        piece = t3[i, h, zl]
        for at in range(1, 8):
            piece = piece + r3[i, at]
        fin[c, i, x, zl] = piece.astype(BF16)
        agz[i].append(Group(
            SLOT["agz"] + i, fin.at[c, i, x, pl.ds(0, 3)],
            [(fin.at[c, i, x, zl], fin.at[c, i, x, zl], {"dp_0": ring4(zl, d)})
             for d in (1, 3, 2)],
        ))
        agz[i][0].start()

    def gather(i):
        take(*agz[i])
        agx[i].append(Group(
            SLOT["agx"] + i, fin.at[c, i, pl.ds(0, 3)],
            [(fin.at[c, i, x], fin.at[c, i, x], to_x(d)) for d in (1, 3, 2)],
        ))
        agx[i][0].start()

    def share(i):
        take(*agx[i])
        osend.append(send(fin.at[c, i], fin.at[c, i], SLOT["out"] + i, sib))
        osend[i].start()

    def drain(copies):
        for copy in copies:
            copy.wait_send()

    osend = []
    combine(0)
    combine(1)
    combine(2)
    drain([sib_w, sib_info, sib_tea, sib_hid, gsend, csend] + first + second)
    drain(handed.values())

    @pl.when(edge)
    def _():
        for i in range(3):
            z_over(i).wait_send()
            z_in(i).wait_send()

    reduce1(0)
    reduce1(1)
    reduce1(2)
    drain([lsend] + sum(relay + stage1, []))
    take(lsends)
    total = lsh[0]
    for i in range(1, 8):
        total = total + lsh[i]
    ldp[gid] = total
    lsends2 = Group(
        SLOT["ldp"], ldp.at[pl.ds(0, 15)],
        [(ldp.at[gid], ldp.at[gid], dev) for _, dev in dp_peers],
    )
    lsends2.start()
    reduce2(0)
    reduce2(1)
    reduce3(0)
    reduce2(2)
    reduce3(1)
    drain([lsends] + sum(stage2, []))
    gather(0)
    reduce3(2)
    gather(1)
    take(lsends2)
    total = ldp[0]
    for i in range(1, 16):
        total = total + ldp[i]
    loss_o[...] = (total / (2.0 * KV * count))[:, 0:1]
    share(0)
    gather(2)
    share(1)
    drain([lsends2] + sum(stage3 + agz, []) + agx[0] + agx[1])
    share(2)
    take(*osend)
    ordered = [
        fin[half, i, xx, 2 * side + l].astype(F32)
        for half in range(2) for side in range(2) for i in range(CH)
        for xx in range(4) for l in range(2)
    ]
    kt[...] = jnp.transpose(jnp.concatenate(ordered, axis=0)).astype(BF16)
    key_out = pltpu.make_async_copy(
        kt.at[pl.ds(pl.multiple_of(c * SL, 64), SL)], key_o, lsem.at[4]
    )
    key_out.start()
    drain(agx[2] + osend)
    key_out.wait()


def finish(key, w, gain, loss, loss_o, gain_o, key_o):
    grad = key[...].astype(F32)
    key_o[...] = grad
    loss_o[...] = loss[...]
    summed = lax.dot_general(
        jnp.ones((8, KV), F32), grad * w[...].astype(F32), (((1,), (1,)), ((), ())),
        preferred_element_type=F32, precision=lax.Precision.HIGHEST,
    )
    gain_o[...] = (summed[0:1, :] / gain[...].astype(F32).reshape(1, SL)).reshape(SL)


def body(hidden_in, teacher, norm_gain, w_key, group_rows, member):
    vm = pl.BlockSpec(memory_space=pltpu.VMEM)
    hbm = pl.BlockSpec(memory_space=pl.ANY)
    loss, key = pl.pallas_call(
        kernel,
        out_shape=(
            jax.ShapeDtypeStruct((1, 1), F32),
            jax.ShapeDtypeStruct((SL, KV), BF16),
        ),
        in_specs=[hbm, hbm, hbm, vm, vm, vm],
        out_specs=(vm, hbm),
        scratch_shapes=[
            pltpu.VMEM((SL, KV), BF16),
            pltpu.VMEM((2, TOK, D), BF16),
            pltpu.VMEM((2, TOK, HK), BF16),
            pltpu.VMEM((4, YB, HK), BF16),
            pltpu.VMEM((2 * TOK, D), BF16),
            pltpu.VMEM((2, TOK, 128), F32),
            pltpu.VMEM((2 * TOK, HK), F32),
            pltpu.VMEM((HK, 2 * TOK), BF16),
            pltpu.VMEM((4, QK, YB), BF16),
            pltpu.VMEM((QK, 4 * YB), BF16),
            pltpu.VMEM((2, QK, PC), BF16),
            pltpu.VMEM((CH, 4, XK, YB), BF16),
            pltpu.VMEM((2, QK, YB), BF16),
            pltpu.VMEM((2, CH, XK, 4 * YB), BF16),
            pltpu.VMEM((QK, YB), F32),
            pltpu.VMEM((CH, 4, XK, YB), F32),
            pltpu.VMEM((CH, 3, XK, YB), F32),
            pltpu.VMEM((CH, 3, XK, YB), F32),
            pltpu.VMEM((CH, 2, 4, ZK, PC), F32),
            pltpu.VMEM((CH, 8, ZK, PC), F32),
            pltpu.VMEM((2, CH, 4, 4, ZK, PC), BF16),
            pltpu.VMEM((PC, KV), BF16),
            pltpu.VMEM((1, PC + 128), F32),
            pltpu.VMEM((1, PC + 128), F32),
            pltpu.VMEM((8, 1, PC + 128), F32),
            pltpu.VMEM((16, 1, 128), F32),
            pltpu.VMEM((1, 128), F32),
            pltpu.VMEM((1, 128), F32),
            pltpu.VMEM((8, 1, 128), F32),
            pltpu.VMEM((16, 1, 128), F32),
            pltpu.SemaphoreType.DMA((5,)),
            pltpu.SemaphoreType.DMA((N_SLOT,)),
            pltpu.SemaphoreType.DMA((N_SLOT,)),
            pltpu.SemaphoreType.DMA((3,)),
        ],
        compiler_params=pltpu.CompilerParams(
            collective_id=0, has_side_effects=True, vmem_limit_bytes=62 * 2**20
        ),
    )(hidden_in, teacher, w_key, norm_gain, group_rows, member)
    loss, grad_gain, grad_key = pl.pallas_call(
        finish,
        out_shape=(
            jax.ShapeDtypeStruct((1, 1), F32),
            jax.ShapeDtypeStruct((SL,), F32),
            jax.ShapeDtypeStruct((SL, KV), F32),
        ),
        in_specs=[vm] * 4,
        out_specs=(vm, vm, vm),
    )(key, w_key, norm_gain, loss)
    return loss.reshape(()), grad_gain, grad_key


def solution(mesh):
    split = Mesh(mesh.devices.reshape(4, 4, 2, 4, 2), DP_SHARD)
    return jax.shard_map(
        body,
        mesh=split,
        in_specs=(
            P(DP_SHARD, None),
            P(DP_SHARD, None),
            P(SHARD),
            P(SHARD, None),
            P(DP),
            P(DP, SHARD),
        ),
        out_specs=(P(), P(SHARD), P(SHARD, None)),
        check_vma=False,
    )
```

```python
import jax
import jax.numpy as jnp
from jax import lax
from jax.experimental import pallas as pl
from jax.experimental.pallas import tpu as pltpu
from jax.sharding import Mesh
from jax.sharding import PartitionSpec as P

SHARD = ("shard_0", "shard_1", "shard_2")
DP_SHARD = ("dp_0", "dp_1", "shard_0", "shard_1", "shard_2")
DP = ("dp_0", "dp_1")
MESH = pl.DeviceIdType.MESH
F32, BF16 = jnp.float32, jnp.bfloat16

EPSILON = 1e-06
SCALE = 1024.0

TOK = 256
D = 5120
KV = 768
HK = KV // 2
SL = 320
PC = 2 * SL
YB = 2 * PC
QK = HK // 2
CH = 3
CK = QK // CH
XK = CK // 4
ZK = XK // 2

HR = 80
DR = 2 * HR
SR = 80
SA = 48

def slots(*groups):
    place, at = {}, 0
    for name, count in groups:
        place[name] = at
        at += count
    return place, at


SLOT, N_SLOT = slots(
    *((name, 1) for name in ("info", "w", "tea", "hid", "lsib", "ginfo", "lsh", "cnt", "ldp")),
    ("wy", 12), ("wx", 8), ("wz", 3), ("qy", CH), ("qx", CH), ("ry", 2 * CH), ("rx", 2 * CH),
    ("s2y", CH), ("s2x", CH), ("s3", CH), ("agz", CH), ("agx", CH), ("out", CH),
)


def kernel(
    hid, tea, w, gain, rows_of, alive, loss_o, gain_o, key_o,
    wv, hbuf, tbuf, wbuf, nbuf, inv, keys, dkt, gup, glow, qy, qx, ry, rx,
    s2y, s2b, sx, sb, r2y, r2x, t3, t3b, r3, pown, prol, psib, fin, kt, info, isib, gfull, cbuf, lown, lsib, lsh, ldp,
    lsem, ssem, rsem, zsem,
):
    zl, x = lax.axis_index("dp_0"), lax.axis_index("dp_1")
    h, y, c = (lax.axis_index(a) for a in SHARD)

    def ring4(v, d):
        return lax.rem(v + d, 4)

    def to_y(d):
        return {"shard_1": ring4(y, d)}

    def to_x(d):
        return {"dp_1": ring4(x, d)}

    sib = {"shard_2": 1 - c}

    def send(src, dst, slot, dev):
        return pltpu.make_async_remote_copy(
            src_ref=src, dst_ref=dst, send_sem=ssem.at[slot], recv_sem=rsem.at[slot],
            device_id=dev, device_id_type=MESH,
        )

    class Group:
        def __init__(self, slot, whole, parts):
            self.copies = [send(src, dst, slot, dev) for src, dst, dev in parts]
            self.whole = send(whole, whole, slot, sib)

        def start(self):
            for copy in self.copies:
                copy.start()

        def wait_recv(self):
            self.whole.wait_recv()

        def wait_send(self):
            self.whole.wait_send()

    shard_peers = [
        (dh * 4 + dy, {"shard_0": lax.rem(h + dh, 2), "shard_1": ring4(y, dy)})
        for dh in range(2) for dy in range(4) if dh or dy
    ]
    dp_peers = [
        (dl * 4 + dx, {"dp_0": ring4(zl, dl), "dp_1": ring4(x, dx)})
        for dl in range(4) for dx in range(4) if dl or dx
    ]
    z_peers = [
        (dh * 4 + dl, {"shard_0": lax.rem(h + dh, 2), "dp_0": ring4(zl, dl)})
        for dh in range(2) for dl in range(4) if dh or dl
    ]
    extra = [dev for at, dev in z_peers if at > 4]
    everyone = [sib] + [dev for _, dev in shard_peers + dp_peers] + extra

    own_rows = pl.ds(pl.multiple_of(h * PC + c * SL, 64), SL)
    my_cols = pl.ds(pl.multiple_of(c * HK, 128), HK)
    sib_cols = pl.ds(pl.multiple_of((1 - c) * HK, 128), HK)
    mine = y * 2 + h
    gid = zl * 4 + x

    own_hid = pltpu.make_async_copy(hid, hbuf.at[c], lsem.at[0])
    own_hid.start()
    own_w = pltpu.make_async_copy(w.at[:, my_cols], wbuf.at[y, own_rows], lsem.at[1])
    own_w.start()
    own_tea = pltpu.make_async_copy(tea.at[:, my_cols], tbuf.at[c], lsem.at[2])
    own_tea.start()
    stage_w = pltpu.make_async_copy(w, wv, lsem.at[3])
    stage_w.start()

    own_gain = gain[...].astype(F32).reshape(1, SL)
    lane = lax.broadcasted_iota(jnp.int32, (1, PC), 1)
    own = (lane >= c * SL) & (lane < c * SL + SL)
    info[:, 0:PC] = jnp.where(own, jnp.concatenate([own_gain, own_gain], axis=1), 0.0)
    live = (alive[...] * rows_of[...].reshape(1, 1)).astype(F32)
    info[:, PC:] = jnp.broadcast_to(live, (1, 128))

    barrier = pltpu.get_barrier_semaphore()
    for dev in everyone:
        pl.semaphore_signal(barrier, inc=1, device_id=dev, device_id_type=MESH)
    pl.semaphore_wait(barrier, len(everyone))

    stage_w.wait()
    sib_w = send(wv.at[:, sib_cols], wbuf.at[y, own_rows], SLOT["w"], sib)
    sib_w.start()
    sib_info = send(info, isib, SLOT["info"], sib)
    sib_info.start()
    sib_tea = send(tea.at[:, sib_cols], tbuf.at[c], SLOT["tea"], sib)
    sib_tea.start()
    sib_hid = send(hid, hbuf.at[c], SLOT["hid"], sib)
    sib_hid.start()

    edge = (zl == 0) | (zl == 3)
    over = {"shard_0": 1 - h, "dp_0": 3 - zl}
    inner = {"dp_0": jnp.where(zl == 0, 1, 2)}
    split = PC // 2 + SR * x

    def part(owner, half, at, n):
        return wbuf.at[owner, pl.ds(pl.multiple_of(half * PC + at, 16), n)]

    z_parts = ((split, SR), (0, DR), (DR, DR))

    def z_over(i):
        ref = part(y, h, *z_parts[i])
        return send(ref, ref, SLOT["wz"] + i, over)

    def z_in(i):
        ref = part(y, 1 - h, *z_parts[i])
        return pltpu.make_async_remote_copy(
            src_ref=ref, dst_ref=ref, send_sem=zsem.at[i], recv_sem=rsem.at[SLOT["wz"] + i],
            device_id=inner, device_id_type=MESH,
        )

    def z_relay(i):
        @pl.when(edge)
        def _():
            z_in(i).wait_recv()
            z_in(i).start()

    def z_take(i):
        @pl.when(jnp.logical_not(edge))
        def _():
            z_in(i).wait_recv()

    def y_copies(g):
        half = h if g == 0 else 1 - h
        back, ahead = ring4(y, 3), ring4(y, 1)
        plan = (
            (y, split, SR, 1), (y, split, SR, 3),
            (y, 0, DR, 1), (y, 0, DR, 3), (y, DR, DR, 1), (y, DR, DR, 3),
            (back, split, SA, 1), (ahead, split + SA, SR - SA, 3),
            (back, 0, HR, 1), (ahead, HR, HR, 3),
            (back, DR, HR, 1), (ahead, DR + HR, HR, 3),
        )
        groups = []
        for i in range(0, len(plan), 2):
            pair = [(part(owner, half, at, n), d) for owner, at, n, d in plan[i : i + 2]]
            total = sum(n for _, _, n, _ in plan[i : i + 2])
            groups.append(Group(
                SLOT["wy"] + 6 * g + i // 2, wbuf.at[0, pl.ds(0, total)],
                [(ref, ref, to_y(d)) for ref, d in pair],
            ))
        return groups

    first, second = y_copies(0), y_copies(1)
    handed = {}

    def hand(g, k):
        ref = part(ring4(y, k), h if g == 0 else 1 - h, split, SR)
        handed[g, k] = Group(
            SLOT["wx"] + 4 * g + k, wbuf.at[0, pl.ds(0, 3 * SR)],
            [(ref, ref, to_x(i)) for i in (1, 3, 2)],
        )
        handed[g, k].start()

    def take(*copies):
        for copy in copies:
            copy.wait_recv()

    def go(*copies):
        for copy in copies:
            copy.start()

    sib_info.wait_recv()
    gfull[mine] = info[...] + isib[...]
    gsend = Group(
        SLOT["ginfo"], gfull.at[pl.ds(0, 7)],
        [(gfull.at[mine], gfull.at[mine], dev) for _, dev in shard_peers],
    )
    gsend.start()
    own_w.wait()
    sib_w.wait_recv()
    go(first[0])

    @pl.when(edge)
    def _():
        z_over(0).start()

    go(first[1])

    @pl.when(edge)
    def _():
        z_over(1).start()
        z_over(2).start()

    def norms(which):
        @pl.loop(0, TOK // 32)
        def _(i):
            rows = pl.ds(pl.multiple_of(i * 32, 32), 32)
            v = hbuf[which, rows, :].astype(F32)
            mean = jnp.sum(v * v, axis=1, keepdims=True) * (1.0 / D)
            inv[which, rows, :] = jnp.broadcast_to(lax.rsqrt(mean + EPSILON), (32, 128))

    def normalize(yy, hh):
        src = (hh * 4 + yy) * PC
        dst = (yy * 2 + hh) * PC
        for which in range(2):
            @pl.loop(0, TOK // 64)
            def _(i):
                rows = pl.ds(pl.multiple_of(i * 64, 64), 64)
                out = pl.ds(pl.multiple_of(which * TOK + i * 64, 64), 64)
                scale = inv[which, rows, :]
                for lane in range(0, PC, 128):
                    by = gfull[yy * 2 + hh, :, lane : lane + 128]
                    v = hbuf[which, rows, src + lane : src + lane + 128].astype(F32)
                    nbuf[out, dst + lane : dst + lane + 128] = (v * scale * by).astype(BF16)

    def project(k, g, start=False):
        half = h if g == 0 else 1 - h
        owner = ring4(y, k)
        cols = pl.ds(pl.multiple_of(owner * YB + half * PC, 128), PC)
        rows = pl.ds(pl.multiple_of(half * PC, 64), PC)
        term = jnp.dot(nbuf[:, cols], wbuf[owner, rows, :], preferred_element_type=F32)
        keys[...] = term if start else keys[...] + term

    own_hid.wait()
    norms(c)
    take(first[0])
    go(first[3])
    hand(0, 3)
    hand(0, 1)
    go(first[2])
    z_relay(0)
    z_take(0)
    go(second[0])
    hand(1, 0)
    z_relay(1)
    take(gsend)
    group = gfull[0, :, PC:]
    for i in range(1, 8):
        group = group + gfull[i, :, PC:]
    cbuf[gid] = group
    csend = Group(
        SLOT["cnt"], cbuf.at[pl.ds(0, 15)],
        [(cbuf.at[gid], cbuf.at[gid], dev) for _, dev in dp_peers],
    )
    csend.start()
    sib_hid.wait_recv()
    norms(1 - c)
    z_relay(2)
    take(first[1])
    go(first[4])
    z_take(1)
    go(second[1])
    take(first[2])
    go(first[5])
    normalize(0, 0)
    take(second[0])
    go(second[3])
    hand(1, 3)
    hand(1, 1)
    normalize(0, 1)
    take(first[3])
    hand(0, 2)
    normalize(1, 0)
    z_take(2)
    go(second[2])
    normalize(1, 1)
    normalize(2, 0)
    take(second[1])
    go(second[4])
    take(second[3])
    hand(1, 2)
    normalize(2, 1)
    normalize(3, 0)
    normalize(3, 1)
    project(0, 0, True)
    take(second[2])
    go(second[5])
    take(handed[0, 3], handed[0, 1])
    project(3, 0)
    project(1, 0)
    take(handed[1, 0])
    project(0, 1)
    take(handed[0, 2], *first[4:])
    project(2, 0)
    take(csend)
    take(handed[1, 3], handed[1, 1])
    project(3, 1)
    project(1, 1)
    take(handed[1, 2], *second[4:])
    project(2, 1)

    count = cbuf[0]
    for i in range(1, 16):
        count = count + cbuf[i]
    count = count[:, 0:1]
    scale = SCALE / count
    sib_tea.wait_recv()
    own_tea.wait()
    own_n = info[:, PC : PC + 1]
    sib_n = isib[:, PC : PC + 1]
    position = lax.broadcasted_iota(jnp.int32, (TOK, 1), 0).astype(F32)
    squares = jnp.zeros((1, HK), F32)
    for which in range(2):
        live = jnp.where(c == which, own_n, sib_n)
        valid = jnp.where(position < live, 1.0, 0.0)
        rows = slice(which * TOK, (which + 1) * TOK)
        diff = keys[rows, :] - tbuf[which].astype(F32)
        squares = squares + jnp.sum(valid * diff * diff, axis=0, keepdims=True)
        dk = scale * valid * diff
        dkt[:, rows] = jnp.transpose(dk).astype(BF16)
    lown[...] = jnp.broadcast_to(jnp.sum(squares, axis=1, keepdims=True), (1, 128))
    lsend = send(lown, lsib, SLOT["lsib"], sib)
    lsend.start()

    def low_rows(i, xx):
        return pl.ds(pl.multiple_of(CK * i + XK * xx, 16), XK)

    def cols_of(j):
        return pl.ds(pl.multiple_of(ring4(y, j) * YB, 128), YB)

    relay = [[] for _ in range(CH)]
    stage1 = [[] for _ in range(CH)]
    for j in (2, 3, 1, 0):
        term = jnp.dot(dkt[...], nbuf[:, cols_of(j)], preferred_element_type=F32)
        gup[ring4(y, j)] = term[:QK].astype(BF16)
        glow[:, cols_of(j)] = term[QK:].astype(BF16)
        for i in range(CH):
            rows = pl.ds(CK * i, CK)
            if j == 2:
                relay[i].append(Group(
                    SLOT["qy"] + i, gup.at[0, rows],
                    [(gup.at[ring4(y, 2), rows, pl.ds(at * PC, PC)], qy.at[at, rows], to_y(d))
                     for at, d in enumerate((1, 3))],
                ))
                relay[i][0].start()
            at = 0 if j in (2, 1) else 1
            part_x = (
                glow.at[low_rows(i, ring4(x, 2)), cols_of(j)], qx.at[i, j], to_x(1 + 2 * at)
            )
            send(part_x[0], part_x[1], SLOT["qx"] + i, part_x[2]).start()
        for i in range(CH):
            rows = pl.ds(CK * i, CK)
            if j in (1, 3):
                at = 0 if j == 1 else 1
                lanes = pl.ds((1 - at) * PC, PC)
                send(
                    gup.at[ring4(y, j), rows, lanes], ry.at[at, rows, lanes],
                    SLOT["ry"] + i, to_y(j),
                ).start()
            at = 1 if j in (2, 1) else 0
            d = 1 + 2 * at
            send(
                glow.at[low_rows(i, ring4(x, d)), cols_of(j)], rx.at[at, i, :, cols_of(j)],
                SLOT["rx"] + i, to_x(d),
            ).start()
    for i in range(CH):
        rows = pl.ds(CK * i, CK)
        relay[i].append(Group(SLOT["qx"] + i, qx.at[i], []))
        stage1[i] += [
            Group(SLOT["ry"] + i, gup.at[0, rows], []),
            Group(SLOT["rx"] + i, rx.at[0, i], []),
        ]

    def combine(i):
        take(*relay[i])
        rows = slice(CK * i, CK * i + CK)
        late_y, late_x = [], []
        for at, d in enumerate((1, 3)):
            yy, lanes = ring4(y, d), slice(at * PC, (at + 1) * PC)
            both = gup[yy, rows, lanes].astype(F32) + qy[at, rows].astype(F32)
            gup[yy, rows, lanes] = both.astype(BF16)
            late_y.append((gup.at[yy, rows, lanes], ry.at[at, rows, lanes], to_y(d)))
        for at, d in enumerate((1, 3)):
            there = low_rows(i, ring4(x, d))
            for j in ((2, 1), (3, 0))[at]:
                both = glow[there, cols_of(j)].astype(F32) + qx[i, j].astype(F32)
                glow[there, cols_of(j)] = both.astype(BF16)
                late_x.append(
                    (glow.at[there, cols_of(j)], rx.at[at, i, :, cols_of(j)], to_x(d))
                )
        rows = pl.ds(CK * i, CK)
        stage1[i] += [
            Group(SLOT["ry"] + CH + i, gup.at[0, rows], late_y),
            Group(SLOT["rx"] + CH + i, rx.at[0, i], late_x),
        ]
        go(*stage1[i][2:])

    take(lsend)
    lsh[mine] = lown[...] + lsib[...]
    lsends = Group(
        SLOT["lsh"], lsh.at[pl.ds(0, 7)],
        [(lsh.at[mine], lsh.at[mine], dev) for _, dev in shard_peers],
    )
    lsends.start()

    stage2 = [[] for _ in range(CH)]
    stage3 = [[] for _ in range(CH)]
    agz = [[] for _ in range(CH)]
    agx = [[] for _ in range(CH)]

    def reduce1(i):
        take(*stage1[i])
        rows = slice(CK * i, CK * i + CK)
        total = (
            gup[y, rows].astype(F32) + ry[0, rows].astype(F32) + ry[1, rows].astype(F32)
        )
        s2y[rows] = total
        s2b[rows] = total.astype(BF16)
        stage2[i].append(Group(
            SLOT["s2y"] + i, r2y.at[i],
            [(s2b.at[low_rows(i, ring4(x, d))], r2y.at[i, d - 1], to_x(d)) for d in (1, 3, 2)],
        ))
        stage2[i][0].start()
        for j in (1, 3, 2, 0):
            cols = cols_of(j)
            total = (
                glow[low_rows(i, x), cols].astype(F32) + rx[0, i, :, cols].astype(F32)
                + rx[1, i, :, cols].astype(F32)
            )
            if j:
                sb[i, j - 1] = total.astype(BF16)
                send(sb.at[i, j - 1], r2x.at[i, j - 1], SLOT["s2x"] + i, to_y(j)).start()
            else:
                sx[i] = total
        stage2[i].append(Group(SLOT["s2x"] + i, r2x.at[i], []))

    def reduce2(i):
        take(*stage2[i])
        upper = s2y[low_rows(i, x), :]
        lower = sx[i]
        for d in range(3):
            upper = upper + r2y[i, d].astype(F32)
            lower = lower + r2x[i, d].astype(F32)
        for hh in range(2):
            for l in range(4):
                both = upper if l < 2 else lower
                at = ZK * (l % 2)
                block = both[at : at + ZK, hh * PC : (hh + 1) * PC]
                t3[i, hh, l] = block
                t3b[i, hh, l] = block.astype(BF16)
        stage3[i].append(Group(
            SLOT["s3"] + i, r3.at[i, pl.ds(1, 7)],
            [(t3b.at[i, lax.rem(h + at // 4, 2), ring4(zl, at % 4)], r3.at[i, at], dev)
             for at, dev in z_peers],
        ))
        stage3[i][0].start()

    def reduce3(i):
        take(*stage3[i])
        piece = t3[i, h, zl]
        for at in range(1, 8):
            piece = piece + r3[i, at].astype(F32)
        pown[i] = piece
        prol[i] = jnp.concatenate([piece[:, SL:], piece[:, :SL]], axis=1)
        swaps.append(send(prol.at[i], psib.at[i], SLOT["out"] + i, sib))
        swaps[i].start()

    def scatter(i):
        take(swaps[i])
        fin[i, x, zl] = jnp.where(own, pown[i], psib[i])
        agz[i].append(Group(
            SLOT["agz"] + i, fin.at[i, x, pl.ds(0, 3)],
            [(fin.at[i, x, zl], fin.at[i, x, zl], {"dp_0": ring4(zl, d)}) for d in (1, 3, 2)],
        ))
        agz[i][0].start()

    def gather(i):
        take(*agz[i])
        agx[i].append(Group(
            SLOT["agx"] + i, fin.at[i, pl.ds(0, 3)],
            [(fin.at[i, x], fin.at[i, x], to_x(d)) for d in (1, 3, 2)],
        ))
        agx[i][0].start()

    def drain(copies):
        for copy in copies:
            copy.wait_send()

    swaps = []
    combine(0)
    combine(1)
    combine(2)
    drain([sib_w, sib_info, sib_tea, sib_hid, gsend, csend] + first + second)
    drain(handed.values())

    @pl.when(edge)
    def _():
        for i in range(3):
            z_over(i).wait_send()
            z_in(i).wait_send()

    reduce1(0)
    reduce1(1)
    reduce1(2)
    drain([lsend] + sum(relay + stage1, []))
    take(lsends)
    total = lsh[0]
    for i in range(1, 8):
        total = total + lsh[i]
    ldp[gid] = total
    lsends2 = Group(
        SLOT["ldp"], ldp.at[pl.ds(0, 15)],
        [(ldp.at[gid], ldp.at[gid], dev) for _, dev in dp_peers],
    )
    lsends2.start()
    reduce2(0)
    reduce2(1)
    reduce3(0)
    reduce2(2)
    scatter(0)
    reduce3(1)
    drain([lsends] + sum(stage2, []))
    scatter(1)
    gather(0)
    reduce3(2)
    scatter(2)
    gather(1)
    take(lsends2)
    total = ldp[0]
    for i in range(1, 16):
        total = total + ldp[i]
    loss_o[...] = (total / (2.0 * KV * count))[:, 0:1]
    drain([lsends2] + sum(stage3, []) + swaps)
    gather(2)
    drain(agz[0] + agz[1] + agx[0])
    for i in range(CH):
        take(*agx[i])
    ordered = [
        fin[i, xx, 2 * side + l]
        for side in range(2) for i in range(CH) for xx in range(4) for l in range(2)
    ]
    kt[...] = jnp.transpose(jnp.concatenate(ordered, axis=0))
    outs = [
        pltpu.make_async_copy(
            kt.at[pl.ds(half * SL, SL)], key_o.at[:, pl.ds(half * HK, HK)], lsem.at[4 + half]
        )
        for half in range(2)
    ]
    go(*outs)
    terms = (
        kt[:SL, :] * wv[:, :HK].astype(F32) + kt[SL:, :] * wv[:, HK:].astype(F32)
    )
    summed = lax.dot_general(
        jnp.ones((8, HK), F32), terms, (((1,), (1,)), ((), ())),
        preferred_element_type=F32, precision=lax.Precision.HIGHEST,
    )
    gain_o[...] = summed[0:1, :] / own_gain
    drain(agz[2] + agx[1] + agx[2])
    for copy in outs:
        copy.wait()


def finish(key, gain, loss, loss_o, gain_o, key_o):
    key_o[...] = key[...]

    @pl.when(pl.program_id(0) == 0)
    def _():
        loss_o[...] = loss[...]
        gain_o[...] = gain[...].reshape(SL)


def body(hidden_in, teacher, norm_gain, w_key, group_rows, member):
    vm = pl.BlockSpec(memory_space=pltpu.VMEM)
    hbm = pl.BlockSpec(memory_space=pl.ANY)
    loss, gain, key = pl.pallas_call(
        kernel,
        out_shape=(
            jax.ShapeDtypeStruct((1, 1), F32),
            jax.ShapeDtypeStruct((1, SL), F32),
            jax.ShapeDtypeStruct((SL, KV), F32),
        ),
        in_specs=[hbm, hbm, hbm, vm, vm, vm],
        out_specs=(vm, vm, hbm),
        scratch_shapes=[
            pltpu.VMEM((SL, KV), BF16),
            pltpu.VMEM((2, TOK, D), BF16),
            pltpu.VMEM((2, TOK, HK), BF16),
            pltpu.VMEM((4, YB, HK), BF16),
            pltpu.VMEM((2 * TOK, D), BF16),
            pltpu.VMEM((2, TOK, 128), F32),
            pltpu.VMEM((2 * TOK, HK), F32),
            pltpu.VMEM((HK, 2 * TOK), BF16),
            pltpu.VMEM((4, QK, YB), BF16),
            pltpu.VMEM((QK, 4 * YB), BF16),
            pltpu.VMEM((2, QK, PC), BF16),
            pltpu.VMEM((CH, 4, XK, YB), BF16),
            pltpu.VMEM((2, QK, YB), BF16),
            pltpu.VMEM((2, CH, XK, 4 * YB), BF16),
            pltpu.VMEM((QK, YB), F32),
            pltpu.VMEM((QK, YB), BF16),
            pltpu.VMEM((CH, XK, YB), F32),
            pltpu.VMEM((CH, 3, XK, YB), BF16),
            pltpu.VMEM((CH, 3, XK, YB), BF16),
            pltpu.VMEM((CH, 3, XK, YB), BF16),
            pltpu.VMEM((CH, 2, 4, ZK, PC), F32),
            pltpu.VMEM((CH, 2, 4, ZK, PC), BF16),
            pltpu.VMEM((CH, 8, ZK, PC), BF16),
            pltpu.VMEM((CH, ZK, PC), F32),
            pltpu.VMEM((CH, ZK, PC), F32),
            pltpu.VMEM((CH, ZK, PC), F32),
            pltpu.VMEM((CH, 4, 4, ZK, PC), F32),
            pltpu.VMEM((PC, HK), F32),
            pltpu.VMEM((1, PC + 128), F32),
            pltpu.VMEM((1, PC + 128), F32),
            pltpu.VMEM((8, 1, PC + 128), F32),
            pltpu.VMEM((16, 1, 128), F32),
            pltpu.VMEM((1, 128), F32),
            pltpu.VMEM((1, 128), F32),
            pltpu.VMEM((8, 1, 128), F32),
            pltpu.VMEM((16, 1, 128), F32),
            pltpu.SemaphoreType.DMA((6,)),
            pltpu.SemaphoreType.DMA((N_SLOT,)),
            pltpu.SemaphoreType.DMA((N_SLOT,)),
            pltpu.SemaphoreType.DMA((3,)),
        ],
        compiler_params=pltpu.CompilerParams(
            collective_id=0, has_side_effects=True, vmem_limit_bytes=62 * 2**20
        ),
    )(hidden_in, teacher, w_key, norm_gain, group_rows, member)
    loss, grad_gain, grad_key = pl.pallas_call(
        finish,
        out_shape=(
            jax.ShapeDtypeStruct((1, 1), F32),
            jax.ShapeDtypeStruct((SL,), F32),
            jax.ShapeDtypeStruct((SL, KV), F32),
        ),
        grid=(4,),
        in_specs=[
            pl.BlockSpec((SL // 4, KV), lambda i: (i, 0)),
            pl.BlockSpec((1, SL), lambda i: (0, 0)),
            pl.BlockSpec((1, 1), lambda i: (0, 0)),
        ],
        out_specs=(
            pl.BlockSpec((1, 1), lambda i: (0, 0)),
            pl.BlockSpec((SL,), lambda i: (0,)),
            pl.BlockSpec((SL // 4, KV), lambda i: (i, 0)),
        ),
    )(key, gain, loss)
    return loss.reshape(()), grad_gain, grad_key


def solution(mesh):
    split = Mesh(mesh.devices.reshape(4, 4, 2, 4, 2), DP_SHARD)
    return jax.shard_map(
        body,
        mesh=split,
        in_specs=(
            P(DP_SHARD, None),
            P(DP_SHARD, None),
            P(SHARD),
            P(SHARD, None),
            P(DP),
            P(DP, SHARD),
        ),
        out_specs=(P(), P(SHARD), P(SHARD, None)),
        check_vma=False,
    )
```

```python
import jax
import jax.numpy as jnp
from jax import lax
from jax.experimental import pallas as pl
from jax.experimental.pallas import tpu as pltpu
from jax.sharding import Mesh
from jax.sharding import PartitionSpec as P

SHARD = ("shard_0", "shard_1", "shard_2")
DP_SHARD = ("dp_0", "dp_1", "shard_0", "shard_1", "shard_2")
DP = ("dp_0", "dp_1")
MESH = pl.DeviceIdType.MESH
F32, BF16 = jnp.float32, jnp.bfloat16

EPSILON = 1e-06
SCALE = 1024.0

TOK = 256
D = 5120
KV = 768
HK = KV // 2
SL = 320
PC = 2 * SL
YB = 2 * PC
QK = HK // 2
CH = 3
CK = QK // CH
XK = CK // 4
ZK = XK // 2

HR = 80
DR = 2 * HR
SR = 80
SA = 48

def slots(*groups):
    place, at = {}, 0
    for name, count in groups:
        place[name] = at
        at += count
    return place, at


SLOT, N_SLOT = slots(
    *((name, 1) for name in ("info", "w", "tea", "hid", "lsib", "ginfo", "lsh", "cnt", "ldp")),
    ("wy", 12), ("wx", 8), ("wz", 3), ("qy", CH), ("qx", CH), ("ry", 2 * CH), ("rx", 2 * CH),
    ("s2y", CH), ("s2x", CH), ("s3", CH), ("agz", CH), ("agx", CH), ("agf", CH), ("out", CH),
)


def kernel(
    hid, tea, w, gain, rows_of, alive, loss_o, gain_o, key_o,
    wv, hbuf, tbuf, wbuf, nbuf, inv, keys, dkt, gup, glow, qy, qx, ry, rx,
    s2y, s2b, sx, sb, r2y, r2x, t3, t3b, r3, pown, prol, psib, fin, kt, info, isib, gfull, cbuf, lown, lsib, lsh, ldp,
    lsem, ssem, rsem, zsem,
):
    zl, x = lax.axis_index("dp_0"), lax.axis_index("dp_1")
    h, y, c = (lax.axis_index(a) for a in SHARD)

    def ring4(v, d):
        return lax.rem(v + d, 4)

    def to_y(d):
        return {"shard_1": ring4(y, d)}

    def to_x(d):
        return {"dp_1": ring4(x, d)}

    sib = {"shard_2": 1 - c}

    def send(src, dst, slot, dev):
        return pltpu.make_async_remote_copy(
            src_ref=src, dst_ref=dst, send_sem=ssem.at[slot], recv_sem=rsem.at[slot],
            device_id=dev, device_id_type=MESH,
        )

    class Group:
        def __init__(self, slot, whole, parts):
            self.copies = [send(src, dst, slot, dev) for src, dst, dev in parts]
            self.whole = send(whole, whole, slot, sib)

        def start(self):
            for copy in self.copies:
                copy.start()

        def wait_recv(self):
            self.whole.wait_recv()

        def wait_send(self):
            self.whole.wait_send()

    shard_peers = [
        (dh * 4 + dy, {"shard_0": lax.rem(h + dh, 2), "shard_1": ring4(y, dy)})
        for dh in range(2) for dy in range(4) if dh or dy
    ]
    dp_peers = [
        (dl * 4 + dx, {"dp_0": ring4(zl, dl), "dp_1": ring4(x, dx)})
        for dl in range(4) for dx in range(4) if dl or dx
    ]
    z_peers = [
        (dh * 4 + dl, {"shard_0": lax.rem(h + dh, 2), "dp_0": ring4(zl, dl)})
        for dh in range(2) for dl in range(4) if dh or dl
    ]
    extra = [dev for at, dev in z_peers if at > 4]
    everyone = [sib] + [dev for _, dev in shard_peers + dp_peers] + extra

    own_rows = pl.ds(pl.multiple_of(h * PC + c * SL, 64), SL)
    my_cols = pl.ds(pl.multiple_of(c * HK, 128), HK)
    sib_cols = pl.ds(pl.multiple_of((1 - c) * HK, 128), HK)
    mine = y * 2 + h
    gid = zl * 4 + x

    stage_w = pltpu.make_async_copy(w, wv, lsem.at[3])
    stage_w.start()
    barrier = pltpu.get_barrier_semaphore()
    for dev in everyone:
        pl.semaphore_signal(barrier, inc=1, device_id=dev, device_id_type=MESH)

    own_hid = pltpu.make_async_copy(hid, hbuf.at[c], lsem.at[0])
    own_hid.start()
    own_w = pltpu.make_async_copy(w.at[:, my_cols], wbuf.at[y, own_rows], lsem.at[1])
    own_w.start()
    own_tea = pltpu.make_async_copy(tea.at[:, my_cols], tbuf.at[c], lsem.at[2])
    own_tea.start()

    own_gain = gain[...].astype(F32).reshape(1, SL)
    lane = lax.broadcasted_iota(jnp.int32, (1, PC), 1)
    own = (lane >= c * SL) & (lane < c * SL + SL)
    info[:, 0:PC] = jnp.where(own, jnp.concatenate([own_gain, own_gain], axis=1), 0.0)
    live = (alive[...] * rows_of[...].reshape(1, 1)).astype(F32)
    info[:, PC:] = jnp.broadcast_to(live, (1, 128))

    pl.semaphore_wait(barrier, len(everyone))

    stage_w.wait()
    sib_w = send(wv.at[:, sib_cols], wbuf.at[y, own_rows], SLOT["w"], sib)
    sib_w.start()
    sib_info = send(info, isib, SLOT["info"], sib)
    sib_info.start()
    sib_tea = send(tea.at[:, sib_cols], tbuf.at[c], SLOT["tea"], sib)
    sib_tea.start()
    sib_hid = send(hid, hbuf.at[c], SLOT["hid"], sib)
    sib_hid.start()

    edge = (zl == 0) | (zl == 3)
    over = {"shard_0": 1 - h, "dp_0": 3 - zl}
    inner = {"dp_0": jnp.where(zl == 0, 1, 2)}
    split = PC // 2 + SR * x

    def part(owner, half, at, n):
        return wbuf.at[owner, pl.ds(pl.multiple_of(half * PC + at, 16), n)]

    z_parts = ((split, SR), (0, DR), (DR, DR))

    def z_over(i):
        ref = part(y, h, *z_parts[i])
        return send(ref, ref, SLOT["wz"] + i, over)

    def z_in(i):
        ref = part(y, 1 - h, *z_parts[i])
        return pltpu.make_async_remote_copy(
            src_ref=ref, dst_ref=ref, send_sem=zsem.at[i], recv_sem=rsem.at[SLOT["wz"] + i],
            device_id=inner, device_id_type=MESH,
        )

    def z_relay(i):
        @pl.when(edge)
        def _():
            z_in(i).wait_recv()
            z_in(i).start()

    def z_take(i):
        @pl.when(jnp.logical_not(edge))
        def _():
            z_in(i).wait_recv()

    def y_copies(g):
        half = h if g == 0 else 1 - h
        back, ahead = ring4(y, 3), ring4(y, 1)
        plan = (
            (y, split, SR, 1), (y, split, SR, 3),
            (y, 0, DR, 1), (y, 0, DR, 3), (y, DR, DR, 1), (y, DR, DR, 3),
            (back, split, SA, 1), (ahead, split + SA, SR - SA, 3),
            (back, 0, HR, 1), (ahead, HR, HR, 3),
            (back, DR, HR, 1), (ahead, DR + HR, HR, 3),
        )
        groups = []
        for i in range(0, len(plan), 2):
            pair = [(part(owner, half, at, n), d) for owner, at, n, d in plan[i : i + 2]]
            total = sum(n for _, _, n, _ in plan[i : i + 2])
            groups.append(Group(
                SLOT["wy"] + 6 * g + i // 2, wbuf.at[0, pl.ds(0, total)],
                [(ref, ref, to_y(d)) for ref, d in pair],
            ))
        return groups

    first, second = y_copies(0), y_copies(1)
    handed = {}

    def hand(g, k):
        ref = part(ring4(y, k), h if g == 0 else 1 - h, split, SR)
        handed[g, k] = Group(
            SLOT["wx"] + 4 * g + k, wbuf.at[0, pl.ds(0, 3 * SR)],
            [(ref, ref, to_x(i)) for i in (1, 3, 2)],
        )
        handed[g, k].start()

    def take(*copies):
        for copy in copies:
            copy.wait_recv()

    def go(*copies):
        for copy in copies:
            copy.start()

    sib_info.wait_recv()
    gfull[mine] = info[...] + isib[...]
    gsend = Group(
        SLOT["ginfo"], gfull.at[pl.ds(0, 7)],
        [(gfull.at[mine], gfull.at[mine], dev) for _, dev in shard_peers],
    )
    gsend.start()
    own_w.wait()
    sib_w.wait_recv()
    go(first[0])

    @pl.when(edge)
    def _():
        z_over(0).start()

    go(first[1])

    @pl.when(edge)
    def _():
        z_over(1).start()
        z_over(2).start()

    def norms(which):
        @pl.loop(0, TOK // 32)
        def _(i):
            rows = pl.ds(pl.multiple_of(i * 32, 32), 32)
            v = hbuf[which, rows, :].astype(F32)
            mean = jnp.sum(v * v, axis=1, keepdims=True) * (1.0 / D)
            inv[which, rows, :] = jnp.broadcast_to(lax.rsqrt(mean + EPSILON), (32, 128))

    def normalize(yy, hh):
        src = (hh * 4 + yy) * PC
        dst = (yy * 2 + hh) * PC
        for which in range(2):
            @pl.loop(0, TOK // 64)
            def _(i):
                rows = pl.ds(pl.multiple_of(i * 64, 64), 64)
                out = pl.ds(pl.multiple_of(which * TOK + i * 64, 64), 64)
                scale = inv[which, rows, :]
                for lane in range(0, PC, 128):
                    by = gfull[yy * 2 + hh, :, lane : lane + 128]
                    v = hbuf[which, rows, src + lane : src + lane + 128].astype(F32)
                    nbuf[out, dst + lane : dst + lane + 128] = (v * scale * by).astype(BF16)

    def project(k, g, start=False):
        half = h if g == 0 else 1 - h
        owner = ring4(y, k)
        cols = pl.ds(pl.multiple_of(owner * YB + half * PC, 128), PC)
        rows = pl.ds(pl.multiple_of(half * PC, 64), PC)
        term = jnp.dot(nbuf[:, cols], wbuf[owner, rows, :], preferred_element_type=F32)
        keys[...] = term if start else keys[...] + term

    own_hid.wait()
    norms(c)
    take(first[0])
    go(first[3])
    hand(0, 3)
    hand(0, 1)
    go(first[2])
    z_relay(0)
    z_take(0)
    go(second[0])
    hand(1, 0)
    z_relay(1)
    take(gsend)
    group = gfull[0, :, PC:]
    for i in range(1, 8):
        group = group + gfull[i, :, PC:]
    cbuf[gid] = group
    csend = Group(
        SLOT["cnt"], cbuf.at[pl.ds(0, 15)],
        [(cbuf.at[gid], cbuf.at[gid], dev) for _, dev in dp_peers],
    )
    csend.start()
    sib_hid.wait_recv()
    norms(1 - c)
    z_relay(2)
    take(first[1])
    go(first[4])
    z_take(1)
    go(second[1])
    take(first[2])
    go(first[5])
    normalize(0, 0)
    take(second[0])
    go(second[3])
    hand(1, 3)
    hand(1, 1)
    normalize(0, 1)
    take(first[3])
    hand(0, 2)
    normalize(1, 0)
    z_take(2)
    go(second[2])
    normalize(1, 1)
    normalize(2, 0)
    take(second[1])
    go(second[4])
    take(second[3])
    hand(1, 2)
    normalize(2, 1)
    normalize(3, 0)
    normalize(3, 1)
    project(0, 0, True)
    take(second[2])
    go(second[5])
    take(handed[0, 3], handed[0, 1])
    project(3, 0)
    project(1, 0)
    take(handed[1, 0])
    project(0, 1)
    take(handed[0, 2], *first[4:])
    project(2, 0)
    take(csend)
    take(handed[1, 3], handed[1, 1])
    project(3, 1)
    project(1, 1)
    take(handed[1, 2], *second[4:])
    project(2, 1)

    count = cbuf[0]
    for i in range(1, 16):
        count = count + cbuf[i]
    count = count[:, 0:1]
    scale = SCALE / count
    sib_tea.wait_recv()
    own_tea.wait()
    own_n = info[:, PC : PC + 1]
    sib_n = isib[:, PC : PC + 1]
    position = lax.broadcasted_iota(jnp.int32, (TOK, 1), 0).astype(F32)
    for which in range(2):
        live = jnp.where(c == which, own_n, sib_n)
        valid = jnp.where(position < live, 1.0, 0.0)
        rows = slice(which * TOK, (which + 1) * TOK)
        diff = keys[rows, :] - tbuf[which].astype(F32)
        keys[rows, :] = valid * diff
        dk = scale * valid * diff
        dkt[:, rows] = jnp.transpose(dk).astype(BF16)
    def low_rows(i, xx):
        return pl.ds(pl.multiple_of(CK * i + XK * xx, 16), XK)

    def cols_of(j):
        return pl.ds(pl.multiple_of(ring4(y, j) * YB, 128), YB)

    relay = [[] for _ in range(CH)]
    stage1 = [[] for _ in range(CH)]
    def issue(i, j):
        rows = pl.ds(CK * i, CK)
        if j == 2:
            relay[i].append(Group(
                SLOT["qy"] + i, gup.at[0, rows],
                [(gup.at[ring4(y, 2), rows, pl.ds(at * PC, PC)], qy.at[at, rows], to_y(d))
                 for at, d in enumerate((1, 3))],
            ))
            relay[i][0].start()
        via, past = (1, 3) if j in (2, 1) else (3, 1)
        send(
            glow.at[low_rows(i, ring4(x, 2)), cols_of(j)], qx.at[i, j],
            SLOT["qx"] + i, to_x(via),
        ).start()
        if j in (1, 3):
            at = 0 if j == 1 else 1
            lanes = pl.ds((1 - at) * PC, PC)
            send(
                gup.at[ring4(y, j), rows, lanes], ry.at[at, rows, lanes],
                SLOT["ry"] + i, to_y(j),
            ).start()
        at = 0 if past == 1 else 1
        send(
            glow.at[low_rows(i, ring4(x, past)), cols_of(j)], rx.at[at, i, :, cols_of(j)],
            SLOT["rx"] + i, to_x(past),
        ).start()

    order = (2, 3, 1, 0)
    for j in order:
        term = jnp.dot(dkt[...], nbuf[:, cols_of(j)], preferred_element_type=F32)
        gup[ring4(y, j)] = term[:QK].astype(BF16)
        glow[:, cols_of(j)] = term[QK:].astype(BF16)
        issue(0, j)
    for j in order:
        issue(1, j)
    def combine(i):
        relay[i].append(Group(SLOT["qx"] + i, qx.at[i], []))
        take(*relay[i])
        rows = slice(CK * i, CK * i + CK)
        late_y, late_x = [], []
        for at, d in enumerate((1, 3)):
            yy, lanes = ring4(y, d), slice(at * PC, (at + 1) * PC)
            both = gup[yy, rows, lanes].astype(F32) + qy[at, rows].astype(F32)
            gup[yy, rows, lanes] = both.astype(BF16)
            late_y.append((gup.at[yy, rows, lanes], ry.at[at, rows, lanes], to_y(d)))
        for at, d in enumerate((1, 3)):
            there = low_rows(i, ring4(x, d))
            for j in ((2, 1), (3, 0))[at]:
                both = glow[there, cols_of(j)].astype(F32) + qx[i, j].astype(F32)
                glow[there, cols_of(j)] = both.astype(BF16)
                late_x.append(
                    (glow.at[there, cols_of(j)], rx.at[at, i, :, cols_of(j)], to_x(d))
                )
        rows = pl.ds(CK * i, CK)
        stage1[i] += [
            Group(SLOT["ry"] + i, gup.at[0, rows], []),
            Group(SLOT["rx"] + i, rx.at[0, i], []),
            Group(SLOT["ry"] + CH + i, gup.at[0, rows], late_y),
            Group(SLOT["rx"] + CH + i, rx.at[0, i], late_x),
        ]
        go(*stage1[i][2:])

    squares = jnp.sum(keys[...] * keys[...], axis=0, keepdims=True)
    lown[...] = jnp.broadcast_to(jnp.sum(squares, axis=1, keepdims=True), (1, 128))
    lsend = send(lown, lsib, SLOT["lsib"], sib)
    lsend.start()
    combine(0)
    for j in order:
        issue(2, j)
    take(lsend)
    lsh[mine] = lown[...] + lsib[...]
    lsends = Group(
        SLOT["lsh"], lsh.at[pl.ds(0, 7)],
        [(lsh.at[mine], lsh.at[mine], dev) for _, dev in shard_peers],
    )
    lsends.start()

    stage2 = [[] for _ in range(CH)]
    stage3 = [[] for _ in range(CH)]
    agz = [[] for _ in range(CH)]
    agx = [[] for _ in range(CH)]

    def reduce1(i):
        take(*stage1[i])
        rows = slice(CK * i, CK * i + CK)
        total = (
            gup[y, rows].astype(F32) + ry[0, rows].astype(F32) + ry[1, rows].astype(F32)
        )
        s2y[rows] = total
        s2b[rows] = total.astype(BF16)
        stage2[i].append(Group(
            SLOT["s2y"] + i, r2y.at[i],
            [(s2b.at[low_rows(i, ring4(x, d))], r2y.at[i, d - 1], to_x(d)) for d in (1, 3, 2)],
        ))
        stage2[i][0].start()
        for j in (1, 3, 2, 0):
            cols = cols_of(j)
            total = (
                glow[low_rows(i, x), cols].astype(F32) + rx[0, i, :, cols].astype(F32)
                + rx[1, i, :, cols].astype(F32)
            )
            if j:
                sb[i, j - 1] = total.astype(BF16)
                send(sb.at[i, j - 1], r2x.at[i, j - 1], SLOT["s2x"] + i, to_y(j)).start()
            else:
                sx[i] = total
        stage2[i].append(Group(SLOT["s2x"] + i, r2x.at[i], []))

    def reduce2(i):
        take(*stage2[i])
        upper = s2y[low_rows(i, x), :]
        lower = sx[i]
        for d in range(3):
            upper = upper + r2y[i, d].astype(F32)
            lower = lower + r2x[i, d].astype(F32)
        for hh in range(2):
            for l in range(4):
                both = upper if l < 2 else lower
                at = ZK * (l % 2)
                block = both[at : at + ZK, hh * PC : (hh + 1) * PC]
                t3[i, hh, l] = block
                t3b[i, hh, l] = block.astype(BF16)
        stage3[i].append(Group(
            SLOT["s3"] + i, r3.at[i, pl.ds(1, 7)],
            [(t3b.at[i, lax.rem(h + at // 4, 2), ring4(zl, at % 4)], r3.at[i, at], dev)
             for at, dev in z_peers],
        ))
        stage3[i][0].start()

    def reduce3(i):
        take(*stage3[i])
        piece = t3[i, h, zl]
        for at in range(1, 8):
            piece = piece + r3[i, at].astype(F32)
        pown[i] = piece
        prol[i] = jnp.concatenate([piece[:, SL:], piece[:, :SL]], axis=1)
        swaps.append(send(prol.at[i], psib.at[i], SLOT["out"] + i, sib))
        swaps[i].start()

    def scatter(i):
        take(swaps[i])
        fin[i, x, zl] = jnp.where(own, pown[i], psib[i])
        agz[i].append(Group(
            SLOT["agz"] + i, fin.at[i, x, pl.ds(0, 3)],
            [(fin.at[i, x, zl], fin.at[i, x, zl], {"dp_0": ring4(zl, d)}) for d in (1, 3, 2)],
        ))
        agz[i][0].start()

    def gather(i):
        take(*agz[i])
        agx[i].append(Group(
            SLOT["agx"] + i, fin.at[i, pl.ds(0, 3 if i == CH - 1 else 2)],
            [(fin.at[i, x], fin.at[i, x], to_x(d)) for d in ((1, 3, 2) if i == CH - 1 else (1, 3))],
        ))
        agx[i][0].start()

    def forward(i):
        take(agx[i][0])
        behind = fin.at[i, ring4(x, 3), pl.ds(0, 2)]
        ahead = fin.at[i, ring4(x, 1), pl.ds(2, 2)]
        agx[i].append(Group(
            SLOT["agf"] + i, fin.at[i, 0],
            [(behind, behind, to_x(1)), (ahead, ahead, to_x(3))],
        ))
        agx[i][1].start()

    def drain(copies):
        for copy in copies:
            copy.wait_send()

    swaps = []
    combine(1)
    reduce1(0)
    combine(2)
    reduce1(1)
    reduce2(0)
    drain([sib_w, sib_info, sib_tea, sib_hid, gsend, csend] + first + second)
    drain(handed.values())

    @pl.when(edge)
    def _():
        for i in range(3):
            z_over(i).wait_send()
            z_in(i).wait_send()

    reduce1(2)
    reduce2(1)
    reduce3(0)
    drain([lsend] + sum(relay + stage1, []))
    reduce2(2)
    scatter(0)
    take(lsends)
    total = lsh[0]
    for i in range(1, 8):
        total = total + lsh[i]
    ldp[gid] = total
    lsends2 = Group(
        SLOT["ldp"], ldp.at[pl.ds(0, 15)],
        [(ldp.at[gid], ldp.at[gid], dev) for _, dev in dp_peers],
    )
    lsends2.start()
    reduce3(1)
    scatter(1)
    gather(0)
    reduce3(2)
    gather(1)
    scatter(2)
    forward(0)
    drain([lsends] + sum(stage2, []))
    take(lsends2)
    total = ldp[0]
    for i in range(1, 16):
        total = total + ldp[i]
    loss_o[...] = (total / (2.0 * KV * count))[:, 0:1]
    drain([lsends2] + sum(stage3, []) + swaps)
    gather(2)
    forward(1)
    drain(agz[0] + agz[1] + agx[0])
    for i in range(CH):
        take(agx[i][-1])
    ordered = [
        fin[i, xx, 2 * side + l]
        for side in range(2) for i in range(CH) for xx in range(4) for l in range(2)
    ]
    kt[...] = jnp.transpose(jnp.concatenate(ordered, axis=0))
    outs = [
        pltpu.make_async_copy(
            kt.at[pl.ds(half * SL, SL)], key_o.at[:, pl.ds(half * HK, HK)], lsem.at[4 + half]
        )
        for half in range(2)
    ]
    go(*outs)
    terms = (
        kt[:SL, :] * wv[:, :HK].astype(F32) + kt[SL:, :] * wv[:, HK:].astype(F32)
    )
    summed = lax.dot_general(
        jnp.ones((8, HK), F32), terms, (((1,), (1,)), ((), ())),
        preferred_element_type=F32, precision=lax.Precision.HIGHEST,
    )
    gain_o[...] = summed[0:1, :] / own_gain
    drain(agz[2] + agx[1] + agx[2])
    for copy in outs:
        copy.wait()


def finish(key, gain, loss, loss_o, gain_o, key_o, sem):
    copy = pltpu.make_async_copy(key, key_o, sem)
    copy.start()
    loss_o[...] = loss[...]
    gain_o[...] = gain[...].reshape(SL)
    copy.wait()


def body(hidden_in, teacher, norm_gain, w_key, group_rows, member):
    vm = pl.BlockSpec(memory_space=pltpu.VMEM)
    hbm = pl.BlockSpec(memory_space=pl.ANY)
    far = pl.BlockSpec(memory_space=pltpu.HBM)
    loss, gain, key = pl.pallas_call(
        kernel,
        out_shape=(
            jax.ShapeDtypeStruct((1, 1), F32),
            pltpu.VMEM((1, SL), F32),
            pltpu.VMEM((SL, KV), F32),
        ),
        in_specs=[far, far, far, vm, vm, vm],
        out_specs=(vm, vm, hbm),
        scratch_shapes=[
            pltpu.VMEM((SL, KV), BF16),
            pltpu.VMEM((2, TOK, D), BF16),
            pltpu.VMEM((2, TOK, HK), BF16),
            pltpu.VMEM((4, YB, HK), BF16),
            pltpu.VMEM((2 * TOK, D), BF16),
            pltpu.VMEM((2, TOK, 128), F32),
            pltpu.VMEM((2 * TOK, HK), F32),
            pltpu.VMEM((HK, 2 * TOK), BF16),
            pltpu.VMEM((4, QK, YB), BF16),
            pltpu.VMEM((QK, 4 * YB), BF16),
            pltpu.VMEM((2, QK, PC), BF16),
            pltpu.VMEM((CH, 4, XK, YB), BF16),
            pltpu.VMEM((2, QK, YB), BF16),
            pltpu.VMEM((2, CH, XK, 4 * YB), BF16),
            pltpu.VMEM((QK, YB), F32),
            pltpu.VMEM((QK, YB), BF16),
            pltpu.VMEM((CH, XK, YB), F32),
            pltpu.VMEM((CH, 3, XK, YB), BF16),
            pltpu.VMEM((CH, 3, XK, YB), BF16),
            pltpu.VMEM((CH, 3, XK, YB), BF16),
            pltpu.VMEM((CH, 2, 4, ZK, PC), F32),
            pltpu.VMEM((CH, 2, 4, ZK, PC), BF16),
            pltpu.VMEM((CH, 8, ZK, PC), BF16),
            pltpu.VMEM((CH, ZK, PC), F32),
            pltpu.VMEM((CH, ZK, PC), F32),
            pltpu.VMEM((CH, ZK, PC), F32),
            pltpu.VMEM((CH, 4, 4, ZK, PC), F32),
            pltpu.VMEM((PC, HK), F32),
            pltpu.VMEM((1, PC + 128), F32),
            pltpu.VMEM((1, PC + 128), F32),
            pltpu.VMEM((8, 1, PC + 128), F32),
            pltpu.VMEM((16, 1, 128), F32),
            pltpu.VMEM((1, 128), F32),
            pltpu.VMEM((1, 128), F32),
            pltpu.VMEM((8, 1, 128), F32),
            pltpu.VMEM((16, 1, 128), F32),
            pltpu.SemaphoreType.DMA((6,)),
            pltpu.SemaphoreType.DMA((N_SLOT,)),
            pltpu.SemaphoreType.DMA((N_SLOT,)),
            pltpu.SemaphoreType.DMA((3,)),
        ],
        compiler_params=pltpu.CompilerParams(
            collective_id=0, has_side_effects=True, vmem_limit_bytes=60 * 2**20
        ),
    )(hidden_in, teacher, w_key, norm_gain, group_rows, member)
    loss, grad_gain, grad_key = pl.pallas_call(
        finish,
        out_shape=(
            jax.ShapeDtypeStruct((1, 1), F32),
            jax.ShapeDtypeStruct((SL,), F32),
            jax.ShapeDtypeStruct((SL, KV), F32),
        ),
        in_specs=[hbm, vm, vm],
        out_specs=(vm, vm, far),
        scratch_shapes=[pltpu.SemaphoreType.DMA],
        compiler_params=pltpu.CompilerParams(vmem_limit_bytes=8 * 2**20),
    )(key, gain, loss)
    return loss.reshape(()), grad_gain, grad_key


def solution(mesh):
    split = Mesh(mesh.devices.reshape(4, 4, 2, 4, 2), DP_SHARD)
    return jax.shard_map(
        body,
        mesh=split,
        in_specs=(
            P(DP_SHARD, None),
            P(DP_SHARD, None),
            P(SHARD),
            P(SHARD, None),
            P(DP),
            P(DP, SHARD),
        ),
        out_specs=(P(), P(SHARD), P(SHARD, None)),
        check_vma=False,
    )
```

```python
import jax
import jax.numpy as jnp
from jax import lax
from jax.experimental import pallas as pl
from jax.experimental.pallas import tpu as pltpu
from jax.sharding import Mesh
from jax.sharding import PartitionSpec as P

SHARD = ("shard_0", "shard_1", "shard_2")
DP_SHARD = ("dp_0", "dp_1", "shard_0", "shard_1", "shard_2")
DP = ("dp_0", "dp_1")
MESH = pl.DeviceIdType.MESH
F32, BF16 = jnp.float32, jnp.bfloat16

EPSILON = 1e-06
SCALE = 1024.0

TOK = 256
D = 5120
KV = 768
HK = KV // 2
SL = 320
PC = 2 * SL
YB = 2 * PC
QK = HK // 2
CH = 3
CK = QK // CH
XK = CK // 4
ZK = XK // 2

HR = 80
DR = 2 * HR
SR = 80
SA = 48

def slots(*groups):
    place, at = {}, 0
    for name, count in groups:
        place[name] = at
        at += count
    return place, at


SLOT, N_SLOT = slots(
    *((name, 1) for name in ("info", "w", "tea", "hid", "lsib", "ginfo", "lsh", "cnt", "ldp")),
    ("wy", 12), ("wx", 8), ("wz", 3), ("qy", CH), ("qx", CH), ("ry", 2 * CH), ("rx", 2 * CH),
    ("s2y", CH), ("s2x", CH), ("s3", CH), ("agz", CH), ("agx", CH), ("agf", CH), ("out", CH),
)


def kernel(
    hid, tea, w, gain, rows_of, alive, loss_o, gain_o, key_o,
    wv, hbuf, tbuf, wbuf, nbuf, inv, keys, dkt, gup, glow, qy, qx, ry, rx,
    s2y, s2b, sx, sb, r2y, r2x, t3, t3b, r3, pown, prol, psib, fin, last, kt, info, isib, gfull, cbuf, lown, lsib, lsh, ldp,
    lsem, ssem, rsem, zsem,
):
    zl, x = lax.axis_index("dp_0"), lax.axis_index("dp_1")
    h, y, c = (lax.axis_index(a) for a in SHARD)

    def ring4(v, d):
        return lax.rem(v + d, 4)

    def to_y(d):
        return {"shard_1": ring4(y, d)}

    def to_x(d):
        return {"dp_1": ring4(x, d)}

    sib = {"shard_2": 1 - c}

    def send(src, dst, slot, dev):
        return pltpu.make_async_remote_copy(
            src_ref=src, dst_ref=dst, send_sem=ssem.at[slot], recv_sem=rsem.at[slot],
            device_id=dev, device_id_type=MESH,
        )

    class Group:
        def __init__(self, slot, whole, parts):
            self.copies = [send(src, dst, slot, dev) for src, dst, dev in parts]
            self.whole = send(whole, whole, slot, sib)

        def start(self):
            for copy in self.copies:
                copy.start()

        def wait_recv(self):
            self.whole.wait_recv()

        def wait_send(self):
            self.whole.wait_send()

    shard_peers = [
        (dh * 4 + dy, {"shard_0": lax.rem(h + dh, 2), "shard_1": ring4(y, dy)})
        for dh in range(2) for dy in range(4) if dh or dy
    ]
    dp_peers = [
        (dl * 4 + dx, {"dp_0": ring4(zl, dl), "dp_1": ring4(x, dx)})
        for dl in range(4) for dx in range(4) if dl or dx
    ]
    z_peers = [
        (dh * 4 + dl, {"shard_0": lax.rem(h + dh, 2), "dp_0": ring4(zl, dl)})
        for dh in range(2) for dl in range(4) if dh or dl
    ]
    extra = [dev for at, dev in z_peers if at > 4]
    everyone = [sib] + [dev for _, dev in shard_peers + dp_peers] + extra

    own_rows = pl.ds(pl.multiple_of(h * PC + c * SL, 64), SL)
    my_cols = pl.ds(pl.multiple_of(c * HK, 128), HK)
    sib_cols = pl.ds(pl.multiple_of((1 - c) * HK, 128), HK)
    mine = y * 2 + h
    gid = zl * 4 + x

    stage_w = pltpu.make_async_copy(w, wv, lsem.at[3])
    stage_w.start()
    barrier = pltpu.get_barrier_semaphore()
    for dev in everyone:
        pl.semaphore_signal(barrier, inc=1, device_id=dev, device_id_type=MESH)

    own_hid = pltpu.make_async_copy(hid, hbuf.at[c], lsem.at[0])
    own_hid.start()
    own_w = pltpu.make_async_copy(w.at[:, my_cols], wbuf.at[y, own_rows], lsem.at[1])
    own_w.start()
    own_tea = pltpu.make_async_copy(tea.at[:, my_cols], tbuf.at[c], lsem.at[2])
    own_tea.start()

    own_gain = gain[...].astype(F32).reshape(1, SL)
    lane = lax.broadcasted_iota(jnp.int32, (1, PC), 1)
    own = (lane >= c * SL) & (lane < c * SL + SL)
    info[:, 0:PC] = jnp.where(own, jnp.concatenate([own_gain, own_gain], axis=1), 0.0)
    live = (alive[...] * rows_of[...].reshape(1, 1)).astype(F32)
    info[:, PC:] = jnp.broadcast_to(live, (1, 128))

    pl.semaphore_wait(barrier, len(everyone))

    stage_w.wait()
    sib_w = send(wv.at[:, sib_cols], wbuf.at[y, own_rows], SLOT["w"], sib)
    sib_w.start()
    sib_info = send(info, isib, SLOT["info"], sib)
    sib_info.start()
    sib_tea = send(tea.at[:, sib_cols], tbuf.at[c], SLOT["tea"], sib)
    sib_tea.start()
    sib_hid = send(hid, hbuf.at[c], SLOT["hid"], sib)
    sib_hid.start()

    edge = (zl == 0) | (zl == 3)
    over = {"shard_0": 1 - h, "dp_0": 3 - zl}
    inner = {"dp_0": jnp.where(zl == 0, 1, 2)}
    split = PC // 2 + SR * x

    def part(owner, half, at, n):
        return wbuf.at[owner, pl.ds(pl.multiple_of(half * PC + at, 16), n)]

    z_parts = ((split, SR), (0, DR), (DR, DR))

    def z_over(i):
        ref = part(y, h, *z_parts[i])
        return send(ref, ref, SLOT["wz"] + i, over)

    def z_in(i):
        ref = part(y, 1 - h, *z_parts[i])
        return pltpu.make_async_remote_copy(
            src_ref=ref, dst_ref=ref, send_sem=zsem.at[i], recv_sem=rsem.at[SLOT["wz"] + i],
            device_id=inner, device_id_type=MESH,
        )

    def z_relay(i):
        @pl.when(edge)
        def _():
            z_in(i).wait_recv()
            z_in(i).start()

    def z_take(i):
        @pl.when(jnp.logical_not(edge))
        def _():
            z_in(i).wait_recv()

    def y_copies(g):
        half = h if g == 0 else 1 - h
        back, ahead = ring4(y, 3), ring4(y, 1)
        plan = (
            (y, split, SR, 1), (y, split, SR, 3),
            (y, 0, DR, 1), (y, 0, DR, 3), (y, DR, DR, 1), (y, DR, DR, 3),
            (back, split, SA, 1), (ahead, split + SA, SR - SA, 3),
            (back, 0, HR, 1), (ahead, HR, HR, 3),
            (back, DR, HR, 1), (ahead, DR + HR, HR, 3),
        )
        groups = []
        for i in range(0, len(plan), 2):
            pair = [(part(owner, half, at, n), d) for owner, at, n, d in plan[i : i + 2]]
            total = sum(n for _, _, n, _ in plan[i : i + 2])
            groups.append(Group(
                SLOT["wy"] + 6 * g + i // 2, wbuf.at[0, pl.ds(0, total)],
                [(ref, ref, to_y(d)) for ref, d in pair],
            ))
        return groups

    first, second = y_copies(0), y_copies(1)
    handed = {}

    def hand(g, k):
        ref = part(ring4(y, k), h if g == 0 else 1 - h, split, SR)
        handed[g, k] = Group(
            SLOT["wx"] + 4 * g + k, wbuf.at[0, pl.ds(0, 3 * SR)],
            [(ref, ref, to_x(i)) for i in (1, 3, 2)],
        )
        handed[g, k].start()

    def take(*copies):
        for copy in copies:
            copy.wait_recv()

    def go(*copies):
        for copy in copies:
            copy.start()

    sib_info.wait_recv()
    gfull[mine] = info[...] + isib[...]
    gsend = Group(
        SLOT["ginfo"], gfull.at[pl.ds(0, 7)],
        [(gfull.at[mine], gfull.at[mine], dev) for _, dev in shard_peers],
    )
    gsend.start()
    own_w.wait()
    sib_w.wait_recv()
    go(first[0])

    @pl.when(edge)
    def _():
        z_over(0).start()

    go(first[1])

    @pl.when(edge)
    def _():
        z_over(1).start()
        z_over(2).start()

    def norms(which):
        @pl.loop(0, TOK // 32)
        def _(i):
            rows = pl.ds(pl.multiple_of(i * 32, 32), 32)
            v = hbuf[which, rows, :].astype(F32)
            mean = jnp.sum(v * v, axis=1, keepdims=True) * (1.0 / D)
            inv[which, rows, :] = jnp.broadcast_to(lax.rsqrt(mean + EPSILON), (32, 128))

    def normalize(yy, hh):
        src = (hh * 4 + yy) * PC
        dst = (yy * 2 + hh) * PC
        for which in range(2):
            @pl.loop(0, TOK // 64)
            def _(i):
                rows = pl.ds(pl.multiple_of(i * 64, 64), 64)
                out = pl.ds(pl.multiple_of(which * TOK + i * 64, 64), 64)
                scale = inv[which, rows, :]
                for lane in range(0, PC, 128):
                    by = gfull[yy * 2 + hh, :, lane : lane + 128]
                    v = hbuf[which, rows, src + lane : src + lane + 128].astype(F32)
                    nbuf[out, dst + lane : dst + lane + 128] = (v * scale * by).astype(BF16)

    def project(k, g, start=False):
        half = h if g == 0 else 1 - h
        owner = ring4(y, k)
        cols = pl.ds(pl.multiple_of(owner * YB + half * PC, 128), PC)
        rows = pl.ds(pl.multiple_of(half * PC, 64), PC)
        term = jnp.dot(nbuf[:, cols], wbuf[owner, rows, :], preferred_element_type=F32)
        keys[...] = term if start else keys[...] + term

    own_hid.wait()
    norms(c)
    take(first[0])
    go(first[3])
    hand(0, 3)
    hand(0, 1)
    go(first[2])
    z_relay(0)
    z_take(0)
    go(second[0])
    hand(1, 0)
    z_relay(1)
    take(gsend)
    group = gfull[0, :, PC:]
    for i in range(1, 8):
        group = group + gfull[i, :, PC:]
    cbuf[gid] = group
    csend = Group(
        SLOT["cnt"], cbuf.at[pl.ds(0, 15)],
        [(cbuf.at[gid], cbuf.at[gid], dev) for _, dev in dp_peers],
    )
    csend.start()
    sib_hid.wait_recv()
    norms(1 - c)
    z_relay(2)
    take(first[1])
    go(first[4])
    z_take(1)
    go(second[1])
    take(first[2])
    go(first[5])
    normalize(0, 0)
    take(second[0])
    go(second[3])
    hand(1, 3)
    hand(1, 1)
    normalize(0, 1)
    take(first[3])
    hand(0, 2)
    normalize(1, 0)
    z_take(2)
    go(second[2])
    normalize(1, 1)
    normalize(2, 0)
    take(second[1])
    go(second[4])
    take(second[3])
    hand(1, 2)
    normalize(2, 1)
    normalize(3, 0)
    normalize(3, 1)
    project(0, 0, True)
    take(second[2])
    go(second[5])
    take(handed[0, 3], handed[0, 1])
    project(3, 0)
    project(1, 0)
    take(handed[1, 0])
    project(0, 1)
    take(handed[0, 2], *first[4:])
    project(2, 0)
    take(csend)
    take(handed[1, 3], handed[1, 1])
    project(3, 1)
    project(1, 1)
    take(handed[1, 2], *second[4:])
    project(2, 1)

    count = cbuf[0]
    for i in range(1, 16):
        count = count + cbuf[i]
    count = count[:, 0:1]
    scale = SCALE / count
    sib_tea.wait_recv()
    own_tea.wait()
    own_n = info[:, PC : PC + 1]
    sib_n = isib[:, PC : PC + 1]
    position = lax.broadcasted_iota(jnp.int32, (TOK, 1), 0).astype(F32)
    for which in range(2):
        live = jnp.where(c == which, own_n, sib_n)
        valid = jnp.where(position < live, 1.0, 0.0)
        rows = slice(which * TOK, (which + 1) * TOK)
        diff = keys[rows, :] - tbuf[which].astype(F32)
        keys[rows, :] = valid * diff
        dk = scale * valid * diff
        dkt[:, rows] = jnp.transpose(dk).astype(BF16)
    def low_rows(i, xx):
        return pl.ds(pl.multiple_of(CK * i + XK * xx, 16), XK)

    def cols_of(j):
        return pl.ds(pl.multiple_of(ring4(y, j) * YB, 128), YB)

    relay = [[] for _ in range(CH)]
    stage1 = [[] for _ in range(CH)]
    def issue(i, j):
        rows = pl.ds(CK * i, CK)
        if j == 2:
            relay[i].append(Group(
                SLOT["qy"] + i, gup.at[0, rows],
                [(gup.at[ring4(y, 2), rows, pl.ds(at * PC, PC)], qy.at[at, rows], to_y(d))
                 for at, d in enumerate((1, 3))],
            ))
            relay[i][0].start()
        via, past = (1, 3) if j in (2, 1) else (3, 1)
        send(
            glow.at[low_rows(i, ring4(x, 2)), cols_of(j)], qx.at[i, j],
            SLOT["qx"] + i, to_x(via),
        ).start()
        if j in (1, 3):
            at = 0 if j == 1 else 1
            lanes = pl.ds((1 - at) * PC, PC)
            send(
                gup.at[ring4(y, j), rows, lanes], ry.at[at, rows, lanes],
                SLOT["ry"] + i, to_y(j),
            ).start()
        at = 0 if past == 1 else 1
        send(
            glow.at[low_rows(i, ring4(x, past)), cols_of(j)], rx.at[at, i, :, cols_of(j)],
            SLOT["rx"] + i, to_x(past),
        ).start()

    order = (2, 3, 1, 0)
    for j in order:
        term = jnp.dot(dkt[...], nbuf[:, cols_of(j)], preferred_element_type=F32)
        gup[ring4(y, j)] = term[:QK].astype(BF16)
        glow[:, cols_of(j)] = term[QK:].astype(BF16)
        issue(0, j)
    for j in order:
        issue(1, j)
    def combine(i):
        relay[i].append(Group(SLOT["qx"] + i, qx.at[i], []))
        take(*relay[i])
        rows = slice(CK * i, CK * i + CK)
        late_y, late_x = [], []
        for at, d in enumerate((1, 3)):
            yy, lanes = ring4(y, d), slice(at * PC, (at + 1) * PC)
            both = gup[yy, rows, lanes].astype(F32) + qy[at, rows].astype(F32)
            gup[yy, rows, lanes] = both.astype(BF16)
            late_y.append((gup.at[yy, rows, lanes], ry.at[at, rows, lanes], to_y(d)))
        for at, d in enumerate((1, 3)):
            there = low_rows(i, ring4(x, d))
            for j in ((2, 1), (3, 0))[at]:
                both = glow[there, cols_of(j)].astype(F32) + qx[i, j].astype(F32)
                glow[there, cols_of(j)] = both.astype(BF16)
                late_x.append(
                    (glow.at[there, cols_of(j)], rx.at[at, i, :, cols_of(j)], to_x(d))
                )
        rows = pl.ds(CK * i, CK)
        stage1[i] += [
            Group(SLOT["ry"] + i, gup.at[0, rows], []),
            Group(SLOT["rx"] + i, rx.at[0, i], []),
            Group(SLOT["ry"] + CH + i, gup.at[0, rows], late_y),
            Group(SLOT["rx"] + CH + i, rx.at[0, i], late_x),
        ]
        go(*stage1[i][2:])

    squares = jnp.sum(keys[...] * keys[...], axis=0, keepdims=True)
    lown[...] = jnp.broadcast_to(jnp.sum(squares, axis=1, keepdims=True), (1, 128))
    lsend = send(lown, lsib, SLOT["lsib"], sib)
    lsend.start()
    combine(0)
    for j in order:
        issue(2, j)
    take(lsend)
    lsh[mine] = lown[...] + lsib[...]
    lsends = Group(
        SLOT["lsh"], lsh.at[pl.ds(0, 7)],
        [(lsh.at[mine], lsh.at[mine], dev) for _, dev in shard_peers],
    )
    lsends.start()

    stage2 = [[] for _ in range(CH)]
    stage3 = [[] for _ in range(CH)]
    agz = [[] for _ in range(CH)]
    agx = [[] for _ in range(CH)]

    def reduce1(i):
        take(*stage1[i])
        rows = slice(CK * i, CK * i + CK)
        total = (
            gup[y, rows].astype(F32) + ry[0, rows].astype(F32) + ry[1, rows].astype(F32)
        )
        s2y[rows] = total
        s2b[rows] = total.astype(BF16)
        stage2[i].append(Group(
            SLOT["s2y"] + i, r2y.at[i],
            [(s2b.at[low_rows(i, ring4(x, d))], r2y.at[i, d - 1], to_x(d)) for d in (1, 3, 2)],
        ))
        stage2[i][0].start()
        for j in (1, 3, 2, 0):
            cols = cols_of(j)
            total = (
                glow[low_rows(i, x), cols].astype(F32) + rx[0, i, :, cols].astype(F32)
                + rx[1, i, :, cols].astype(F32)
            )
            if j:
                sb[i, j - 1] = total.astype(BF16)
                send(sb.at[i, j - 1], r2x.at[i, j - 1], SLOT["s2x"] + i, to_y(j)).start()
            else:
                sx[i] = total
        stage2[i].append(Group(SLOT["s2x"] + i, r2x.at[i], []))

    def reduce2(i):
        take(*stage2[i])
        upper = s2y[low_rows(i, x), :]
        lower = sx[i]
        for d in range(3):
            upper = upper + r2y[i, d].astype(F32)
            lower = lower + r2x[i, d].astype(F32)
        for hh in range(2):
            for l in range(4):
                both = upper if l < 2 else lower
                at = ZK * (l % 2)
                block = both[at : at + ZK, hh * PC : (hh + 1) * PC]
                t3[i, hh, l] = block
                t3b[i, hh, l] = block.astype(BF16)
        stage3[i].append(Group(
            SLOT["s3"] + i, r3.at[i, pl.ds(1, 7)],
            [(t3b.at[i, lax.rem(h + at // 4, 2), ring4(zl, at % 4)], r3.at[i, at], dev)
             for at, dev in z_peers],
        ))
        stage3[i][0].start()

    def reduce3(i):
        take(*stage3[i])
        piece = t3[i, h, zl]
        for at in range(1, 8):
            piece = piece + r3[i, at].astype(F32)
        pown[i] = piece
        prol[i] = jnp.concatenate([piece[:, SL:], piece[:, :SL]], axis=1)
        swaps.append(send(prol.at[i], psib.at[i], SLOT["out"] + i, sib))
        swaps[i].start()

    def done(i):
        return last if i == CH - 1 else fin.at[i]

    def scatter(i):
        take(swaps[i])
        to = done(i)
        to[x, zl] = jnp.where(own, pown[i], psib[i]).astype(to.dtype)
        agz[i].append(Group(
            SLOT["agz"] + i, to.at[x, pl.ds(0, 3)],
            [(to.at[x, zl], to.at[x, zl], {"dp_0": ring4(zl, d)}) for d in (1, 3, 2)],
        ))
        agz[i][0].start()

    def gather(i):
        take(*agz[i])
        to, steps = done(i), (1, 3, 2) if i == CH - 1 else (1, 3)
        agx[i].append(Group(
            SLOT["agx"] + i, to.at[pl.ds(0, len(steps))],
            [(to.at[x], to.at[x], to_x(d)) for d in steps],
        ))
        agx[i][0].start()

    def forward(i):
        take(agx[i][0])
        behind = fin.at[i, ring4(x, 3), pl.ds(0, 2)]
        ahead = fin.at[i, ring4(x, 1), pl.ds(2, 2)]
        agx[i].append(Group(
            SLOT["agf"] + i, fin.at[i, 0],
            [(behind, behind, to_x(1)), (ahead, ahead, to_x(3))],
        ))
        agx[i][1].start()

    def drain(copies):
        for copy in copies:
            copy.wait_send()

    swaps = []
    combine(1)
    reduce1(0)
    combine(2)
    reduce1(1)
    reduce2(0)
    drain([sib_w, sib_info, sib_tea, sib_hid, gsend, csend] + first + second)
    drain(handed.values())

    @pl.when(edge)
    def _():
        for i in range(3):
            z_over(i).wait_send()
            z_in(i).wait_send()

    reduce1(2)
    reduce2(1)
    reduce3(0)
    drain([lsend] + sum(relay + stage1, []))
    reduce2(2)
    scatter(0)
    take(lsends)
    total = lsh[0]
    for i in range(1, 8):
        total = total + lsh[i]
    ldp[gid] = total
    lsends2 = Group(
        SLOT["ldp"], ldp.at[pl.ds(0, 15)],
        [(ldp.at[gid], ldp.at[gid], dev) for _, dev in dp_peers],
    )
    lsends2.start()
    reduce3(1)
    scatter(1)
    gather(0)
    reduce3(2)
    gather(1)
    scatter(2)
    forward(0)
    drain([lsends] + sum(stage2, []))
    take(lsends2)
    total = ldp[0]
    for i in range(1, 16):
        total = total + ldp[i]
    loss_o[...] = (total / (2.0 * KV * count))[:, 0:1]
    drain([lsends2] + sum(stage3, []) + swaps)
    gather(2)
    forward(1)
    drain(agz[0] + agz[1] + agx[0])
    for i in range(CH):
        take(agx[i][-1])
    ordered = [
        done(i)[xx, 2 * side + l].astype(F32)
        for side in range(2) for i in range(CH) for xx in range(4) for l in range(2)
    ]
    kt[...] = jnp.transpose(jnp.concatenate(ordered, axis=0))
    outs = [
        pltpu.make_async_copy(
            kt.at[pl.ds(half * SL, SL)], key_o.at[:, pl.ds(half * HK, HK)], lsem.at[4 + half]
        )
        for half in range(2)
    ]
    go(*outs)
    terms = (
        kt[:SL, :] * wv[:, :HK].astype(F32) + kt[SL:, :] * wv[:, HK:].astype(F32)
    )
    summed = lax.dot_general(
        jnp.ones((8, HK), F32), terms, (((1,), (1,)), ((), ())),
        preferred_element_type=F32, precision=lax.Precision.HIGHEST,
    )
    gain_o[...] = summed[0:1, :] / own_gain
    drain(agz[2] + agx[1] + agx[2])
    for copy in outs:
        copy.wait()


def finish(key, gain, loss, loss_o, gain_o, key_o, sem):
    copy = pltpu.make_async_copy(key, key_o, sem)
    copy.start()
    loss_o[...] = loss[...]
    gain_o[...] = gain[...].reshape(SL)
    copy.wait()


def body(hidden_in, teacher, norm_gain, w_key, group_rows, member):
    vm = pl.BlockSpec(memory_space=pltpu.VMEM)
    hbm = pl.BlockSpec(memory_space=pl.ANY)
    far = pl.BlockSpec(memory_space=pltpu.HBM)
    loss, gain, key = pl.pallas_call(
        kernel,
        out_shape=(
            jax.ShapeDtypeStruct((1, 1), F32),
            pltpu.VMEM((1, SL), F32),
            pltpu.VMEM((SL, KV), F32),
        ),
        in_specs=[far, far, far, vm, vm, vm],
        out_specs=(vm, vm, hbm),
        scratch_shapes=[
            pltpu.VMEM((SL, KV), BF16),
            pltpu.VMEM((2, TOK, D), BF16),
            pltpu.VMEM((2, TOK, HK), BF16),
            pltpu.VMEM((4, YB, HK), BF16),
            pltpu.VMEM((2 * TOK, D), BF16),
            pltpu.VMEM((2, TOK, 128), F32),
            pltpu.VMEM((2 * TOK, HK), F32),
            pltpu.VMEM((HK, 2 * TOK), BF16),
            pltpu.VMEM((4, QK, YB), BF16),
            pltpu.VMEM((QK, 4 * YB), BF16),
            pltpu.VMEM((2, QK, PC), BF16),
            pltpu.VMEM((CH, 4, XK, YB), BF16),
            pltpu.VMEM((2, QK, YB), BF16),
            pltpu.VMEM((2, CH, XK, 4 * YB), BF16),
            pltpu.VMEM((QK, YB), F32),
            pltpu.VMEM((QK, YB), BF16),
            pltpu.VMEM((CH, XK, YB), F32),
            pltpu.VMEM((CH, 3, XK, YB), BF16),
            pltpu.VMEM((CH, 3, XK, YB), BF16),
            pltpu.VMEM((CH, 3, XK, YB), BF16),
            pltpu.VMEM((CH, 2, 4, ZK, PC), F32),
            pltpu.VMEM((CH, 2, 4, ZK, PC), BF16),
            pltpu.VMEM((CH, 8, ZK, PC), BF16),
            pltpu.VMEM((CH, ZK, PC), F32),
            pltpu.VMEM((CH, ZK, PC), F32),
            pltpu.VMEM((CH, ZK, PC), F32),
            pltpu.VMEM((CH - 1, 4, 4, ZK, PC), F32),
            pltpu.VMEM((4, 4, ZK, PC), BF16),
            pltpu.VMEM((PC, HK), F32),
            pltpu.VMEM((1, PC + 128), F32),
            pltpu.VMEM((1, PC + 128), F32),
            pltpu.VMEM((8, 1, PC + 128), F32),
            pltpu.VMEM((16, 1, 128), F32),
            pltpu.VMEM((1, 128), F32),
            pltpu.VMEM((1, 128), F32),
            pltpu.VMEM((8, 1, 128), F32),
            pltpu.VMEM((16, 1, 128), F32),
            pltpu.SemaphoreType.DMA((6,)),
            pltpu.SemaphoreType.DMA((N_SLOT,)),
            pltpu.SemaphoreType.DMA((N_SLOT,)),
            pltpu.SemaphoreType.DMA((3,)),
        ],
        compiler_params=pltpu.CompilerParams(
            collective_id=0, has_side_effects=True, vmem_limit_bytes=60 * 2**20
        ),
    )(hidden_in, teacher, w_key, norm_gain, group_rows, member)
    loss, grad_gain, grad_key = pl.pallas_call(
        finish,
        out_shape=(
            jax.ShapeDtypeStruct((1, 1), F32),
            jax.ShapeDtypeStruct((SL,), F32),
            jax.ShapeDtypeStruct((SL, KV), F32),
        ),
        in_specs=[hbm, vm, vm],
        out_specs=(vm, vm, far),
        scratch_shapes=[pltpu.SemaphoreType.DMA],
        compiler_params=pltpu.CompilerParams(vmem_limit_bytes=8 * 2**20),
    )(key, gain, loss)
    return loss.reshape(()), grad_gain, grad_key


def solution(mesh):
    split = Mesh(mesh.devices.reshape(4, 4, 2, 4, 2), DP_SHARD)
    return jax.shard_map(
        body,
        mesh=split,
        in_specs=(
            P(DP_SHARD, None),
            P(DP_SHARD, None),
            P(SHARD),
            P(SHARD, None),
            P(DP),
            P(DP, SHARD),
        ),
        out_specs=(P(), P(SHARD), P(SHARD, None)),
        check_vma=False,
    )
```

```python
import jax
import jax.numpy as jnp
from jax import lax
from jax.experimental import pallas as pl
from jax.experimental.pallas import tpu as pltpu
from jax.sharding import Mesh
from jax.sharding import PartitionSpec as P

SHARD = ("shard_0", "shard_1", "shard_2")
DP_SHARD = ("dp_0", "dp_1", "shard_0", "shard_1", "shard_2")
DP = ("dp_0", "dp_1")
MESH = pl.DeviceIdType.MESH
F32, BF16 = jnp.float32, jnp.bfloat16

EPSILON = 1e-06
SCALE = 1024.0

TOK = 256
D = 5120
KV = 768
HK = KV // 2
SL = 320
PC = 2 * SL
YB = 2 * PC
QK = HK // 2
CH = 3
CK = QK // CH
XK = CK // 4
ZK = XK // 2

HR = 80
DR = 2 * HR
SR = 80
SA = 48

def slots(*groups):
    place, at = {}, 0
    for name, count in groups:
        place[name] = at
        at += count
    return place, at


SLOT, N_SLOT = slots(
    *((name, 1) for name in ("info", "w", "tea", "hid", "lsib", "ginfo", "lsh", "cnt", "ldp")),
    ("wy", 12), ("wx", 8), ("wz", 3), ("via", CH), ("s1", CH), ("s2", CH), ("s3", CH), ("agz", CH), ("agx", CH), ("agf", CH), ("out", CH),
)


def kernel(
    hid, tea, w, gain, rows_of, alive, loss_o, key_o,
    wv, hbuf, tbuf, wbuf, nbuf, inv, keys, dkt, gup, glow, qy, qx, ry, rx,
    s2y, s2b, sx, sb, r2y, r2x, t3, t3b, r3, pown, prol, psib, fin, last, kt, info, isib, gfull, cbuf, lown, lsib, lsh, ldp,
    lsem, ssem, rsem, zsem,
):
    zl, x = lax.axis_index("dp_0"), lax.axis_index("dp_1")
    h, y, c = (lax.axis_index(a) for a in SHARD)

    def ring4(v, d):
        return lax.rem(v + d, 4)

    def to_y(d):
        return {"shard_1": ring4(y, d)}

    def to_x(d):
        return {"dp_1": ring4(x, d)}

    sib = {"shard_2": 1 - c}

    def send(src, dst, slot, dev):
        return pltpu.make_async_remote_copy(
            src_ref=src, dst_ref=dst, send_sem=ssem.at[slot], recv_sem=rsem.at[slot],
            device_id=dev, device_id_type=MESH,
        )

    class Group:
        def __init__(self, slot, whole, parts):
            self.copies = [send(src, dst, slot, dev) for src, dst, dev in parts]
            self.whole = send(whole, whole, slot, sib)

        def start(self):
            for copy in self.copies:
                copy.start()

        def wait_recv(self):
            self.whole.wait_recv()

        def wait_send(self):
            self.whole.wait_send()

    shard_peers = [
        (dh * 4 + dy, {"shard_0": lax.rem(h + dh, 2), "shard_1": ring4(y, dy)})
        for dh in range(2) for dy in range(4) if dh or dy
    ]
    dp_peers = [
        (dl * 4 + dx, {"dp_0": ring4(zl, dl), "dp_1": ring4(x, dx)})
        for dl in range(4) for dx in range(4) if dl or dx
    ]
    z_peers = [
        (dh * 4 + dl, {"shard_0": lax.rem(h + dh, 2), "dp_0": ring4(zl, dl)})
        for dh in range(2) for dl in range(4) if dh or dl
    ]
    extra = [dev for at, dev in z_peers if at > 4]
    everyone = [sib] + [dev for _, dev in shard_peers + dp_peers] + extra

    own_rows = pl.ds(pl.multiple_of(h * PC + c * SL, 64), SL)
    my_cols = pl.ds(pl.multiple_of(c * HK, 128), HK)
    sib_cols = pl.ds(pl.multiple_of((1 - c) * HK, 128), HK)
    mine = y * 2 + h
    gid = zl * 4 + x

    stage_w = pltpu.make_async_copy(w, wv, lsem.at[3])
    stage_w.start()
    barrier = pltpu.get_barrier_semaphore()
    for dev in everyone:
        pl.semaphore_signal(barrier, inc=1, device_id=dev, device_id_type=MESH)

    own_hid = pltpu.make_async_copy(hid, hbuf.at[c], lsem.at[0])
    own_hid.start()
    own_w = pltpu.make_async_copy(w.at[:, my_cols], wbuf.at[y, own_rows], lsem.at[1])
    own_w.start()
    own_tea = pltpu.make_async_copy(tea.at[:, my_cols], tbuf.at[c], lsem.at[2])
    own_tea.start()

    own_gain = gain[...].astype(F32).reshape(1, SL)
    lane = lax.broadcasted_iota(jnp.int32, (1, PC), 1)
    own = (lane >= c * SL) & (lane < c * SL + SL)
    info[:, 0:PC] = jnp.where(own, jnp.concatenate([own_gain, own_gain], axis=1), 0.0)
    live = (alive[...] * rows_of[...].reshape(1, 1)).astype(F32)
    info[:, PC:] = jnp.broadcast_to(live, (1, 128))

    pl.semaphore_wait(barrier, len(everyone))

    stage_w.wait()
    sib_w = send(wv.at[:, sib_cols], wbuf.at[y, own_rows], SLOT["w"], sib)
    sib_w.start()
    sib_info = send(info, isib, SLOT["info"], sib)
    sib_info.start()
    sib_tea = send(tea.at[:, sib_cols], tbuf.at[c], SLOT["tea"], sib)
    sib_tea.start()
    sib_hid = send(hid, hbuf.at[c], SLOT["hid"], sib)
    sib_hid.start()

    edge = (zl == 0) | (zl == 3)
    over = {"shard_0": 1 - h, "dp_0": 3 - zl}
    inner = {"dp_0": jnp.where(zl == 0, 1, 2)}
    split = PC // 2 + SR * x

    def part(owner, half, at, n):
        return wbuf.at[owner, pl.ds(pl.multiple_of(half * PC + at, 16), n)]

    z_parts = ((split, SR), (0, DR), (DR, DR))

    def z_over(i):
        ref = part(y, h, *z_parts[i])
        return send(ref, ref, SLOT["wz"] + i, over)

    def z_in(i):
        ref = part(y, 1 - h, *z_parts[i])
        return pltpu.make_async_remote_copy(
            src_ref=ref, dst_ref=ref, send_sem=zsem.at[i], recv_sem=rsem.at[SLOT["wz"] + i],
            device_id=inner, device_id_type=MESH,
        )

    def z_relay(i):
        @pl.when(edge)
        def _():
            z_in(i).wait_recv()
            z_in(i).start()

    def z_take(i):
        @pl.when(jnp.logical_not(edge))
        def _():
            z_in(i).wait_recv()

    def y_copies(g):
        half = h if g == 0 else 1 - h
        back, ahead = ring4(y, 3), ring4(y, 1)
        plan = (
            (y, split, SR, 1), (y, split, SR, 3),
            (y, 0, DR, 1), (y, 0, DR, 3), (y, DR, DR, 1), (y, DR, DR, 3),
            (back, split, SA, 1), (ahead, split + SA, SR - SA, 3),
            (back, 0, HR, 1), (ahead, HR, HR, 3),
            (back, DR, HR, 1), (ahead, DR + HR, HR, 3),
        )
        groups = []
        for i in range(0, len(plan), 2):
            pair = [(part(owner, half, at, n), d) for owner, at, n, d in plan[i : i + 2]]
            total = sum(n for _, _, n, _ in plan[i : i + 2])
            groups.append(Group(
                SLOT["wy"] + 6 * g + i // 2, wbuf.at[0, pl.ds(0, total)],
                [(ref, ref, to_y(d)) for ref, d in pair],
            ))
        return groups

    first, second = y_copies(0), y_copies(1)
    handed = {}

    def hand(g, k):
        ref = part(ring4(y, k), h if g == 0 else 1 - h, split, SR)
        handed[g, k] = Group(
            SLOT["wx"] + 4 * g + k, wbuf.at[0, pl.ds(0, 3 * SR)],
            [(ref, ref, to_x(i)) for i in (1, 3, 2)],
        )
        handed[g, k].start()

    def take(*copies):
        for copy in copies:
            copy.wait_recv()

    def go(*copies):
        for copy in copies:
            copy.start()

    sib_info.wait_recv()
    gfull[mine] = info[...] + isib[...]
    gsend = Group(
        SLOT["ginfo"], gfull.at[pl.ds(0, 7)],
        [(gfull.at[mine], gfull.at[mine], dev) for _, dev in shard_peers],
    )
    gsend.start()
    own_w.wait()
    sib_w.wait_recv()
    go(first[0])

    @pl.when(edge)
    def _():
        z_over(0).start()

    go(first[1])

    @pl.when(edge)
    def _():
        z_over(1).start()
        z_over(2).start()

    def norms(which):
        @pl.loop(0, TOK // 32)
        def _(i):
            rows = pl.ds(pl.multiple_of(i * 32, 32), 32)
            v = hbuf[which, rows, :].astype(F32)
            mean = jnp.sum(v * v, axis=1, keepdims=True) * (1.0 / D)
            inv[which, rows, :] = jnp.broadcast_to(lax.rsqrt(mean + EPSILON), (32, 128))

    def normalize(yy, hh):
        src = (hh * 4 + yy) * PC
        dst = (yy * 2 + hh) * PC
        for which in range(2):
            @pl.loop(0, TOK // 64)
            def _(i):
                rows = pl.ds(pl.multiple_of(i * 64, 64), 64)
                out = pl.ds(pl.multiple_of(which * TOK + i * 64, 64), 64)
                scale = inv[which, rows, :]
                for lane in range(0, PC, 128):
                    by = gfull[yy * 2 + hh, :, lane : lane + 128]
                    v = hbuf[which, rows, src + lane : src + lane + 128].astype(F32)
                    nbuf[out, dst + lane : dst + lane + 128] = (v * scale * by).astype(BF16)

    def project(k, g, start=False):
        half = h if g == 0 else 1 - h
        owner = ring4(y, k)
        cols = pl.ds(pl.multiple_of(owner * YB + half * PC, 128), PC)
        rows = pl.ds(pl.multiple_of(half * PC, 64), PC)
        term = jnp.dot(nbuf[:, cols], wbuf[owner, rows, :], preferred_element_type=F32)
        keys[...] = term if start else keys[...] + term

    own_hid.wait()
    norms(c)
    take(first[0])
    go(first[3])
    hand(0, 3)
    hand(0, 1)
    go(first[2])
    z_relay(0)
    z_take(0)
    go(second[0])
    hand(1, 0)
    z_relay(1)
    take(gsend)
    group = gfull[0, :, PC:]
    for i in range(1, 8):
        group = group + gfull[i, :, PC:]
    cbuf[gid] = group
    csend = Group(
        SLOT["cnt"], cbuf.at[pl.ds(0, 15)],
        [(cbuf.at[gid], cbuf.at[gid], dev) for _, dev in dp_peers],
    )
    csend.start()
    sib_hid.wait_recv()
    norms(1 - c)
    z_relay(2)
    take(first[1])
    go(first[4])
    z_take(1)
    go(second[1])
    take(first[2])
    go(first[5])
    normalize(0, 0)
    take(second[0])
    go(second[3])
    hand(1, 3)
    hand(1, 1)
    normalize(0, 1)
    take(first[3])
    hand(0, 2)
    normalize(1, 0)
    z_take(2)
    go(second[2])
    normalize(1, 1)
    normalize(2, 0)
    take(second[1])
    go(second[4])
    take(second[3])
    hand(1, 2)
    normalize(2, 1)
    normalize(3, 0)
    normalize(3, 1)
    project(0, 0, True)
    take(second[2])
    go(second[5])
    take(handed[0, 3], handed[0, 1])
    project(3, 0)
    project(1, 0)
    take(handed[1, 0])
    project(0, 1)
    take(handed[0, 2], *first[4:])
    project(2, 0)
    take(csend)
    take(handed[1, 3], handed[1, 1])
    project(3, 1)
    project(1, 1)
    take(handed[1, 2], *second[4:])
    project(2, 1)

    count = cbuf[0]
    for i in range(1, 16):
        count = count + cbuf[i]
    count = count[:, 0:1]
    scale = SCALE / count
    sib_tea.wait_recv()
    own_tea.wait()
    own_n = info[:, PC : PC + 1]
    sib_n = isib[:, PC : PC + 1]
    position = lax.broadcasted_iota(jnp.int32, (TOK, 1), 0).astype(F32)
    for which in range(2):
        live = jnp.where(c == which, own_n, sib_n)
        valid = jnp.where(position < live, 1.0, 0.0)
        rows = slice(which * TOK, (which + 1) * TOK)
        diff = keys[rows, :] - tbuf[which].astype(F32)
        keys[rows, :] = valid * diff
        dk = scale * valid * diff
        dkt[:, rows] = jnp.transpose(dk).astype(BF16)
    def low_rows(i, xx):
        return pl.ds(pl.multiple_of(CK * i + XK * xx, 16), XK)

    def cols_of(j):
        return pl.ds(pl.multiple_of(ring4(y, j) * YB, 128), YB)

    relay = [[] for _ in range(CH)]
    stage1 = [[] for _ in range(CH)]
    def issue(i, j):
        rows = pl.ds(CK * i, CK)
        if j == 2:
            relay[i].append(Group(
                SLOT["via"] + i, gup.at[0, pl.ds(0, 2 * CK)],
                [(gup.at[ring4(y, 2), rows, pl.ds(at * PC, PC)], qy.at[at, rows], to_y(d))
                 for at, d in enumerate((1, 3))],
            ))
            relay[i][0].start()
        via, past = (1, 3) if j in (2, 1) else (3, 1)
        send(
            glow.at[low_rows(i, ring4(x, 2)), cols_of(j)], qx.at[i, j],
            SLOT["via"] + i, to_x(via),
        ).start()
        if j in (1, 3):
            at = 0 if j == 1 else 1
            lanes = pl.ds((1 - at) * PC, PC)
            send(
                gup.at[ring4(y, j), rows, lanes], ry.at[at, rows, lanes],
                SLOT["s1"] + i, to_y(j),
            ).start()
        at = 0 if past == 1 else 1
        send(
            glow.at[low_rows(i, ring4(x, past)), cols_of(j)], rx.at[at, i, :, cols_of(j)],
            SLOT["s1"] + i, to_x(past),
        ).start()

    order = (2, 3, 1, 0)
    for j in order:
        term = jnp.dot(dkt[...], nbuf[:, cols_of(j)], preferred_element_type=F32)
        gup[ring4(y, j)] = term[:QK].astype(BF16)
        glow[:, cols_of(j)] = term[QK:].astype(BF16)
        issue(0, j)
    for j in order:
        issue(1, j)
    def combine(i):
        take(*relay[i])
        rows = slice(CK * i, CK * i + CK)
        late_y, late_x = [], []
        for at, d in enumerate((1, 3)):
            yy, lanes = ring4(y, d), slice(at * PC, (at + 1) * PC)
            both = gup[yy, rows, lanes].astype(F32) + qy[at, rows].astype(F32)
            gup[yy, rows, lanes] = both.astype(BF16)
            late_y.append((gup.at[yy, rows, lanes], ry.at[at, rows, lanes], to_y(d)))
        for at, d in enumerate((1, 3)):
            there = low_rows(i, ring4(x, d))
            for j in ((2, 1), (3, 0))[at]:
                both = glow[there, cols_of(j)].astype(F32) + qx[i, j].astype(F32)
                glow[there, cols_of(j)] = both.astype(BF16)
                late_x.append(
                    (glow.at[there, cols_of(j)], rx.at[at, i, :, cols_of(j)], to_x(d))
                )
        stage1[i].append(Group(
            SLOT["s1"] + i, gup.at[pl.ds(0, 2), pl.ds(0, 2 * CK)], late_y + late_x
        ))
        stage1[i][0].start()

    squares = jnp.sum(keys[...] * keys[...], axis=0, keepdims=True)
    lown[...] = jnp.broadcast_to(jnp.sum(squares, axis=1, keepdims=True), (1, 128))
    lsend = send(lown, lsib, SLOT["lsib"], sib)
    lsend.start()
    combine(0)
    for j in order:
        issue(2, j)
    take(lsend)
    lsh[mine] = lown[...] + lsib[...]
    lsends = Group(
        SLOT["lsh"], lsh.at[pl.ds(0, 7)],
        [(lsh.at[mine], lsh.at[mine], dev) for _, dev in shard_peers],
    )
    lsends.start()

    stage2 = [[] for _ in range(CH)]
    stage3 = [[] for _ in range(CH)]
    agz = [[] for _ in range(CH)]
    agx = [[] for _ in range(CH)]

    def reduce1(i):
        take(*stage1[i])
        rows = slice(CK * i, CK * i + CK)
        total = (
            gup[y, rows].astype(F32) + ry[0, rows].astype(F32) + ry[1, rows].astype(F32)
        )
        s2y[rows] = total
        s2b[rows] = total.astype(BF16)
        stage2[i].append(Group(
            SLOT["s2"] + i, gup.at[0, pl.ds(0, 6 * XK)],
            [(s2b.at[low_rows(i, ring4(x, d))], r2y.at[i, d - 1], to_x(d)) for d in (1, 3, 2)],
        ))
        stage2[i][0].start()
        for j in (1, 3, 2, 0):
            cols = cols_of(j)
            total = (
                glow[low_rows(i, x), cols].astype(F32) + rx[0, i, :, cols].astype(F32)
                + rx[1, i, :, cols].astype(F32)
            )
            if j:
                sb[i, j - 1] = total.astype(BF16)
                send(sb.at[i, j - 1], r2x.at[i, j - 1], SLOT["s2"] + i, to_y(j)).start()
            else:
                sx[i] = total

    def reduce2(i):
        take(*stage2[i])
        upper = s2y[low_rows(i, x), :]
        lower = sx[i]
        for d in range(3):
            upper = upper + r2y[i, d].astype(F32)
            lower = lower + r2x[i, d].astype(F32)
        for hh in range(2):
            for l in range(4):
                both = upper if l < 2 else lower
                at = ZK * (l % 2)
                block = both[at : at + ZK, hh * PC : (hh + 1) * PC]
                t3[i, hh, l] = block
                t3b[i, hh, l] = block.astype(BF16)
        stage3[i].append(Group(
            SLOT["s3"] + i, r3.at[i, pl.ds(1, 7)],
            [(t3b.at[i, lax.rem(h + at // 4, 2), ring4(zl, at % 4)], r3.at[i, at], dev)
             for at, dev in z_peers],
        ))
        stage3[i][0].start()

    def reduce3(i):
        take(*stage3[i])
        piece = t3[i, h, zl]
        for at in range(1, 8):
            piece = piece + r3[i, at].astype(F32)
        pown[i] = piece
        prol[i] = jnp.concatenate([piece[:, SL:], piece[:, :SL]], axis=1)
        swaps.append(send(prol.at[i], psib.at[i], SLOT["out"] + i, sib))
        swaps[i].start()

    def done(i):
        return last if i == CH - 1 else fin.at[i]

    def scatter(i):
        take(swaps[i])
        to = done(i)
        to[x, zl] = jnp.where(own, pown[i], psib[i]).astype(to.dtype)
        agz[i].append(Group(
            SLOT["agz"] + i, to.at[x, pl.ds(0, 3)],
            [(to.at[x, zl], to.at[x, zl], {"dp_0": ring4(zl, d)}) for d in (1, 3, 2)],
        ))
        agz[i][0].start()

    def gather(i):
        take(*agz[i])
        to, steps = done(i), (1, 3, 2) if i == CH - 1 else (1, 3)
        agx[i].append(Group(
            SLOT["agx"] + i, to.at[pl.ds(0, len(steps))],
            [(to.at[x], to.at[x], to_x(d)) for d in steps],
        ))
        agx[i][0].start()

    def forward(i):
        take(agx[i][0])
        behind = fin.at[i, ring4(x, 3), pl.ds(0, 2)]
        ahead = fin.at[i, ring4(x, 1), pl.ds(2, 2)]
        agx[i].append(Group(
            SLOT["agf"] + i, fin.at[i, 0],
            [(behind, behind, to_x(1)), (ahead, ahead, to_x(3))],
        ))
        agx[i][1].start()

    def drain(copies):
        for copy in copies:
            copy.wait_send()

    swaps = []
    combine(1)
    reduce1(0)
    combine(2)
    reduce1(1)
    reduce2(0)
    drain([sib_w, sib_info, sib_tea, sib_hid, gsend, csend] + first + second)
    drain(handed.values())

    @pl.when(edge)
    def _():
        for i in range(3):
            z_over(i).wait_send()
            z_in(i).wait_send()

    reduce1(2)
    reduce2(1)
    reduce3(0)
    drain([lsend] + sum(relay + stage1, []))
    reduce2(2)
    scatter(0)
    take(lsends)
    total = lsh[0]
    for i in range(1, 8):
        total = total + lsh[i]
    ldp[gid] = total
    lsends2 = Group(
        SLOT["ldp"], ldp.at[pl.ds(0, 15)],
        [(ldp.at[gid], ldp.at[gid], dev) for _, dev in dp_peers],
    )
    lsends2.start()
    reduce3(1)
    scatter(1)
    gather(0)
    reduce3(2)
    gather(1)
    scatter(2)
    forward(0)
    drain([lsends] + sum(stage2, []))
    take(lsends2)
    total = ldp[0]
    for i in range(1, 16):
        total = total + ldp[i]
    loss_o[...] = (total / (2.0 * KV * count))[:, 0:1]
    drain([lsends2] + sum(stage3, []) + swaps)
    gather(2)
    forward(1)
    drain(agz[0] + agz[1] + agx[0])
    for i in range(CH):
        take(agx[i][-1])
    ordered = [
        done(i)[xx, 2 * side + l].astype(F32)
        for side in range(2) for i in range(CH) for xx in range(4) for l in range(2)
    ]
    kt[...] = jnp.transpose(jnp.concatenate(ordered, axis=0))
    outs = [
        pltpu.make_async_copy(
            kt.at[pl.ds(half * SL, SL)], key_o.at[:, pl.ds(half * HK, HK)], lsem.at[4 + half]
        )
        for half in range(2)
    ]
    go(*outs)
    drain(agz[2] + agx[1] + agx[2])
    for copy in outs:
        copy.wait()


def finish(key, w, gain, loss, loss_o, gain_o, key_o, wv, sem):
    read = pltpu.make_async_copy(w, wv, sem.at[0])
    write = pltpu.make_async_copy(key, key_o, sem.at[1])
    read.start()
    write.start()
    loss_o[...] = loss[...]
    read.wait()
    summed = lax.dot_general(
        jnp.ones((8, KV), F32), key[...] * wv[...].astype(F32), (((1,), (1,)), ((), ())),
        preferred_element_type=F32, precision=lax.Precision.HIGHEST,
    )
    gain_o[...] = (summed[0:1, :] / gain[...].astype(F32).reshape(1, SL)).reshape(SL)
    write.wait()


def body(hidden_in, teacher, norm_gain, w_key, group_rows, member):
    vm = pl.BlockSpec(memory_space=pltpu.VMEM)
    hbm = pl.BlockSpec(memory_space=pl.ANY)
    far = pl.BlockSpec(memory_space=pltpu.HBM)
    loss, key = pl.pallas_call(
        kernel,
        out_shape=(
            jax.ShapeDtypeStruct((1, 1), F32),
            pltpu.VMEM((SL, KV), F32),
        ),
        in_specs=[far, far, far, vm, vm, vm],
        out_specs=(vm, hbm),
        scratch_shapes=[
            pltpu.VMEM((SL, KV), BF16),
            pltpu.VMEM((2, TOK, D), BF16),
            pltpu.VMEM((2, TOK, HK), BF16),
            pltpu.VMEM((4, YB, HK), BF16),
            pltpu.VMEM((2 * TOK, D), BF16),
            pltpu.VMEM((2, TOK, 128), F32),
            pltpu.VMEM((2 * TOK, HK), F32),
            pltpu.VMEM((HK, 2 * TOK), BF16),
            pltpu.VMEM((4, QK, YB), BF16),
            pltpu.VMEM((QK, 4 * YB), BF16),
            pltpu.VMEM((2, QK, PC), BF16),
            pltpu.VMEM((CH, 4, XK, YB), BF16),
            pltpu.VMEM((2, QK, YB), BF16),
            pltpu.VMEM((2, CH, XK, 4 * YB), BF16),
            pltpu.VMEM((QK, YB), F32),
            pltpu.VMEM((QK, YB), BF16),
            pltpu.VMEM((CH, XK, YB), F32),
            pltpu.VMEM((CH, 3, XK, YB), BF16),
            pltpu.VMEM((CH, 3, XK, YB), BF16),
            pltpu.VMEM((CH, 3, XK, YB), BF16),
            pltpu.VMEM((CH, 2, 4, ZK, PC), F32),
            pltpu.VMEM((CH, 2, 4, ZK, PC), BF16),
            pltpu.VMEM((CH, 8, ZK, PC), BF16),
            pltpu.VMEM((CH, ZK, PC), F32),
            pltpu.VMEM((CH, ZK, PC), F32),
            pltpu.VMEM((CH, ZK, PC), F32),
            pltpu.VMEM((CH - 1, 4, 4, ZK, PC), F32),
            pltpu.VMEM((4, 4, ZK, PC), BF16),
            pltpu.VMEM((PC, HK), F32),
            pltpu.VMEM((1, PC + 128), F32),
            pltpu.VMEM((1, PC + 128), F32),
            pltpu.VMEM((8, 1, PC + 128), F32),
            pltpu.VMEM((16, 1, 128), F32),
            pltpu.VMEM((1, 128), F32),
            pltpu.VMEM((1, 128), F32),
            pltpu.VMEM((8, 1, 128), F32),
            pltpu.VMEM((16, 1, 128), F32),
            pltpu.SemaphoreType.DMA((6,)),
            pltpu.SemaphoreType.DMA((N_SLOT,)),
            pltpu.SemaphoreType.DMA((N_SLOT,)),
            pltpu.SemaphoreType.DMA((3,)),
        ],
        compiler_params=pltpu.CompilerParams(
            collective_id=0, has_side_effects=True, vmem_limit_bytes=60 * 2**20
        ),
    )(hidden_in, teacher, w_key, norm_gain, group_rows, member)
    loss, grad_gain, grad_key = pl.pallas_call(
        finish,
        out_shape=(
            jax.ShapeDtypeStruct((1, 1), F32),
            jax.ShapeDtypeStruct((SL,), F32),
            jax.ShapeDtypeStruct((SL, KV), F32),
        ),
        in_specs=[vm, far, vm, vm],
        out_specs=(vm, vm, far),
        scratch_shapes=[pltpu.VMEM((SL, KV), BF16), pltpu.SemaphoreType.DMA((2,))],
        compiler_params=pltpu.CompilerParams(vmem_limit_bytes=8 * 2**20),
    )(key, w_key, norm_gain, loss)
    return loss.reshape(()), grad_gain, grad_key


def solution(mesh):
    split = Mesh(mesh.devices.reshape(4, 4, 2, 4, 2), DP_SHARD)
    return jax.shard_map(
        body,
        mesh=split,
        in_specs=(
            P(DP_SHARD, None),
            P(DP_SHARD, None),
            P(SHARD),
            P(SHARD, None),
            P(DP),
            P(DP, SHARD),
        ),
        out_specs=(P(), P(SHARD), P(SHARD, None)),
        check_vma=False,
    )
```
